32 devices in a mesh: dp: 1 (over z), tp: 4 (over y), pp: 8 (over x, core).
Axes of the slice: x: 4, y: 4, z: 1, core: 2. Of those that a mesh axis runs over, the one named last changes fastest.
The devices are a block of a 4x4x8 slice.
Arguments:
- x_micro: bfloat16 [8, 6, 128, 1536], P(None, 'dp')
- ln1_gain: bfloat16 [8, 1536], P('pp')
- ln1_bias: bfloat16 [8, 1536], P('pp')
- w_qkv: bfloat16 [8, 3, 1536, 16, 96], P('pp', None, None, 'tp')
- b_qkv: bfloat16 [8, 3, 16, 96], P('pp', None, 'tp')
- w_out: bfloat16 [8, 16, 96, 1536], P('pp', 'tp')
- b_out: bfloat16 [8, 1536], P('pp')
- ln2_gain: bfloat16 [8, 1536], P('pp')
- ln2_bias: bfloat16 [8, 1536], P('pp')
- w_up: bfloat16 [8, 1536, 6144], P('pp', None, 'tp')
- b_up: bfloat16 [8, 6144], P('pp', 'tp')
- w_down: bfloat16 [8, 6144, 1536], P('pp', 'tp')
- b_down: bfloat16 [8, 1536], P('pp')
Outputs:
- output: bfloat16 [8, 8, 6, 128, 1536], P('pp', None, 'dp')
All inputs are finite; a program needn't handle non-finite values.
Results may differ from the reference program's by a relative error of at most 0.02.
Values are sent between devices in bfloat16 or wider.
A program may use at most 768 MiB of HBM per device.

```python
import jax
import jax.numpy as jnp
from jax import lax

LAYERS = 8
MICRO_BATCHES = 8
MB_ROWS = 6
SEQ_LEN = 128
D_MODEL = 1536
N_HEADS = 16
HEAD_DIM = 96
FF_DIM = 6144
LN_EPS = 1e-5


def setup_inputs(seed: int = 0, part: int = 0) -> dict:
    base_key = jax.random.key(seed)
    key_list = jax.random.split(base_key, 13)
    x_key = jax.random.fold_in(key_list[0], part)

    def normal_bf16(key_in, shape_dims, scale_by, centre=0.0):
        sample_f32 = jax.random.normal(key_in, shape_dims, jnp.float32) * scale_by + centre
        return sample_f32.astype(jnp.bfloat16)

    return {
        'x_micro': normal_bf16(x_key, (MICRO_BATCHES, MB_ROWS, SEQ_LEN, D_MODEL), 1.0),
        'ln1_gain': normal_bf16(key_list[1], (LAYERS, D_MODEL), 0.2, 1.0),
        'ln1_bias': normal_bf16(key_list[2], (LAYERS, D_MODEL), 0.2),
        'w_qkv': normal_bf16(key_list[3], (LAYERS, 3, D_MODEL, N_HEADS, HEAD_DIM), D_MODEL ** -0.5),
        'b_qkv': normal_bf16(key_list[4], (LAYERS, 3, N_HEADS, HEAD_DIM), 0.5),
        'w_out': normal_bf16(key_list[5], (LAYERS, N_HEADS, HEAD_DIM, D_MODEL), (N_HEADS * HEAD_DIM) ** -0.5),
        'b_out': normal_bf16(key_list[6], (LAYERS, D_MODEL), 0.2),
        'ln2_gain': normal_bf16(key_list[7], (LAYERS, D_MODEL), 0.2, 1.0),
        'ln2_bias': normal_bf16(key_list[8], (LAYERS, D_MODEL), 0.2),
        'w_up': normal_bf16(key_list[9], (LAYERS, D_MODEL, FF_DIM), D_MODEL ** -0.5),
        'b_up': normal_bf16(key_list[10], (LAYERS, FF_DIM), 0.2),
        'w_down': normal_bf16(key_list[11], (LAYERS, FF_DIM, D_MODEL), FF_DIM ** -0.5),
        'b_down': normal_bf16(key_list[12], (LAYERS, D_MODEL), 0.2),
    }


def layer_norm(act_in, gain_vec, bias_vec):
    act_f32 = act_in.astype(jnp.float32)
    row_mean = jnp.mean(act_f32, axis=-1, keepdims=True)
    centered = act_f32 - row_mean
    row_var = jnp.mean(centered * centered, axis=-1, keepdims=True)
    normed = centered * lax.rsqrt(row_var + LN_EPS)
    return (normed * gain_vec.astype(jnp.float32) + bias_vec.astype(jnp.float32)).astype(jnp.bfloat16)


def one_layer(act_in, layer_params):
    ln1_gain, ln1_bias, w_qkv, b_qkv, w_out, b_out, ln2_gain, ln2_bias, w_up, b_up, w_down, b_down = layer_params
    token_rows = MB_ROWS * SEQ_LEN
    head_width = N_HEADS * HEAD_DIM
    flat_in = act_in.reshape(token_rows, D_MODEL)
    normed_in = layer_norm(flat_in, ln1_gain, ln1_bias)
    w_flat = w_qkv.reshape(3, D_MODEL, head_width)
    b_flat = b_qkv.reshape(3, head_width).astype(jnp.float32)
    projected = [
        (jnp.dot(normed_in, w_flat[proj_idx], preferred_element_type=jnp.float32) + b_flat[proj_idx])
        .astype(jnp.bfloat16).astype(jnp.float32).reshape(MB_ROWS, SEQ_LEN, N_HEADS, HEAD_DIM)
        for proj_idx in range(3)
    ]
    query_f, key_f, value_f = projected
    scores = jnp.einsum('bqhd,bkhd->bhqk', query_f, key_f) * (HEAD_DIM ** -0.5)
    causal = lax.broadcasted_iota(jnp.int32, (SEQ_LEN, SEQ_LEN), 0) >= lax.broadcasted_iota(jnp.int32, (SEQ_LEN, SEQ_LEN), 1)
    scores = jnp.where(causal, scores, -1e30)
    attn_probs = jax.nn.softmax(scores, axis=-1).astype(jnp.bfloat16).astype(jnp.float32)
    context = jnp.einsum('bhqk,bkhd->bqhd', attn_probs, value_f).astype(jnp.bfloat16)
    attn_out = (jnp.dot(context.reshape(token_rows, head_width), w_out.reshape(head_width, D_MODEL), preferred_element_type=jnp.float32) + b_out.astype(jnp.float32)).astype(jnp.bfloat16)
    resid_mid = (flat_in.astype(jnp.float32) + attn_out.astype(jnp.float32)).astype(jnp.bfloat16)
    normed_mid = layer_norm(resid_mid, ln2_gain, ln2_bias)
    hidden_up = jax.nn.gelu(jnp.dot(normed_mid, w_up, preferred_element_type=jnp.float32) + b_up.astype(jnp.float32), approximate=True).astype(jnp.bfloat16)
    mlp_out = (jnp.dot(hidden_up, w_down, preferred_element_type=jnp.float32) + b_down.astype(jnp.float32)).astype(jnp.bfloat16)
    result = (resid_mid.astype(jnp.float32) + mlp_out.astype(jnp.float32)).astype(jnp.bfloat16)
    return result.reshape(MB_ROWS, SEQ_LEN, D_MODEL)


def reference(x_micro, ln1_gain, ln1_bias, w_qkv, b_qkv, w_out, b_out, ln2_gain, ln2_bias, w_up, b_up, w_down, b_down):
    stacked_params = (ln1_gain, ln1_bias, w_qkv, b_qkv, w_out, b_out, ln2_gain, ln2_bias, w_up, b_up, w_down, b_down)

    def layer_step(micro_acts, layer_params):
        new_acts = lax.map(lambda micro_in: one_layer(micro_in, layer_params), micro_acts)
        return new_acts, new_acts

    final_acts, y_all = lax.scan(layer_step, x_micro, stacked_params)
    return y_all
```

```python
import functools

import jax
import jax.numpy as jnp
from jax import lax
from jax.experimental import pallas as pl
from jax.experimental.pallas import tpu as pltpu
from jax.sharding import PartitionSpec as P

LN_EPS = 1e-5
MESH = pl.DeviceIdType.MESH
LN_ROWS = 16
UP_CHUNK = 512
DOWN_CHUNK = 512
OUT_CHUNK = 512
QKV_CHUNK = 768


def _f32(val):
    return val.astype(jnp.float32)


def _norm_rows(rows, gain, bias):
    width = rows.shape[-1]
    mean = jnp.sum(rows, axis=-1, keepdims=True) * (1.0 / width)
    cen = rows - mean
    var = jnp.sum(cen * cen, axis=-1, keepdims=True) * (1.0 / width)
    return (cen * lax.rsqrt(var + LN_EPS) * gain + bias).astype(jnp.bfloat16)


def _dot(lhs, rhs):
    return jnp.dot(lhs, rhs, preferred_element_type=jnp.float32)


def _pipeline_kernel(stages, head_dim, x_hbm, wqkv_hbm, wout_hbm, wup_hbm, wdn_hbm, bqkv_in, bup_in,
                     ln1_gain, ln1_bias, b_out, ln2_gain, ln2_bias, b_down,
                     y_hbm,
                     wqkv, wout, wup, wdn, bqkv, bup, xbuf, hbuf, qkv, obuf, acc, x1buf, ubuf, pown, prcv, ybuf,
                     x_sem, yr_sem, wl_sem, ws_sem, wr_sem, os_sem, or_sem, ps_sem, pr_sem, yl_sem, yn_sem, ye_sem, wb_sem):
    units, seq, d_model = xbuf.shape
    group_w = wout_hbm.shape[0]
    group_heads = group_w // head_dim
    qkv_w = 3 * group_w
    ff = wup_hbm.shape[1]
    rr = lax.axis_index("tp")
    pp = lax.axis_index("pp")
    odd_type = ((pp + 1) // 2) % 2
    even_type = 1 - odd_type
    near, far = rr + 1 - 2 * (rr % 2), 3 - rr
    mate = odd_type * near + even_type * far
    twin = odd_type * far + even_type * near
    cross = rr + 2 - 4 * (rr // 2)
    side = odd_type * (rr % 2) + even_type * (rr // 2)
    twin_side = odd_type * (1 - side) + even_type * side
    half = odd_type * (rr // 2) + even_type * (((rr + 1) // 2) % 2)
    base = half * units
    has_next = pp + 1 < stages
    diag_send = (pp % 2 == 0) & (rr % 2 == 0)
    diag_recv = (pp % 2 == 1) & (rr % 2 == 1)

    def local(src, dst, sem):
        return pltpu.make_async_copy(src, dst, sem)

    def remote(src, dst, send, recv, dev):
        return pltpu.make_async_remote_copy(src_ref=src, dst_ref=dst, send_sem=send, recv_sem=recv, device_id=dev, device_id_type=MESH)

    own_cols, twin_cols = pl.ds(0, qkv_w), pl.ds(qkv_w, qkv_w)
    loads = [
        local(wqkv_hbm, wqkv.at[:, own_cols], wl_sem.at[0]),
        local(bqkv_in, bqkv.at[0], wl_sem.at[1]),
        local(wout_hbm, wout.at[2 * side], wl_sem.at[2]),
        local(wup_hbm, wup.at[0], wl_sem.at[3]),
        local(bup_in, bup.at[0], wl_sem.at[4]),
        local(wdn_hbm, wdn.at[0], wl_sem.at[5]),
    ]
    passes = [
        remote(wqkv_hbm, wqkv.at[:, twin_cols], ws_sem.at[0], wr_sem.at[0], {"tp": twin}),
        remote(bqkv_in, bqkv.at[1], ws_sem.at[1], wr_sem.at[1], {"tp": twin}),
        remote(wout_hbm, wout.at[2 * twin_side + 1], ws_sem.at[2], wr_sem.at[2], {"tp": twin}),
        remote(wout_hbm, wout.at[2 * side], ws_sem.at[3], wr_sem.at[3], {"tp": mate}),
        remote(wout_hbm, wout.at[2 * twin_side + 1], ws_sem.at[4], wr_sem.at[4], {"tp": cross}),
        remote(wup_hbm, wup.at[1], ws_sem.at[5], wr_sem.at[5], {"tp": twin}),
        remote(bup_in, bup.at[1], ws_sem.at[6], wr_sem.at[6], {"tp": twin}),
        remote(wdn_hbm, wdn.at[1], ws_sem.at[7], wr_sem.at[7], {"tp": twin}),
    ]

    def x_copy(k):
        return local(x_hbm.at[base + k], xbuf.at[k], x_sem.at[k])

    loads[0].start()
    loads[1].start()

    @pl.when(pp == 0)
    def _():
        def start_x(k, carry):
            x_copy(k).start()
            return carry
        lax.fori_loop(0, units, start_x, 0)

    for copy in loads[2:]:
        copy.start()

    barrier = pltpu.get_barrier_semaphore()

    def greet(dev):
        pl.semaphore_signal(barrier, inc=1, device_id=dev, device_id_type=MESH)

    for other in (mate, twin, cross):
        greet({"tp": other})

    @pl.when(has_next)
    def _():
        greet({"pp": pp + 1})

    @pl.when(pp > 0)
    def _():
        greet({"pp": pp - 1})

    @pl.when(diag_send)
    def _():
        greet({"tp": twin, "pp": pp + 1})

    @pl.when(diag_recv)
    def _():
        greet({"tp": mate, "pp": pp - 1})

    diag_count = (1 - (pp % 2)) * (1 - (rr % 2)) + (pp % 2) * (rr % 2)
    inner = jnp.where(has_next, 1, 0) + jnp.where(pp > 0, 1, 0)
    pl.semaphore_wait(barrier, 3 + inner + diag_count)

    for copy in passes:
        copy.start()

    def wait_weights(load_idx, pass_idx):
        for idx in load_idx:
            loads[idx].wait()
        for idx in pass_idx:
            passes[idx].wait_recv()

    row_id = lax.broadcasted_iota(jnp.int32, (seq, seq), 0)
    col_id = lax.broadcasted_iota(jnp.int32, (seq, seq), 1)

    def o_copy(slot, grp):
        ref = obuf.at[slot, side, :, pl.ds(grp * group_w, group_w)]
        return remote(ref, ref, os_sem.at[slot, grp], or_sem.at[slot, grp], {"tp": mate})

    def p_copy(slot, idx):
        cols = pl.ds(idx * DOWN_CHUNK, DOWN_CHUNK)
        return remote(pown.at[slot, :, cols], prcv.at[slot, :, cols], ps_sem.at[slot, idx], pr_sem.at[slot, idx], {"tp": mate})

    p_chunks = d_model // DOWN_CHUNK

    def y_local(k, slot):
        return local(ybuf.at[slot], y_hbm.at[base + k], yl_sem.at[slot])

    def y_next(k, slot):
        return remote(ybuf.at[slot], xbuf.at[k], yn_sem.at[slot], x_sem.at[k], {"pp": pp + 1})

    def y_twin(k, slot):
        return remote(ybuf.at[slot], y_hbm.at[base + k], ye_sem.at[slot], yr_sem.at[k], {"tp": twin})

    def y_diag(k, slot):
        return remote(ybuf.at[slot], xbuf.at[k], ye_sem.at[slot], x_sem.at[k], {"tp": twin, "pp": pp + 1})

    sends_next = has_next & ((pp % 2 == 1) | (rr % 2 == 0))

    def y_start(k, slot):
        y_local(k, slot).start()

        @pl.when(sends_next)
        def _():
            y_next(k, slot).start()

        @pl.when(diag_send)
        def _():
            y_diag(k, slot).start()

        @pl.when(jnp.logical_not(diag_send))
        def _():
            y_twin(k, slot).start()

    def y_wait(k, slot):
        y_local(k, slot).wait()

        @pl.when(sends_next)
        def _():
            y_next(k, slot).wait_send()

        @pl.when(diag_send)
        def _():
            y_diag(k, slot).wait_send()

        @pl.when(jnp.logical_not(diag_send))
        def _():
            y_twin(k, slot).wait_send()

    def wb_copy(k, slot):
        return remote(xbuf.at[k], y_hbm.at[base + k], wb_sem.at[slot], yr_sem.at[k], {"pp": pp - 1})

    def attention(k):
        slot = k % 2
        x_copy(k).wait()

        @pl.when(diag_recv)
        def _():
            @pl.when(k >= 2)
            def _():
                wb_copy(k - 2, slot).wait_send()
            wb_copy(k, slot).start()

        gain, bias = _f32(ln1_gain[...]), _f32(ln1_bias[...])
        for r0 in range(0, seq, LN_ROWS):
            rows = pl.ds(r0, LN_ROWS)
            hbuf[rows, :] = _norm_rows(_f32(xbuf[k, rows, :]), gain, bias)

        @pl.when(k == 0)
        def _():
            wait_weights((0, 1), (0, 1))

        for c0 in range(0, 2 * qkv_w, QKV_CHUNK):
            grp, off = c0 // qkv_w, c0 % qkv_w
            cols = pl.ds(c0, QKV_CHUNK)
            if off + QKV_CHUNK <= qkv_w:
                add = _f32(bqkv[grp, :, pl.ds(off, QKV_CHUNK)])
            else:
                add = jnp.concatenate([_f32(bqkv[grp, :, pl.ds(off, qkv_w - off)]), _f32(bqkv[grp + 1, :, pl.ds(0, QKV_CHUNK - (qkv_w - off))])], axis=1)
            qkv[:, cols] = (_dot(hbuf[...], wqkv[:, cols]) + add).astype(jnp.bfloat16)

        @pl.when(k >= 2)
        def _():
            for grp in range(2):
                o_copy(slot, grp).wait_send()

        lane_head = lax.broadcasted_iota(jnp.int32, (seq, group_w), 1)
        masks = [(lane_head >= hd * head_dim) & (lane_head < (hd + 1) * head_dim) for hd in range(group_heads)]
        causal = row_id >= col_id
        for grp in range(2):
            q = qkv[:, pl.ds(grp * qkv_w, group_w)]
            key = qkv[:, pl.ds(grp * qkv_w + group_w, group_w)]
            val = qkv[:, pl.ds(grp * qkv_w + 2 * group_w, group_w)]
            zero = jnp.zeros_like(q)
            q_heads = jnp.concatenate([jnp.where(m, q, zero) for m in masks], axis=0)
            scores = lax.dot_general(q_heads, key, (((1,), (1,)), ((), ())), preferred_element_type=jnp.float32)
            probs = []
            for hd in range(group_heads):
                sc = jnp.where(causal, scores[hd * seq:(hd + 1) * seq] * (head_dim ** -0.5), -1e30)
                ex = jnp.exp(sc - jnp.max(sc, axis=-1, keepdims=True))
                probs.append((ex / jnp.sum(ex, axis=-1, keepdims=True)).astype(jnp.bfloat16))
            v_heads = jnp.concatenate([jnp.where(m, val, zero) for m in masks], axis=0)
            o_grp = _dot(jnp.concatenate(probs, axis=1), v_heads)
            obuf[slot, side, :, pl.ds(grp * group_w, group_w)] = o_grp.astype(jnp.bfloat16)
            o_copy(slot, grp).start()

    def mlp(k):
        slot = k % 2

        @pl.when(k == 0)
        def _():
            wait_weights((2,), (2, 3, 4))

        for c0 in range(0, d_model, OUT_CHUNK):
            cols = pl.ds(c0, OUT_CHUNK)
            acc[:, cols] = _dot(obuf[slot, side, :, pl.ds(0, group_w * 2)], jnp.concatenate([wout[2 * side, :, cols], wout[2 * side + 1, :, cols]], axis=0))
        for grp in range(2):
            o_copy(slot, grp).wait_recv()
        oth = 1 - side
        for c0 in range(0, d_model, OUT_CHUNK):
            cols = pl.ds(c0, OUT_CHUNK)
            part = _dot(obuf[slot, oth, :, pl.ds(0, group_w * 2)], jnp.concatenate([wout[2 * oth, :, cols], wout[2 * oth + 1, :, cols]], axis=0))
            att = ((acc[:, cols] + part) + _f32(b_out[:, cols])).astype(jnp.bfloat16)
            x1buf[:, cols] = (_f32(xbuf[k, :, cols]) + _f32(att)).astype(jnp.bfloat16)

        gain, bias = _f32(ln2_gain[...]), _f32(ln2_bias[...])
        for r0 in range(0, seq, LN_ROWS):
            rows = pl.ds(r0, LN_ROWS)
            hbuf[rows, :] = _norm_rows(_f32(x1buf[rows, :]), gain, bias)

        @pl.when(k == 0)
        def _():
            wait_weights((3, 4), (5, 6))

        for grp in range(2):
            for c0 in range(0, ff, UP_CHUNK):
                cols = pl.ds(c0, UP_CHUNK)
                pre = _dot(hbuf[...], wup[grp, :, cols]) + _f32(bup[grp, :, cols])
                ubuf[grp, :, cols] = jax.nn.gelu(pre, approximate=True).astype(jnp.bfloat16)

        @pl.when(k == 0)
        def _():
            wait_weights((5,), (7,))

        @pl.when(k >= 2)
        def _():
            for idx in range(p_chunks):
                p_copy(slot, idx).wait_send()

        for idx in range(p_chunks):
            cols = pl.ds(idx * DOWN_CHUNK, DOWN_CHUNK)
            part = _dot(ubuf[0], wdn[0, :, cols]) + _dot(ubuf[1], wdn[1, :, cols])
            pown[slot, :, cols] = part.astype(jnp.bfloat16)
            p_copy(slot, idx).start()

    def finish(k):
        slot = k % 2

        @pl.when(k >= 2)
        def _():
            y_wait(k - 2, slot)

        for idx in range(p_chunks):
            cols = pl.ds(idx * DOWN_CHUNK, DOWN_CHUNK)
            p_copy(slot, idx).wait_recv()
            both = (_f32(pown[slot, :, cols]) + _f32(prcv[slot, :, cols])) + _f32(b_down[:, cols])
            ybuf[slot, :, cols] = (_f32(x1buf[:, cols]) + _f32(both.astype(jnp.bfloat16))).astype(jnp.bfloat16)
        y_start(k, slot)

    def step(k, carry):
        attention(k)

        @pl.when(k >= 1)
        def _():
            finish(k - 1)

        mlp(k)
        return carry

    lax.fori_loop(0, units, step, 0)
    finish(units - 1)

    for k in range(max(units - 2, 0), units):
        slot = k % 2
        for grp in range(2):
            o_copy(slot, grp).wait_send()
        for idx in range(p_chunks):
            p_copy(slot, idx).wait_send()
        y_wait(k, slot)

        @pl.when(diag_recv)
        def _():
            wb_copy(k, slot).wait_send()

    for copy in passes:
        copy.wait_send()

    def wait_y(k, carry):
        y_twin(k, 0).wait_recv()
        return carry

    lax.fori_loop(0, units, wait_y, 0)


def solution(mesh):
    stages = mesh.shape["pp"]
    weight_specs = (
        P('pp', None), P('pp', None),
        P('pp', None, None, 'tp', None), P('pp', None, 'tp', None),
        P('pp', 'tp', None, None), P('pp', None),
        P('pp', None), P('pp', None),
        P('pp', None, 'tp'), P('pp', 'tp'),
        P('pp', 'tp', None), P('pp', None),
    )
    if mesh.shape["tp"] != 4 or stages % 2:
        raise ValueError("unsupported mesh")

    def local_run(x_micro, ln1_gain, ln1_bias, w_qkv, b_qkv, w_out, b_out, ln2_gain, ln2_bias, w_up, b_up, w_down, b_down):
        micro, rows, seq, d_model = x_micro.shape
        total = micro * rows
        units = total // 2
        _, _, _, heads, head_dim = w_qkv.shape
        group_w = heads * head_dim
        ff = w_up.shape[-1]
        x_seqs = x_micro.reshape(total, seq, d_model)
        w_qkv = jnp.transpose(w_qkv[0], (1, 0, 2, 3)).reshape(d_model, 3 * group_w)
        b_qkv = b_qkv.reshape(1, 3 * group_w)
        w_out = w_out.reshape(group_w, d_model)
        any_spec = pl.BlockSpec(memory_space=pl.ANY)
        vmem_spec = pl.BlockSpec(memory_space=pltpu.VMEM)
        bf16, dma = jnp.bfloat16, pltpu.SemaphoreType.DMA
        p_chunks = d_model // DOWN_CHUNK
        y_all = pl.pallas_call(
            functools.partial(_pipeline_kernel, stages, head_dim),
            out_shape=jax.ShapeDtypeStruct((total, seq, d_model), bf16),
            in_specs=[any_spec] * 5 + [any_spec] * 2 + [vmem_spec] * 6,
            out_specs=any_spec,
            scratch_shapes=[
                pltpu.VMEM((d_model, 6 * group_w), bf16),
                pltpu.VMEM((4, group_w, d_model), bf16),
                pltpu.VMEM((2, d_model, ff), bf16),
                pltpu.VMEM((2, ff, d_model), bf16),
                pltpu.VMEM((2, 1, 3 * group_w), bf16),
                pltpu.VMEM((2, 1, ff), bf16),
                pltpu.VMEM((units, seq, d_model), bf16),
                pltpu.VMEM((seq, d_model), bf16),
                pltpu.VMEM((seq, 6 * group_w), bf16),
                pltpu.VMEM((2, 2, seq, 2 * group_w), bf16),
                pltpu.VMEM((seq, d_model), jnp.float32),
                pltpu.VMEM((seq, d_model), bf16),
                pltpu.VMEM((2, seq, ff), bf16),
                pltpu.VMEM((2, seq, d_model), bf16),
                pltpu.VMEM((2, seq, d_model), bf16),
                pltpu.VMEM((2, seq, d_model), bf16),
                dma((units,)), dma((units,)),
                dma((6,)), dma((8,)), dma((8,)),
                dma((2, 2)), dma((2, 2)),
                dma((2, p_chunks)), dma((2, p_chunks)),
                dma((2,)), dma((2,)), dma((2,)), dma((2,)),
            ],
            compiler_params=pltpu.CompilerParams(collective_id=0, has_side_effects=True, vmem_limit_bytes=60 * 1024 * 1024),
            name="stage_pipeline",
        )(x_seqs, w_qkv, w_out, w_up.reshape(d_model, ff), w_down.reshape(ff, d_model), b_qkv, b_up,
          ln1_gain, ln1_bias, b_out, ln2_gain, ln2_bias, b_down)
        return y_all.reshape(1, micro, rows, seq, d_model)

    return jax.shard_map(local_run, mesh=mesh, in_specs=(P(None, 'dp', None, None),) + weight_specs, out_specs=P('pp', None, 'dp', None, None), check_vma=False)
```

```python
import functools

import jax
import jax.numpy as jnp
from jax import lax
from jax.experimental import pallas as pl
from jax.experimental.pallas import tpu as pltpu
from jax.sharding import PartitionSpec as P

LN_EPS = 1e-5
MESH = pl.DeviceIdType.MESH
LN_ROWS = 16
UP_CHUNK = 512
DOWN_CHUNK = 512
OUT_CHUNK = 512
QKV_CHUNK = 768
RELAY_STEPS = 16


def _f32(val):
    return val.astype(jnp.float32)


def _norm_rows(rows, gain, bias):
    width = rows.shape[-1]
    mean = jnp.sum(rows, axis=-1, keepdims=True) * (1.0 / width)
    cen = rows - mean
    var = jnp.sum(cen * cen, axis=-1, keepdims=True) * (1.0 / width)
    return (cen * lax.rsqrt(var + LN_EPS) * gain + bias).astype(jnp.bfloat16)


def _dot(lhs, rhs):
    return jnp.dot(lhs, rhs, preferred_element_type=jnp.float32)


def _pipeline_kernel(stages, head_dim, x_hbm, wqkv_hbm, wout_hbm, wup_hbm, wdn_hbm, bqkv_in, bup_in,
                     ln1_gain, ln1_bias, b_out, ln2_gain, ln2_bias, b_down,
                     y_hbm,
                     wqkv, wout, wup, wdn, bqkv, bup, xbuf, hbuf, qkv, obuf, acc, x1buf, ubuf, pown, prcv, ybuf,
                     x_sem, yr_sem, wl_sem, ws_sem, wr_sem, os_sem, or_sem, ps_sem, pr_sem, yl_sem, yn_sem, ye_sem, wb_sem,
                     relay_a, relay_b, ra_sem, rb_sem, hop_sem):
    units, seq, d_model = xbuf.shape
    group_w = wout_hbm.shape[0]
    group_heads = group_w // head_dim
    qkv_w = 3 * group_w
    ff = wup_hbm.shape[1]
    rr = lax.axis_index("tp")
    pp = lax.axis_index("pp")
    odd_type = ((pp + 1) // 2) % 2
    even_type = 1 - odd_type
    near, far = rr + 1 - 2 * (rr % 2), 3 - rr
    mate = odd_type * near + even_type * far
    twin = odd_type * far + even_type * near
    cross = rr + 2 - 4 * (rr // 2)
    side = odd_type * (rr % 2) + even_type * (rr // 2)
    twin_side = odd_type * (1 - side) + even_type * side
    half = odd_type * (rr // 2) + even_type * (((rr + 1) // 2) % 2)
    base = half * units
    has_next = pp + 1 < stages
    lender = pp < stages // 2
    ally = stages - 2 - pp + 2 * (pp % 2)
    diag_send = (pp % 2 == 0) & (rr % 2 == 0)
    diag_recv = (pp % 2 == 1) & (rr % 2 == 1)

    def local(src, dst, sem):
        return pltpu.make_async_copy(src, dst, sem)

    def remote(src, dst, send, recv, dev):
        return pltpu.make_async_remote_copy(src_ref=src, dst_ref=dst, send_sem=send, recv_sem=recv, device_id=dev, device_id_type=MESH)

    own_cols, twin_cols = pl.ds(0, qkv_w), pl.ds(qkv_w, qkv_w)
    loads = [
        local(wqkv_hbm, wqkv.at[:, own_cols], wl_sem.at[0]),
        local(bqkv_in, bqkv.at[0], wl_sem.at[1]),
        local(wout_hbm, wout.at[2 * side], wl_sem.at[2]),
        local(wup_hbm, wup.at[0], wl_sem.at[3]),
        local(bup_in, bup.at[0], wl_sem.at[4]),
        local(wdn_hbm, wdn.at[0], wl_sem.at[5]),
    ]
    passes = [
        remote(wqkv_hbm, wqkv.at[:, twin_cols], ws_sem.at[0], wr_sem.at[0], {"tp": twin}),
        remote(bqkv_in, bqkv.at[1], ws_sem.at[1], wr_sem.at[1], {"tp": twin}),
        remote(wout_hbm, wout.at[2 * twin_side + 1], ws_sem.at[2], wr_sem.at[2], {"tp": twin}),
        remote(wout_hbm, wout.at[2 * side], ws_sem.at[3], wr_sem.at[3], {"tp": mate}),
        remote(wout.at[2 * side + 1], wout.at[2 * side + 1], ws_sem.at[4], wr_sem.at[4], {"tp": mate}),
        remote(wup_hbm, wup.at[1], ws_sem.at[5], wr_sem.at[5], {"tp": twin}),
        remote(bup_in, bup.at[1], ws_sem.at[6], wr_sem.at[6], {"tp": twin}),
        remote(wdn_hbm, wdn.at[1], ws_sem.at[7], wr_sem.at[7], {"tp": twin}),
    ]

    def x_copy(k):
        return local(x_hbm.at[base + k], xbuf.at[k], x_sem.at[k])

    loads[0].start()
    loads[1].start()

    @pl.when(pp == 0)
    def _():
        def start_x(k, carry):
            x_copy(k).start()
            return carry
        lax.fori_loop(0, units, start_x, 0)

    for copy in loads[2:]:
        copy.start()

    barrier = pltpu.get_barrier_semaphore()

    def greet(dev):
        pl.semaphore_signal(barrier, inc=1, device_id=dev, device_id_type=MESH)

    for other in (mate, twin, cross):
        greet({"tp": other})

    @pl.when(has_next)
    def _():
        greet({"pp": pp + 1})

    @pl.when(pp > 0)
    def _():
        greet({"pp": pp - 1})

    @pl.when(diag_send)
    def _():
        greet({"tp": twin, "pp": pp + 1})

    @pl.when(diag_recv)
    def _():
        greet({"tp": mate, "pp": pp - 1})

    diag_count = (1 - (pp % 2)) * (1 - (rr % 2)) + (pp % 2) * (rr % 2)
    inner = jnp.where(has_next, 1, 0) + jnp.where(pp > 0, 1, 0)
    greet({"pp": ally})
    pl.semaphore_wait(barrier, 4 + inner + diag_count)

    for idx in (2, 0, 1, 5, 6):
        passes[idx].start()

    steps = RELAY_STEPS
    part = ff // steps

    def relay_rows(c):
        return pl.ds(c * part, part)

    def hop_in(c):
        return remote(wdn_hbm.at[relay_rows(c)], relay_a.at[relay_rows(c)], ws_sem.at[7], ra_sem.at[c], {"pp": ally})

    def hop_over(c):
        return remote(relay_a.at[relay_rows(c)], relay_b.at[relay_rows(c)], hop_sem.at[0], rb_sem.at[c], {"tp": mate})

    def hop_out(c):
        return remote(relay_b.at[relay_rows(c)], wdn.at[1, relay_rows(c)], hop_sem.at[1], wr_sem.at[7], {"pp": ally})

    @pl.when(lender)
    def _():
        def lend(c, carry):
            hop_in(c).start()
            return carry
        lax.fori_loop(0, steps, lend, 0)
        passes[3].start()
        passes[2].wait_recv()
        passes[4].start()

    @pl.when(jnp.logical_not(lender))
    def _():
        passes[7].start()

    @pl.when(jnp.logical_not(lender))
    def _():
        def relay(c, carry):
            @pl.when(c < steps)
            def _():
                hop_in(c).wait_recv()
                hop_over(c).start()

            @pl.when(c >= 1)
            def _():
                hop_over(c - 1).wait_recv()
                hop_out(c - 1).start()
            return carry
        lax.fori_loop(0, steps + 1, relay, 0)
        passes[3].start()
        passes[2].wait_recv()
        passes[4].start()

    def wait_weights(load_idx, pass_idx):
        for idx in load_idx:
            loads[idx].wait()
        for idx in pass_idx:
            passes[idx].wait_recv()

    row_id = lax.broadcasted_iota(jnp.int32, (seq, seq), 0)
    col_id = lax.broadcasted_iota(jnp.int32, (seq, seq), 1)

    def o_copy(slot, grp):
        ref = obuf.at[slot, side, :, pl.ds(grp * group_w, group_w)]
        return remote(ref, ref, os_sem.at[slot, grp], or_sem.at[slot, grp], {"tp": mate})

    def p_copy(slot, idx):
        cols = pl.ds(idx * DOWN_CHUNK, DOWN_CHUNK)
        return remote(pown.at[slot, :, cols], prcv.at[slot, :, cols], ps_sem.at[slot, idx], pr_sem.at[slot, idx], {"tp": mate})

    p_chunks = d_model // DOWN_CHUNK

    def y_local(k, slot):
        return local(ybuf.at[slot], y_hbm.at[base + k], yl_sem.at[slot])

    def y_next(k, slot, cols):
        return remote(ybuf.at[slot, :, cols], xbuf.at[k, :, cols], yn_sem.at[slot], x_sem.at[k], {"pp": pp + 1})

    def y_twin(k, slot, cols):
        return remote(ybuf.at[slot, :, cols], y_hbm.at[base + k, :, cols], ye_sem.at[slot], yr_sem.at[k], {"tp": twin})

    def y_diag(k, slot, cols):
        return remote(ybuf.at[slot, :, cols], xbuf.at[k, :, cols], ye_sem.at[slot], x_sem.at[k], {"tp": twin, "pp": pp + 1})

    sends_next = has_next & ((pp % 2 == 1) | (rr % 2 == 0))
    all_cols = pl.ds(0, d_model)

    def y_start(k, slot, cols):
        @pl.when(sends_next)
        def _():
            y_next(k, slot, cols).start()

        @pl.when(diag_send)
        def _():
            y_diag(k, slot, cols).start()

        @pl.when(jnp.logical_not(diag_send))
        def _():
            y_twin(k, slot, cols).start()

    def y_wait(k, slot):
        y_local(k, slot).wait()

        @pl.when(sends_next)
        def _():
            y_next(k, slot, all_cols).wait_send()

        @pl.when(diag_send)
        def _():
            y_diag(k, slot, all_cols).wait_send()

        @pl.when(jnp.logical_not(diag_send))
        def _():
            y_twin(k, slot, all_cols).wait_send()

    def wb_copy(k, slot):
        return remote(xbuf.at[k], y_hbm.at[base + k], wb_sem.at[slot], yr_sem.at[k], {"pp": pp - 1})

    def attention(k):
        slot = k % 2
        x_copy(k).wait()

        @pl.when(diag_recv)
        def _():
            @pl.when(k >= 2)
            def _():
                wb_copy(k - 2, slot).wait_send()
            wb_copy(k, slot).start()

        gain, bias = _f32(ln1_gain[...]), _f32(ln1_bias[...])
        for r0 in range(0, seq, LN_ROWS):
            rows = pl.ds(r0, LN_ROWS)
            hbuf[rows, :] = _norm_rows(_f32(xbuf[k, rows, :]), gain, bias)

        @pl.when(k == 0)
        def _():
            wait_weights((0, 1), (0, 1))

        for c0 in range(0, 2 * qkv_w, QKV_CHUNK):
            grp, off = c0 // qkv_w, c0 % qkv_w
            cols = pl.ds(c0, QKV_CHUNK)
            if off + QKV_CHUNK <= qkv_w:
                add = _f32(bqkv[grp, :, pl.ds(off, QKV_CHUNK)])
            else:
                add = jnp.concatenate([_f32(bqkv[grp, :, pl.ds(off, qkv_w - off)]), _f32(bqkv[grp + 1, :, pl.ds(0, QKV_CHUNK - (qkv_w - off))])], axis=1)
            qkv[:, cols] = (_dot(hbuf[...], wqkv[:, cols]) + add).astype(jnp.bfloat16)

        @pl.when(k >= 2)
        def _():
            for grp in range(2):
                o_copy(slot, grp).wait_send()

        lane_head = lax.broadcasted_iota(jnp.int32, (seq, group_w), 1)
        masks = [(lane_head >= hd * head_dim) & (lane_head < (hd + 1) * head_dim) for hd in range(group_heads)]
        causal = row_id >= col_id
        for grp in range(2):
            q = qkv[:, pl.ds(grp * qkv_w, group_w)]
            key = qkv[:, pl.ds(grp * qkv_w + group_w, group_w)]
            val = qkv[:, pl.ds(grp * qkv_w + 2 * group_w, group_w)]
            zero = jnp.zeros_like(q)
            q_heads = jnp.concatenate([jnp.where(m, q, zero) for m in masks], axis=0)
            scores = lax.dot_general(q_heads, key, (((1,), (1,)), ((), ())), preferred_element_type=jnp.float32)
            probs = []
            for hd in range(group_heads):
                sc = jnp.where(causal, scores[hd * seq:(hd + 1) * seq] * (head_dim ** -0.5), -1e30)
                ex = jnp.exp(sc - jnp.max(sc, axis=-1, keepdims=True))
                probs.append((ex / jnp.sum(ex, axis=-1, keepdims=True)).astype(jnp.bfloat16))
            v_heads = jnp.concatenate([jnp.where(m, val, zero) for m in masks], axis=0)
            o_grp = _dot(jnp.concatenate(probs, axis=1), v_heads)
            obuf[slot, side, :, pl.ds(grp * group_w, group_w)] = o_grp.astype(jnp.bfloat16)
            o_copy(slot, grp).start()

    def mlp(k):
        slot = k % 2

        @pl.when(k == 0)
        def _():
            wait_weights((2,), (3, 4))

        for c0 in range(0, d_model, OUT_CHUNK):
            cols = pl.ds(c0, OUT_CHUNK)
            acc[:, cols] = _dot(obuf[slot, side, :, pl.ds(0, group_w * 2)], jnp.concatenate([wout[2 * side, :, cols], wout[2 * side + 1, :, cols]], axis=0))
        for grp in range(2):
            o_copy(slot, grp).wait_recv()
        oth = 1 - side
        for c0 in range(0, d_model, OUT_CHUNK):
            cols = pl.ds(c0, OUT_CHUNK)
            part = _dot(obuf[slot, oth, :, pl.ds(0, group_w * 2)], jnp.concatenate([wout[2 * oth, :, cols], wout[2 * oth + 1, :, cols]], axis=0))
            att = ((acc[:, cols] + part) + _f32(b_out[:, cols])).astype(jnp.bfloat16)
            x1buf[slot, :, cols] = (_f32(xbuf[k, :, cols]) + _f32(att)).astype(jnp.bfloat16)

        gain, bias = _f32(ln2_gain[...]), _f32(ln2_bias[...])
        for r0 in range(0, seq, LN_ROWS):
            rows = pl.ds(r0, LN_ROWS)
            hbuf[rows, :] = _norm_rows(_f32(x1buf[slot, rows, :]), gain, bias)

        @pl.when(k == 0)
        def _():
            wait_weights((3, 4), (5, 6))

        for grp in range(2):
            for c0 in range(0, ff, UP_CHUNK):
                cols = pl.ds(c0, UP_CHUNK)
                pre = _dot(hbuf[...], wup[grp, :, cols]) + _f32(bup[grp, :, cols])
                ubuf[grp, :, cols] = jax.nn.gelu(pre, approximate=True).astype(jnp.bfloat16)

        @pl.when(k == 0)
        def _():
            wait_weights((5,), (7,))

        @pl.when(k >= 2)
        def _():
            for idx in range(p_chunks):
                p_copy(slot, idx).wait_send()

        for idx in range(p_chunks):
            cols = pl.ds(idx * DOWN_CHUNK, DOWN_CHUNK)
            part = _dot(ubuf[0], wdn[0, :, cols]) + _dot(ubuf[1], wdn[1, :, cols])
            pown[slot, :, cols] = part.astype(jnp.bfloat16)
            p_copy(slot, idx).start()

    def finish(k):
        slot = k % 2

        @pl.when(k >= 2)
        def _():
            y_wait(k - 2, slot)

        for idx in range(p_chunks):
            cols = pl.ds(idx * DOWN_CHUNK, DOWN_CHUNK)
            p_copy(slot, idx).wait_recv()
            both = (_f32(pown[slot, :, cols]) + _f32(prcv[slot, :, cols])) + _f32(b_down[:, cols])
            ybuf[slot, :, cols] = (_f32(x1buf[slot, :, cols]) + _f32(both.astype(jnp.bfloat16))).astype(jnp.bfloat16)
            y_start(k, slot, cols)
        y_local(k, slot).start()

    def step(i, carry):
        def attention_pair(par, inner):
            attention(2 * i + par)

            @pl.when((par == 0) & (i >= 1))
            def _():
                finish(2 * i - 1)
            return inner

        def mlp_pair(par, inner):
            mlp(2 * i + par)
            return inner

        lax.fori_loop(0, 2, attention_pair, 0)
        lax.fori_loop(0, 2, mlp_pair, 0)
        finish(2 * i)
        return carry

    lax.fori_loop(0, units // 2, step, 0)
    finish(units - 1)

    for k in range(max(units - 2, 0), units):
        slot = k % 2
        for grp in range(2):
            o_copy(slot, grp).wait_send()
        for idx in range(p_chunks):
            p_copy(slot, idx).wait_send()
        y_wait(k, slot)

        @pl.when(diag_recv)
        def _():
            wb_copy(k, slot).wait_send()

    for copy in passes:
        copy.wait_send()

    @pl.when(jnp.logical_not(lender))
    def _():
        remote(relay_a, relay_b, hop_sem.at[0], rb_sem.at[0], {"tp": mate}).wait_send()
        remote(relay_b, wdn.at[1], hop_sem.at[1], wr_sem.at[7], {"pp": ally}).wait_send()

    def wait_y(k, carry):
        y_twin(k, 0, all_cols).wait_recv()
        return carry

    lax.fori_loop(0, units, wait_y, 0)


def solution(mesh):
    stages = mesh.shape["pp"]
    weight_specs = (
        P('pp', None), P('pp', None),
        P('pp', None, None, 'tp', None), P('pp', None, 'tp', None),
        P('pp', 'tp', None, None), P('pp', None),
        P('pp', None), P('pp', None),
        P('pp', None, 'tp'), P('pp', 'tp'),
        P('pp', 'tp', None), P('pp', None),
    )
    if mesh.shape["tp"] != 4 or stages % 4:
        raise ValueError("unsupported mesh")

    def local_run(x_micro, ln1_gain, ln1_bias, w_qkv, b_qkv, w_out, b_out, ln2_gain, ln2_bias, w_up, b_up, w_down, b_down):
        micro, rows, seq, d_model = x_micro.shape
        total = micro * rows
        units = total // 2
        _, _, _, heads, head_dim = w_qkv.shape
        group_w = heads * head_dim
        ff = w_up.shape[-1]
        x_seqs = x_micro.reshape(total, seq, d_model)
        w_qkv = jnp.transpose(w_qkv[0], (1, 0, 2, 3)).reshape(d_model, 3 * group_w)
        b_qkv = b_qkv.reshape(1, 3 * group_w)
        w_out = w_out.reshape(group_w, d_model)
        any_spec = pl.BlockSpec(memory_space=pl.ANY)
        vmem_spec = pl.BlockSpec(memory_space=pltpu.VMEM)
        bf16, dma = jnp.bfloat16, pltpu.SemaphoreType.DMA
        p_chunks = d_model // DOWN_CHUNK
        y_all = pl.pallas_call(
            functools.partial(_pipeline_kernel, stages, head_dim),
            out_shape=jax.ShapeDtypeStruct((total, seq, d_model), bf16),
            in_specs=[any_spec] * 5 + [any_spec] * 2 + [vmem_spec] * 6,
            out_specs=any_spec,
            scratch_shapes=[
                pltpu.VMEM((d_model, 6 * group_w), bf16),
                pltpu.VMEM((4, group_w, d_model), bf16),
                pltpu.VMEM((2, d_model, ff), bf16),
                pltpu.VMEM((2, ff, d_model), bf16),
                pltpu.VMEM((2, 1, 3 * group_w), bf16),
                pltpu.VMEM((2, 1, ff), bf16),
                pltpu.VMEM((units, seq, d_model), bf16),
                pltpu.VMEM((seq, d_model), bf16),
                pltpu.VMEM((seq, 6 * group_w), bf16),
                pltpu.VMEM((2, 2, seq, 2 * group_w), bf16),
                pltpu.VMEM((seq, d_model), jnp.float32),
                pltpu.VMEM((2, seq, d_model), bf16),
                pltpu.VMEM((2, seq, ff), bf16),
                pltpu.VMEM((2, seq, d_model), bf16),
                pltpu.VMEM((2, seq, d_model), bf16),
                pltpu.VMEM((2, seq, d_model), bf16),
                dma((units,)), dma((units,)),
                dma((6,)), dma((8,)), dma((8,)),
                dma((2, 2)), dma((2, 2)),
                dma((2, p_chunks)), dma((2, p_chunks)),
                dma((2,)), dma((2,)), dma((2,)), dma((2,)),
                pltpu.VMEM((ff, d_model), bf16),
                pltpu.VMEM((ff, d_model), bf16),
                dma((RELAY_STEPS,)), dma((RELAY_STEPS,)), dma((2,)),
            ],
            compiler_params=pltpu.CompilerParams(collective_id=0, has_side_effects=True, vmem_limit_bytes=60 * 1024 * 1024),
            name="stage_pipeline",
        )(x_seqs, w_qkv, w_out, w_up.reshape(d_model, ff), w_down.reshape(ff, d_model), b_qkv, b_up,
          ln1_gain, ln1_bias, b_out, ln2_gain, ln2_bias, b_down)
        return y_all.reshape(1, micro, rows, seq, d_model)

    return jax.shard_map(local_run, mesh=mesh, in_specs=(P(None, 'dp', None, None),) + weight_specs, out_specs=P('pp', None, 'dp', None, None), check_vma=False)
```

```python
import functools

import jax
import jax.numpy as jnp
from jax import lax
from jax.experimental import pallas as pl
from jax.experimental.pallas import tpu as pltpu
from jax.sharding import PartitionSpec as P

LN_EPS = 1e-5
MESH = pl.DeviceIdType.MESH
LN_ROWS = 16
UP_CHUNK = 512
DOWN_CHUNK = 512
OUT_CHUNK = 512
RELAY_STEPS = 16
LAGGED_STAGES = 2
EAGER_UNITS = (0, 0, 1, 12)
TURN_ROWS = 128


def _f32(val):
    return val.astype(jnp.float32)


def _norm_rows(rows, gain, bias):
    width = rows.shape[-1]
    mean = jnp.sum(rows, axis=-1, keepdims=True) * (1.0 / width)
    cen = rows - mean
    var = jnp.sum(cen * cen, axis=-1, keepdims=True) * (1.0 / width)
    return (cen * lax.rsqrt(var + LN_EPS) * gain + bias).astype(jnp.bfloat16)


def _dot(lhs, rhs):
    return jnp.dot(lhs, rhs, preferred_element_type=jnp.float32)


def _pipeline_kernel(stages, head_dim, x_hbm, wqkv_hbm, wout_hbm, wup_hbm, wdn_hbm, bqkv_in, bup_in,
                     ln1_gain, ln1_bias, b_out, ln2_gain, ln2_bias, b_down,
                     y_hbm,
                     wqkv, wout, wup, wdn, bqkv, bup, xbuf, hbuf, qkv, obuf, acc, x1buf, ubuf, pown, prcv, ybuf,
                     relay_a, relay_b, turn,
                     x_sem, wl_sem, ws_sem, wr_sem, os_sem, or_sem, ps_sem, pr_sem, yl_sem, yn_sem, yd_sem, ym_sem, ymr_sem, yf_sem, yt_sem, yl_late,
                     wb_sem, ra_sem, rb_sem, hop_sem):
    _, units, seq, d_model = xbuf.shape
    group_w = wout_hbm.shape[0]
    group_heads = group_w // head_dim
    qk_w = 2 * group_w
    v_col = 2 * qk_w
    ff = wup_hbm.shape[1]
    rr = lax.axis_index("tp")
    pp = lax.axis_index("pp")
    odd = pp % 2
    near, far = rr + 1 - 2 * (rr % 2), 3 - rr
    mate = odd * near + (1 - odd) * far
    twin = odd * far + (1 - odd) * near
    has_next = pp + 1 < stages
    has_prev = pp > 0
    lagged = pp >= stages - LAGGED_STAGES
    is_last = pp == stages - 1
    eager = 0
    for quarter, amount in enumerate(EAGER_UNITS):
        eager = eager + jnp.where(pp * len(EAGER_UNITS) // stages == quarter, min(amount, units), 0)
    lender = pp < stages // 2
    ally = stages - 1 - pp
    OWN, MATE = 0, 1

    def local(src, dst, sem):
        return pltpu.make_async_copy(src, dst, sem)

    def remote(src, dst, send, recv, dev):
        return pltpu.make_async_remote_copy(src_ref=src, dst_ref=dst, send_sem=send, recv_sem=recv, device_id=dev, device_id_type=MESH)

    own_qk, twin_qk = pl.ds(0, qk_w), pl.ds(qk_w, qk_w)
    own_v, twin_v = pl.ds(v_col, group_w), pl.ds(v_col + group_w, group_w)
    turn_rows = turn.shape[1]
    turns = 3 * group_w // turn_rows

    def turn_load(c, slot):
        return local(wqkv_hbm.at[pl.ds(c * turn_rows, turn_rows)], turn.at[slot], wl_sem.at[slot])

    loads = [
        local(wout_hbm, wout.at[0], wl_sem.at[2]),
        local(wup_hbm, wup.at[0], wl_sem.at[3]),
        local(bup_in, bup.at[0], wl_sem.at[4]),
        local(wdn_hbm, wdn.at[0], wl_sem.at[5]),
    ]
    to_twin, to_mate = {"tp": twin}, {"tp": mate}
    passes = [
        remote(wqkv.at[:, own_qk], wqkv.at[:, twin_qk], ws_sem.at[0], wr_sem.at[0], to_twin),
        remote(bqkv.at[:, own_qk], bqkv.at[:, twin_qk], ws_sem.at[1], wr_sem.at[1], to_twin),
        remote(wout_hbm, wout.at[1], ws_sem.at[2], wr_sem.at[2], to_twin),
        remote(wout_hbm, wout.at[2], ws_sem.at[3], wr_sem.at[3], to_mate),
        remote(wout.at[1], wout.at[3], ws_sem.at[4], wr_sem.at[4], to_mate),
        remote(wup_hbm, wup.at[1], ws_sem.at[5], wr_sem.at[5], to_twin),
        remote(bup_in, bup.at[1], ws_sem.at[6], wr_sem.at[6], to_twin),
        remote(wdn_hbm, wdn.at[1], ws_sem.at[7], wr_sem.at[7], to_twin),
        remote(wqkv.at[:, own_v], wqkv.at[:, twin_v], ws_sem.at[8], wr_sem.at[8], to_twin),
        remote(bqkv.at[:, own_v], bqkv.at[:, twin_v], ws_sem.at[9], wr_sem.at[9], to_twin),
    ]

    def x_load(kind, i, row):
        return local(x_hbm.at[row * units + i], xbuf.at[kind, i], x_sem.at[kind, i])

    turn_load(0, 0).start()
    turn_load(1, 1).start()

    @pl.when(pp == 0)
    def _():
        def start_x(i, carry):
            x_load(OWN, i, rr).start()
            x_load(MATE, i, mate).start()
            return carry
        lax.fori_loop(0, units, start_x, 0)

    for copy in loads:
        copy.start()

    barrier = pltpu.get_barrier_semaphore()

    def greet(dev):
        pl.semaphore_signal(barrier, inc=1, device_id=dev, device_id_type=MESH)

    greet(to_mate)
    greet(to_twin)
    greet({"pp": ally})

    @pl.when(has_next)
    def _():
        greet({"pp": pp + 1})
        greet({"tp": twin, "pp": pp + 1})

    @pl.when(has_prev)
    def _():
        greet({"pp": pp - 1})
        greet({"tp": mate, "pp": pp - 1})

    pl.semaphore_wait(barrier, 3 + 2 * (jnp.where(has_next, 1, 0) + jnp.where(has_prev, 1, 0)))

    passes[2].start()

    steps = RELAY_STEPS
    part = ff // steps
    lend_some = max(steps // 4, 1)
    lends_all = (pp < stages // 4) | (pp >= stages - stages // 4)
    lent = jnp.where(lends_all, steps, lend_some)

    def relay_rows(c):
        return pl.ds(c * part, part)

    def hop_in(c):
        return remote(wdn_hbm.at[relay_rows(c)], relay_a.at[relay_rows(c)], ws_sem.at[7], ra_sem.at[c], {"pp": ally})

    def hop_over(c):
        return remote(relay_a.at[relay_rows(c)], relay_b.at[relay_rows(c)], hop_sem.at[0], rb_sem.at[c], to_mate)

    def hop_out(c):
        return remote(relay_b.at[relay_rows(c)], wdn.at[1, relay_rows(c)], hop_sem.at[1], wr_sem.at[7], {"pp": ally})

    def direct(c):
        return remote(wdn_hbm.at[relay_rows(c)], wdn.at[1, relay_rows(c)], ws_sem.at[7], wr_sem.at[7], to_twin)

    @pl.when(lender)
    def _():
        def lend(c, carry):
            hop_in(c).start()
            return carry
        lax.fori_loop(0, lent, lend, 0)
        passes[3].start()
        passes[2].wait_recv()
        passes[4].start()

    def turn_block(c, carry):
        slot = c % 2
        turn_load(c, slot).wait()
        first = c * turn_rows
        col = first + (first // qk_w) * (v_col - qk_w)
        wqkv[:, pl.ds(pl.multiple_of(col, 128), turn_rows)] = turn[slot].T

        @pl.when(c + 2 < turns)
        def _():
            turn_load(c + 2, slot).start()
        return carry

    lax.fori_loop(0, turns, turn_block, 0)
    spread_row = lax.broadcasted_iota(jnp.int32, (head_dim, group_w), 0)
    spread_col = lax.broadcasted_iota(jnp.int32, (head_dim, group_w), 1)
    spread = jnp.zeros((head_dim, group_w), jnp.float32)
    for hd in range(group_heads):
        spread = spread + jnp.where(spread_row + hd * head_dim == spread_col, 1.0, 0.0)
    spread = spread.astype(jnp.bfloat16)
    head_row = lax.broadcasted_iota(jnp.int32, (group_heads, group_w), 0)
    head_lane = lax.broadcasted_iota(jnp.int32, (group_heads, group_w), 1)
    in_head = (head_lane >= head_row * head_dim) & (head_lane < (head_row + 1) * head_dim)
    for third in range(3):
        wide = jnp.where(in_head, _dot(bqkv_in[0, third], spread), 0.0)
        col = third * group_w if third < 2 else v_col
        bqkv[:, pl.ds(col, group_w)] = jnp.sum(wide, axis=0, keepdims=True)
    for idx in (0, 8, 1, 9, 5, 6):
        passes[idx].start()

    @pl.when(lender)
    def _():
        def keep(c, carry):
            direct(c).start()
            return carry
        lax.fori_loop(lent, steps, keep, 0)

    @pl.when(jnp.logical_not(lender))
    def _():
        passes[7].start()

        def relay(c, carry):
            @pl.when(c < lent)
            def _():
                hop_in(c).wait_recv()
                hop_over(c).start()

            @pl.when(c >= 1)
            def _():
                hop_over(c - 1).wait_recv()
                hop_out(c - 1).start()
            return carry
        lax.fori_loop(0, lent + 1, relay, 0)
        passes[3].start()
        passes[2].wait_recv()
        passes[4].start()

    def wait_weights(load_idx, pass_idx):
        for idx in load_idx:
            loads[idx].wait()
        for idx in pass_idx:
            passes[idx].wait_recv()

    row_id = lax.broadcasted_iota(jnp.int32, (seq, seq), 0)
    col_id = lax.broadcasted_iota(jnp.int32, (seq, seq), 1)

    def o_copy(kind, slot, grp):
        cols = pl.ds(grp * group_w, group_w)
        return remote(obuf.at[slot, kind, 0, :, cols], obuf.at[slot, 1 - kind, 1, :, cols],
                      os_sem.at[slot, kind, grp], or_sem.at[slot, 1 - kind, grp], to_mate)

    def p_copy(slot, idx):
        cols = pl.ds(idx * DOWN_CHUNK, DOWN_CHUNK)
        return remote(pown.at[MATE, :, cols], prcv.at[slot, :, cols], ps_sem.at[idx], pr_sem.at[slot, idx], to_mate)

    p_chunks = d_model // DOWN_CHUNK
    all_cols = pl.ds(0, d_model)

    def y_local(i, slot):
        return local(ybuf.at[slot], y_hbm.at[rr * units + i], yl_sem.at[slot])

    def y_next(i, slot, cols):
        return remote(ybuf.at[slot, :, cols], xbuf.at[OWN, i, :, cols], yn_sem.at[slot], x_sem.at[OWN, i], {"pp": pp + 1})

    def y_diag(i, slot, cols):
        return remote(ybuf.at[slot, :, cols], xbuf.at[MATE, i, :, cols], yd_sem.at[slot], x_sem.at[MATE, i], {"tp": twin, "pp": pp + 1})

    def y_twin(i, slot, cols):
        return remote(ybuf.at[slot, :, cols], y_hbm.at[rr * units + i, :, cols], yd_sem.at[slot], yt_sem.at[i], to_twin)

    def y_mate(i, slot):
        return remote(ybuf.at[slot], y_hbm.at[rr * units + i], ym_sem.at[slot], ymr_sem.at[i], to_mate)

    def y_mate_late(i):
        ref = y_hbm.at[rr * units + i]
        return remote(ref, ref, yl_late.at[i], ymr_sem.at[i], to_mate)

    def y_forward_mate(i):
        ref = y_hbm.at[mate * units + i]
        return remote(ref, ref, yf_sem.at[0], yf_sem.at[1], to_twin)

    def y_forward_twin(i):
        ref = y_hbm.at[twin * units + i]
        return remote(ref, ref, yf_sem.at[0], yf_sem.at[1], to_mate)

    def twin_arrival(i):
        ref = y_hbm.at[twin * units + i]
        return remote(ref, ref, yd_sem.at[0], yt_sem.at[i], to_twin)

    def y_forward(i):
        by_mate = is_last & (i % 2 == 0)

        @pl.when(by_mate)
        def _():
            twin_arrival(i).wait_recv()
            y_forward_twin(i).start()

        @pl.when(jnp.logical_not(by_mate))
        def _():
            y_mate_late(i).wait_recv()
            y_forward_mate(i).start()

    def y_start(i, slot, cols):
        @pl.when(has_next)
        def _():
            y_next(i, slot, cols).start()
            y_diag(i, slot, cols).start()

        @pl.when(jnp.logical_not(has_next))
        def _():
            y_twin(i, slot, cols).start()

    def y_wait(i, slot):
        y_local(i, slot).wait()

        @pl.when(has_next)
        def _():
            y_next(i, slot, all_cols).wait_send()
            y_diag(i, slot, all_cols).wait_send()

        @pl.when(jnp.logical_not(has_next))
        def _():
            y_twin(i, slot, all_cols).wait_send()

        @pl.when(i < eager)
        def _():
            y_mate(i, slot).wait_send()

    def wb_copy(i, slot):
        return remote(xbuf.at[MATE, i], y_hbm.at[mate * units + i], wb_sem.at[slot], yt_sem.at[i], {"pp": pp - 1})

    def attention(kind, i):
        slot = i % 2
        x_load(kind, i, rr).wait()

        @pl.when((kind == MATE) & has_prev)
        def _():
            @pl.when(i >= 2)
            def _():
                wb_copy(i - 2, slot).wait_send()
            wb_copy(i, slot).start()

        @pl.when((kind == OWN) & (i == 0))
        def _():
            wait_weights((), (0, 1, 8, 9))

        @pl.when(i >= 2)
        def _():
            for grp in range(2):
                o_copy(kind, slot, grp).wait_send()

        gain, bias = _f32(ln1_gain[...]), _f32(ln1_bias[...])
        for r0 in range(0, seq, LN_ROWS):
            rows = pl.ds(r0, LN_ROWS)
            hbuf[rows, :] = _norm_rows(_f32(xbuf[kind, i, rows, :]), gain, bias)

        lane_head = lax.broadcasted_iota(jnp.int32, (seq, group_w), 1)
        masks = [(lane_head >= hd * head_dim) & (lane_head < (hd + 1) * head_dim) for hd in range(group_heads)]
        causal = row_id >= col_id

        def project(col):
            cols = pl.ds(col, qk_w)
            qkv[:, cols] = (_dot(hbuf[...], wqkv[:, cols]) + bqkv[:, cols]).astype(jnp.bfloat16)

        def by_head(act):
            zero = jnp.zeros_like(act)
            return jnp.concatenate([jnp.where(m, act, zero) for m in masks], axis=0)

        def scores_of(grp):
            q_heads = by_head(qkv[:, pl.ds(grp * qk_w, group_w)])
            key = qkv[:, pl.ds(grp * qk_w + group_w, group_w)]
            return lax.dot_general(q_heads, key, (((1,), (1,)), ((), ())), preferred_element_type=jnp.float32)

        def probs_of(scores):
            probs = []
            for hd in range(group_heads):
                sc = jnp.where(causal, scores[hd * seq:(hd + 1) * seq] * (head_dim ** -0.5), -1e30)
                ex = jnp.exp(sc - jnp.max(sc, axis=-1, keepdims=True))
                probs.append((ex * (1.0 / jnp.sum(ex, axis=-1, keepdims=True))).astype(jnp.bfloat16))
            return jnp.concatenate(probs, axis=1)

        project(0)
        scores_0 = scores_of(0)
        project(qk_w)
        probs_0 = probs_of(scores_0)
        scores_1 = scores_of(1)
        project(v_col)
        probs_1 = probs_of(scores_1)
        for grp, probs in enumerate((probs_0, probs_1)):
            val = qkv[:, pl.ds(v_col + grp * group_w, group_w)]
            obuf[slot, kind, 0, :, pl.ds(grp * group_w, group_w)] = _dot(probs, by_head(val)).astype(jnp.bfloat16)
            o_copy(kind, slot, grp).start()

    def mlp(kind, i):
        slot = i % 2
        if kind == MATE:
            @pl.when(i == 0)
            def _():
                wait_weights((0,), (3, 4))

        def out_part(half, cols):
            return _dot(obuf[slot, kind, half], jnp.concatenate([wout[2 * half, :, cols], wout[2 * half + 1, :, cols]], axis=0))

        for c0 in range(0, d_model, OUT_CHUNK):
            cols = pl.ds(c0, OUT_CHUNK)
            acc[:, cols] = out_part(0, cols)
        for grp in range(2):
            o_copy(1 - kind, slot, grp).wait_recv()
        for c0 in range(0, d_model, OUT_CHUNK):
            cols = pl.ds(c0, OUT_CHUNK)
            att = ((acc[:, cols] + out_part(1, cols)) + _f32(b_out[:, cols])).astype(jnp.bfloat16)
            x1buf[:, cols] = (_f32(xbuf[kind, i, :, cols]) + _f32(att)).astype(jnp.bfloat16)

        gain, bias = _f32(ln2_gain[...]), _f32(ln2_bias[...])
        for r0 in range(0, seq, LN_ROWS):
            rows = pl.ds(r0, LN_ROWS)
            hbuf[rows, :] = _norm_rows(_f32(x1buf[rows, :]), gain, bias)

        if kind == MATE:
            @pl.when(i == 0)
            def _():
                wait_weights((1, 2), (5, 6))

        for grp in range(2):
            for c0 in range(0, ff, UP_CHUNK):
                cols = pl.ds(c0, UP_CHUNK)
                pre = _dot(hbuf[...], wup[grp, :, cols]) + _f32(bup[grp, :, cols])
                ubuf[grp, :, cols] = jax.nn.gelu(pre, approximate=True).astype(jnp.bfloat16)

        if kind == MATE:
            @pl.when(i == 0)
            def _():
                wait_weights((3,), (7,))

            @pl.when(i >= 1)
            def _():
                for idx in range(p_chunks):
                    p_copy(slot, idx).wait_send()

        for idx in range(p_chunks):
            cols = pl.ds(idx * DOWN_CHUNK, DOWN_CHUNK)
            pown[kind, :, cols] = (_dot(ubuf[0], wdn[0, :, cols]) + _dot(ubuf[1], wdn[1, :, cols])).astype(jnp.bfloat16)
            if kind == MATE:
                p_copy(slot, idx).start()

    def finish(i):
        slot = i % 2

        @pl.when(i >= 2)
        def _():
            y_wait(i - 2, slot)

        for idx in range(p_chunks):
            cols = pl.ds(idx * DOWN_CHUNK, DOWN_CHUNK)
            p_copy(slot, idx).wait_recv()
            both = (_f32(pown[OWN, :, cols]) + _f32(prcv[slot, :, cols])) + _f32(b_down[:, cols])
            ybuf[slot, :, cols] = (_f32(x1buf[:, cols]) + _f32(both.astype(jnp.bfloat16))).astype(jnp.bfloat16)
            y_start(i, slot, cols)
        y_local(i, slot).start()

        @pl.when(i < eager)
        def _():
            y_mate(i, slot).start()

            @pl.when(i >= 1)
            def _():
                y_forward(i - 1)

    def step(i, carry):
        def attention_kind(kind, inner):
            attention(kind, i)
            return inner

        lax.fori_loop(0, 2, attention_kind, 0)

        @pl.when(lagged & (i >= 1))
        def _():
            finish(i - 1)
        mlp(MATE, i)
        mlp(OWN, i)

        @pl.when(jnp.logical_not(lagged))
        def _():
            finish(i)
        return carry

    lax.fori_loop(0, units, step, 0)

    @pl.when(lagged)
    def _():
        finish(units - 1)

    for i in range(max(units - 2, 0), units):
        y_wait(i, i % 2)

    def late(i, carry):
        y_mate_late(i).start()
        return carry

    def forward(i, carry):
        y_forward(i)
        return carry

    lax.fori_loop(eager, units, late, 0)
    lax.fori_loop(jnp.maximum(eager - 1, 0), units, forward, 0)

    for i in range(max(units - 2, 0), units):
        for kind in range(2):
            for grp in range(2):
                o_copy(kind, i % 2, grp).wait_send()

        @pl.when(has_prev)
        def _():
            wb_copy(i, i % 2).wait_send()
    for idx in range(p_chunks):
        p_copy(0, idx).wait_send()
    for copy in passes:
        copy.wait_send()

    @pl.when(jnp.logical_not(lender) & lends_all)
    def _():
        remote(relay_a, relay_b, hop_sem.at[0], rb_sem.at[0], to_mate).wait_send()
        remote(relay_b, wdn.at[1], hop_sem.at[1], wr_sem.at[7], {"pp": ally}).wait_send()

    @pl.when(jnp.logical_not(lender) & jnp.logical_not(lends_all))
    def _():
        some = pl.ds(0, lend_some * part)
        remote(relay_a.at[some], relay_b.at[some], hop_sem.at[0], rb_sem.at[0], to_mate).wait_send()
        remote(relay_b.at[some], wdn.at[1, some], hop_sem.at[1], wr_sem.at[7], {"pp": ally}).wait_send()

    def late_sent(i, carry):
        y_mate_late(i).wait_send()
        return carry

    lax.fori_loop(eager, units, late_sent, 0)

    def arrived(i, carry):
        by_mate = is_last & (i % 2 == 0)

        @pl.when(by_mate)
        def _():
            y_mate_late(i).wait_recv()

        @pl.when(jnp.logical_not(by_mate))
        def _():
            twin_arrival(i).wait_recv()
        return carry

    lax.fori_loop(0, units, arrived, 0)
    mate_rows = pl.ds(mate * units, units)
    remote(y_hbm.at[mate_rows], y_hbm.at[mate_rows], yf_sem.at[0], yf_sem.at[1], to_twin).wait()


def solution(mesh):
    stages = mesh.shape["pp"]
    weight_specs = (
        P('pp', None), P('pp', None),
        P('pp', None, None, 'tp', None), P('pp', None, 'tp', None),
        P('pp', 'tp', None, None), P('pp', None),
        P('pp', None), P('pp', None),
        P('pp', None, 'tp'), P('pp', 'tp'),
        P('pp', 'tp', None), P('pp', None),
    )
    if mesh.shape["tp"] != 4 or stages % 4:
        raise ValueError("unsupported mesh")

    def local_run(x_micro, ln1_gain, ln1_bias, w_qkv, b_qkv, w_out, b_out, ln2_gain, ln2_bias, w_up, b_up, w_down, b_down):
        micro, rows, seq, d_model = x_micro.shape
        total = micro * rows
        units = total // mesh.shape["tp"]
        _, _, _, heads, head_dim = w_qkv.shape
        group_w = heads * head_dim
        ff = w_up.shape[-1]
        x_seqs = x_micro.reshape(total, seq, d_model)
        w_qkv = jnp.transpose(w_qkv[0], (0, 2, 3, 1)).reshape(3 * group_w, d_model)
        w_out = w_out.reshape(group_w, d_model)
        any_spec = pl.BlockSpec(memory_space=pl.ANY)
        vmem_spec = pl.BlockSpec(memory_space=pltpu.VMEM)
        bf16, dma = jnp.bfloat16, pltpu.SemaphoreType.DMA
        p_chunks = d_model // DOWN_CHUNK
        y_all = pl.pallas_call(
            functools.partial(_pipeline_kernel, stages, head_dim),
            out_shape=jax.ShapeDtypeStruct((total, seq, d_model), bf16),
            in_specs=[any_spec] * 5 + [vmem_spec, any_spec] + [vmem_spec] * 6,
            out_specs=any_spec,
            scratch_shapes=[
                pltpu.VMEM((d_model, 6 * group_w), bf16),
                pltpu.VMEM((4, group_w, d_model), bf16),
                pltpu.VMEM((2, d_model, ff), bf16),
                pltpu.VMEM((2, ff, d_model), bf16),
                pltpu.VMEM((1, 6 * group_w), jnp.float32),
                pltpu.VMEM((2, 1, ff), bf16),
                pltpu.VMEM((2, units, seq, d_model), bf16),
                pltpu.VMEM((seq, d_model), bf16),
                pltpu.VMEM((seq, 6 * group_w), bf16),
                pltpu.VMEM((2, 2, 2, seq, 2 * group_w), bf16),
                pltpu.VMEM((seq, d_model), jnp.float32),
                pltpu.VMEM((seq, d_model), bf16),
                pltpu.VMEM((2, seq, ff), bf16),
                pltpu.VMEM((2, seq, d_model), bf16),
                pltpu.VMEM((2, seq, d_model), bf16),
                pltpu.VMEM((2, seq, d_model), bf16),
                pltpu.VMEM((ff, d_model), bf16),
                pltpu.VMEM((ff, d_model), bf16),
                pltpu.VMEM((2, TURN_ROWS, d_model), bf16),
                dma((2, units)), dma((6,)), dma((10,)), dma((10,)),
                dma((2, 2, 2)), dma((2, 2, 2)), dma((p_chunks,)), dma((2, p_chunks)),
                dma((2,)), dma((2,)), dma((2,)), dma((2,)), dma((units,)), dma((2,)), dma((units,)), dma((units,)),
                dma((2,)), dma((RELAY_STEPS,)), dma((RELAY_STEPS,)), dma((2,)),
            ],
            compiler_params=pltpu.CompilerParams(collective_id=0, has_side_effects=True, vmem_limit_bytes=60 * 1024 * 1024),
            name="stage_pipeline",
        )(x_seqs, w_qkv, w_out, w_up.reshape(d_model, ff), w_down.reshape(ff, d_model), b_qkv, b_up,
          ln1_gain, ln1_bias, b_out, ln2_gain, ln2_bias, b_down)
        return y_all.reshape(1, micro, rows, seq, d_model)

    return jax.shard_map(local_run, mesh=mesh, in_specs=(P(None, 'dp', None, None),) + weight_specs, out_specs=P('pp', None, 'dp', None, None), check_vma=False)
```

```python
import functools

import jax
import jax.numpy as jnp
from jax import lax
from jax.experimental import pallas as pl
from jax.experimental.pallas import tpu as pltpu
from jax.sharding import PartitionSpec as P

LN_EPS = 1e-5
LOG2_E = 1.4426950408889634
MESH = pl.DeviceIdType.MESH
LN_ROWS = 16
UP_CHUNK = 512
DOWN_CHUNK = 512
OUT_CHUNK = 512
RELAY_STEPS = 16
LAGGED_STAGES = 2
RELAY_UNITS = 10
EAGER_UNITS = (0, 0, 2, 12)
TURN_ROWS = 128
COPY_ROWS = 4
COPY_SLOTS = 8


def _f32(val):
    return val.astype(jnp.float32)


def _norm_rows(rows, gain, bias):
    width = rows.shape[-1]
    mean = jnp.sum(rows, axis=-1, keepdims=True) * (1.0 / width)
    cen = rows - mean
    var = jnp.sum(cen * cen, axis=-1, keepdims=True) * (1.0 / width)
    return (cen * lax.rsqrt(var + LN_EPS) * gain + bias).astype(jnp.bfloat16)


def _dot(lhs, rhs):
    return jnp.dot(lhs, rhs, preferred_element_type=jnp.float32)


def _pipeline_kernel(stages, head_dim, x_hbm, wqkv_hbm, wout_hbm, wup_hbm, wdn_hbm, bqkv_in, bup_in,
                     ln1_gain, ln1_bias, b_out, ln2_gain, ln2_bias, b_down,
                     y_hbm,
                     wqkv, wout, wup, wdn, bqkv, bup, xbuf, hbuf, qkv, obuf, acc, x1buf, ubuf, pown, prcv, ybuf,
                     relay_a, relay_b, turn,
                     x_sem, wl_sem, ws_sem, wr_sem, os_sem, or_sem, ps_sem, pr_sem, yl_sem, yn_sem, yd_sem, ym_sem, ymr_sem, yf_sem, yt_sem, yl_late,
                     wb_sem, ra_sem, rb_sem, hop_sem, rya_sem, ryb_sem, ryh_sem):
    _, units, seq, d_model = xbuf.shape
    group_w = wout_hbm.shape[0]
    group_heads = group_w // head_dim
    qk_w = 2 * group_w
    v_col, twin_col = qk_w, qk_w + 2 * group_w
    ff = wup_hbm.shape[1]
    rr = lax.axis_index("tp")
    pp = lax.axis_index("pp")
    odd = pp % 2
    near, far = rr + 1 - 2 * (rr % 2), 3 - rr
    mate = odd * near + (1 - odd) * far
    twin = odd * far + (1 - odd) * near
    has_next = pp + 1 < stages
    has_prev = pp > 0
    lagged = pp >= stages - LAGGED_STAGES
    is_last = pp == stages - 1
    relayed = jnp.where(pp >= stages - stages // 4, min(RELAY_UNITS, units), 0)
    helps = pp < stages // 4
    cross = rr + 2 - 4 * (rr // 2)
    eager = 0
    for quarter, amount in enumerate(EAGER_UNITS):
        eager = eager + jnp.where(pp * len(EAGER_UNITS) // stages == quarter, min(amount, units), 0)
    lender = pp < stages // 2
    ally = stages - 1 - pp
    OWN, MATE = 0, 1

    def local(src, dst, sem):
        return pltpu.make_async_copy(src, dst, sem)

    def remote(src, dst, send, recv, dev):
        return pltpu.make_async_remote_copy(src_ref=src, dst_ref=dst, send_sem=send, recv_sem=recv, device_id=dev, device_id_type=MESH)

    barrier = pltpu.get_barrier_semaphore()

    def greet(dev):
        pl.semaphore_signal(barrier, inc=1, device_id=dev, device_id_type=MESH)

    greet({"tp": mate})
    greet({"tp": twin})
    greet({"pp": ally})

    @pl.when(has_next)
    def _():
        greet({"pp": pp + 1})
        greet({"tp": twin, "pp": pp + 1})

    @pl.when(has_prev)
    def _():
        greet({"pp": pp - 1})
        greet({"tp": mate, "pp": pp - 1})

    own_qk, twin_qk = pl.ds(0, qk_w), pl.ds(twin_col, qk_w)
    own_v, twin_v = pl.ds(v_col, group_w), pl.ds(v_col + group_w, group_w)
    turn_rows = turn.shape[1]
    turns = 3 * group_w // turn_rows

    def turn_load(c, slot):
        return local(wqkv_hbm.at[pl.ds(c * turn_rows, turn_rows)], turn.at[slot], wl_sem.at[slot])

    loads = [
        local(wout_hbm, wout.at[0], wl_sem.at[2]),
        local(wup_hbm, wup.at[0], wl_sem.at[3]),
        local(bup_in, bup.at[0], wl_sem.at[4]),
        local(wdn_hbm, wdn.at[0], wl_sem.at[5]),
    ]
    to_twin, to_mate = {"tp": twin}, {"tp": mate}
    passes = [
        remote(wqkv.at[:, own_qk], wqkv.at[:, twin_qk], ws_sem.at[0], wr_sem.at[0], to_twin),
        remote(bqkv.at[:, own_qk], bqkv.at[:, twin_qk], ws_sem.at[1], wr_sem.at[1], to_twin),
        remote(wout_hbm, wout.at[1], ws_sem.at[2], wr_sem.at[2], to_twin),
        remote(wout_hbm, wout.at[2], ws_sem.at[3], wr_sem.at[3], to_mate),
        remote(wout.at[1], wout.at[3], ws_sem.at[4], wr_sem.at[4], to_mate),
        remote(wup_hbm, wup.at[1], ws_sem.at[5], wr_sem.at[5], to_twin),
        remote(bup_in, bup.at[1], ws_sem.at[6], wr_sem.at[6], to_twin),
        remote(wdn_hbm, wdn.at[1], ws_sem.at[7], wr_sem.at[7], to_twin),
        remote(wqkv.at[:, own_v], wqkv.at[:, twin_v], ws_sem.at[8], wr_sem.at[8], to_twin),
        remote(bqkv.at[:, own_v], bqkv.at[:, twin_v], ws_sem.at[9], wr_sem.at[9], to_twin),
    ]

    def x_load(kind, i, row):
        return local(x_hbm.at[row * units + i], xbuf.at[kind, i], x_sem.at[kind, i])

    turn_load(0, 0).start()
    turn_load(1, 1).start()

    @pl.when(pp == 0)
    def _():
        def start_x(i, carry):
            x_load(OWN, i, rr).start()
            x_load(MATE, i, mate).start()
            return carry
        lax.fori_loop(0, units, start_x, 0)

    for copy in loads:
        copy.start()

    pl.semaphore_wait(barrier, 3 + 2 * (jnp.where(has_next, 1, 0) + jnp.where(has_prev, 1, 0)))

    passes[2].start()

    steps = RELAY_STEPS
    part = ff // steps
    lend_some = max(steps // 4, 1)
    lends_all = (pp < stages // 4) | (pp >= stages - stages // 4)
    lent = jnp.where(lends_all, steps, lend_some)

    def relay_rows(c):
        return pl.ds(c * part, part)

    def hop_in(c):
        return remote(wdn_hbm.at[relay_rows(c)], relay_a.at[relay_rows(c)], ws_sem.at[7], ra_sem.at[c], {"pp": ally})

    def hop_over(c):
        return remote(relay_a.at[relay_rows(c)], relay_b.at[relay_rows(c)], hop_sem.at[0], rb_sem.at[c], to_mate)

    def hop_out(c):
        return remote(relay_b.at[relay_rows(c)], wdn.at[1, relay_rows(c)], hop_sem.at[1], wr_sem.at[7], {"pp": ally})

    def direct(c):
        return remote(wdn_hbm.at[relay_rows(c)], wdn.at[1, relay_rows(c)], ws_sem.at[7], wr_sem.at[7], to_twin)

    @pl.when(lender)
    def _():
        def lend(c, carry):
            hop_in(c).start()
            return carry
        lax.fori_loop(0, lent, lend, 0)
        passes[3].start()
        passes[2].wait_recv()
        passes[4].start()

    def turn_block(c, carry):
        slot = c % 2
        turn_load(c, slot).wait()
        wqkv[:, pl.ds(pl.multiple_of(c * turn_rows, 128), turn_rows)] = turn[slot].T

        @pl.when(c + 2 < turns)
        def _():
            turn_load(c + 2, slot).start()
        return carry

    lax.fori_loop(0, turns, turn_block, 0)
    spread_row = lax.broadcasted_iota(jnp.int32, (head_dim, group_w), 0)
    spread_col = lax.broadcasted_iota(jnp.int32, (head_dim, group_w), 1)
    spread = jnp.zeros((head_dim, group_w), jnp.float32)
    for hd in range(group_heads):
        spread = spread + jnp.where(spread_row + hd * head_dim == spread_col, 1.0, 0.0)
    spread = spread.astype(jnp.bfloat16)
    head_row = lax.broadcasted_iota(jnp.int32, (group_heads, group_w), 0)
    head_lane = lax.broadcasted_iota(jnp.int32, (group_heads, group_w), 1)
    in_head = (head_lane >= head_row * head_dim) & (head_lane < (head_row + 1) * head_dim)
    for third in range(3):
        wide = jnp.where(in_head, _dot(bqkv_in[0, third], spread), 0.0)
        bqkv[:, pl.ds(third * group_w, group_w)] = jnp.sum(wide, axis=0, keepdims=True)
    for idx in (0, 8, 1, 9, 5, 6):
        passes[idx].start()

    @pl.when(lender)
    def _():
        def keep(c, carry):
            direct(c).start()
            return carry
        lax.fori_loop(lent, steps, keep, 0)

    @pl.when(jnp.logical_not(lender))
    def _():
        passes[7].start()

        def relay(c, carry):
            @pl.when(c < lent)
            def _():
                hop_in(c).wait_recv()
                hop_over(c).start()

            @pl.when(c >= 1)
            def _():
                hop_over(c - 1).wait_recv()
                hop_out(c - 1).start()
            return carry
        lax.fori_loop(0, lent + 1, relay, 0)
        passes[3].start()
        passes[2].wait_recv()
        passes[4].start()

    def wait_weights(load_idx, pass_idx):
        for idx in load_idx:
            loads[idx].wait()
        for idx in pass_idx:
            passes[idx].wait_recv()

    row_id = lax.broadcasted_iota(jnp.int32, (seq, seq), 0)
    col_id = lax.broadcasted_iota(jnp.int32, (seq, seq), 1)

    def o_copy(kind, slot, grp):
        cols = pl.ds(grp * group_w, group_w)
        return remote(obuf.at[slot, kind, 0, :, cols], obuf.at[slot, 1 - kind, 1, :, cols],
                      os_sem.at[slot, kind, grp], or_sem.at[slot, 1 - kind, grp], to_mate)

    def p_copy(slot, idx):
        cols = pl.ds(idx * DOWN_CHUNK, DOWN_CHUNK)
        return remote(pown.at[MATE, :, cols], prcv.at[slot, :, cols], ps_sem.at[idx], pr_sem.at[slot, idx], to_mate)

    p_chunks = d_model // DOWN_CHUNK
    all_cols = pl.ds(0, d_model)

    def y_local(i, slot):
        return local(ybuf.at[slot], y_hbm.at[rr * units + i], yl_sem.at[slot])

    def y_next(i, slot, cols):
        return remote(ybuf.at[slot, :, cols], xbuf.at[OWN, i, :, cols], yn_sem.at[slot], x_sem.at[OWN, i], {"pp": pp + 1})

    def y_diag(i, slot, cols):
        return remote(ybuf.at[slot, :, cols], xbuf.at[MATE, i, :, cols], yd_sem.at[slot], x_sem.at[MATE, i], {"tp": twin, "pp": pp + 1})

    def y_twin(i, slot, cols):
        return remote(ybuf.at[slot, :, cols], y_hbm.at[rr * units + i, :, cols], yd_sem.at[slot], yt_sem.at[i], to_twin)

    def y_mate(i, slot):
        return remote(ybuf.at[slot], y_hbm.at[rr * units + i], ym_sem.at[slot], ymr_sem.at[i], to_mate)

    def y_mate_late(i):
        ref = y_hbm.at[rr * units + i]
        return remote(ref, ref, yl_late.at[i], ymr_sem.at[i], to_mate)

    def y_forward_mate(i):
        ref = y_hbm.at[mate * units + i]
        return remote(ref, ref, yf_sem.at[0], yf_sem.at[1], to_twin)

    def y_forward_twin(i):
        ref = y_hbm.at[twin * units + i]
        return remote(ref, ref, yf_sem.at[0], yf_sem.at[1], to_mate)

    def twin_arrival(i):
        ref = y_hbm.at[twin * units + i]
        return remote(ref, ref, yd_sem.at[0], yt_sem.at[i], to_twin)

    def y_hop_in(i):
        return remote(y_hbm.at[mate * units + i], relay_a.at[pl.ds(i * seq, seq)], yf_sem.at[0], rya_sem.at[i], {"pp": ally})

    def y_hop_over(i):
        rows = pl.ds(i * seq, seq)
        return remote(relay_a.at[rows], relay_b.at[rows], ryh_sem.at[0], ryb_sem.at[i], to_mate)

    def y_hop_out(i):
        return remote(relay_b.at[pl.ds(i * seq, seq)], y_hbm.at[cross * units + i], ryh_sem.at[1], yf_sem.at[1], {"pp": ally})

    def by_mate(i):
        return is_last & (i % 2 == 0) & (i >= relayed)

    def y_forward(i):
        @pl.when(by_mate(i))
        def _():
            twin_arrival(i).wait_recv()
            y_forward_twin(i).start()

        @pl.when(jnp.logical_not(by_mate(i)))
        def _():
            y_mate_late(i).wait_recv()

            @pl.when(i < relayed)
            def _():
                y_hop_in(i).start()

            @pl.when(i >= relayed)
            def _():
                y_forward_mate(i).start()

    def y_start(i, slot, cols):
        @pl.when(has_next)
        def _():
            y_next(i, slot, cols).start()
            y_diag(i, slot, cols).start()

        @pl.when(jnp.logical_not(has_next))
        def _():
            y_twin(i, slot, cols).start()

    def y_wait(i, slot):
        y_local(i, slot).wait()

        @pl.when(has_next)
        def _():
            y_next(i, slot, all_cols).wait_send()
            y_diag(i, slot, all_cols).wait_send()

        @pl.when(jnp.logical_not(has_next))
        def _():
            y_twin(i, slot, all_cols).wait_send()

        @pl.when(i < eager)
        def _():
            y_mate(i, slot).wait_send()

    def wb_copy(i, slot):
        return remote(xbuf.at[MATE, i], y_hbm.at[mate * units + i], wb_sem.at[slot], yt_sem.at[i], {"pp": pp - 1})

    def attention(kind, i):
        slot = i % 2
        x_load(kind, i, rr).wait()

        @pl.when((kind == MATE) & has_prev)
        def _():
            @pl.when(i >= 2)
            def _():
                wb_copy(i - 2, slot).wait_send()
            wb_copy(i, slot).start()

        @pl.when((kind == OWN) & (i == 0))
        def _():
            wait_weights((), (0, 1, 8, 9))

        @pl.when(i >= 2)
        def _():
            for grp in range(2):
                o_copy(kind, slot, grp).wait_send()

        gain, bias = _f32(ln1_gain[...]), _f32(ln1_bias[...])
        for r0 in range(0, seq, LN_ROWS):
            rows = pl.ds(r0, LN_ROWS)
            hbuf[rows, :] = _norm_rows(_f32(xbuf[kind, i, rows, :]), gain, bias)

        lane_head = lax.broadcasted_iota(jnp.int32, (seq, group_w), 1)
        masks = [(lane_head >= hd * head_dim) & (lane_head < (hd + 1) * head_dim) for hd in range(group_heads)]
        causal = row_id >= col_id

        def project(col):
            cols = pl.ds(col, qk_w)
            qkv[:, cols] = (_dot(hbuf[...], wqkv[:, cols]) + bqkv[:, cols]).astype(jnp.bfloat16)

        def by_head(act):
            zero = jnp.zeros_like(act)
            return jnp.concatenate([jnp.where(m, act, zero) for m in masks], axis=0)

        def scores_of(grp):
            q_heads = by_head(qkv[:, pl.ds(grp * twin_col, group_w)])
            key = qkv[:, pl.ds(grp * twin_col + group_w, group_w)]
            return lax.dot_general(q_heads, key, (((1,), (1,)), ((), ())), preferred_element_type=jnp.float32)

        def probs_of(scores):
            probs = []
            for hd in range(group_heads):
                sc = jnp.where(causal, scores[hd * seq:(hd + 1) * seq], -1e30)
                ex = jnp.exp2((sc - jnp.max(sc, axis=-1, keepdims=True)) * (head_dim ** -0.5 * LOG2_E))
                probs.append((ex * (1.0 / jnp.sum(ex, axis=-1, keepdims=True))).astype(jnp.bfloat16))
            return jnp.concatenate(probs, axis=1)

        def send_heads(grp, probs):
            val = qkv[:, pl.ds(v_col + grp * group_w, group_w)]
            obuf[slot, kind, 0, :, pl.ds(grp * group_w, group_w)] = _dot(probs, by_head(val)).astype(jnp.bfloat16)
            o_copy(kind, slot, grp).start()

        project(0)
        scores_0 = scores_of(0)
        project(twin_col)
        probs_0 = probs_of(scores_0)
        scores_1 = scores_of(1)
        project(v_col)
        send_heads(0, probs_0)
        send_heads(1, probs_of(scores_1))

    def mlp(kind, i):
        slot = i % 2
        if kind == MATE:
            @pl.when(i == 0)
            def _():
                wait_weights((0,), (3, 4))

        def out_part(half, cols, kind=kind):
            return _dot(obuf[slot, kind, half], jnp.concatenate([wout[2 * half, :, cols], wout[2 * half + 1, :, cols]], axis=0))

        if kind == MATE:
            for both in (MATE, OWN):
                for c0 in range(0, d_model, OUT_CHUNK):
                    cols = pl.ds(c0, OUT_CHUNK)
                    acc[both, :, cols] = out_part(0, cols, both)
        for grp in range(2):
            o_copy(1 - kind, slot, grp).wait_recv()
        for c0 in range(0, d_model, OUT_CHUNK):
            cols = pl.ds(c0, OUT_CHUNK)
            att = ((acc[kind, :, cols] + out_part(1, cols)) + _f32(b_out[:, cols])).astype(jnp.bfloat16)
            x1buf[:, cols] = (_f32(xbuf[kind, i, :, cols]) + _f32(att)).astype(jnp.bfloat16)

        gain, bias = _f32(ln2_gain[...]), _f32(ln2_bias[...])
        for r0 in range(0, seq, LN_ROWS):
            rows = pl.ds(r0, LN_ROWS)
            hbuf[rows, :] = _norm_rows(_f32(x1buf[rows, :]), gain, bias)

        if kind == MATE:
            @pl.when(i == 0)
            def _():
                wait_weights((1, 2), (5, 6))

        for grp in range(2):
            for c0 in range(0, ff, UP_CHUNK):
                cols = pl.ds(c0, UP_CHUNK)
                pre = _dot(hbuf[...], wup[grp, :, cols]) + _f32(bup[grp, :, cols])
                ubuf[grp, :, cols] = jax.nn.gelu(pre, approximate=True).astype(jnp.bfloat16)

        if kind == MATE:
            @pl.when(i == 0)
            def _():
                wait_weights((3,), (7,))

            @pl.when(i >= 1)
            def _():
                for idx in range(p_chunks):
                    p_copy(slot, idx).wait_send()

        for idx in range(p_chunks):
            cols = pl.ds(idx * DOWN_CHUNK, DOWN_CHUNK)
            pown[kind, :, cols] = (_dot(ubuf[0], wdn[0, :, cols]) + _dot(ubuf[1], wdn[1, :, cols])).astype(jnp.bfloat16)
            if kind == MATE:
                p_copy(slot, idx).start()

    def finish(i):
        slot = i % 2

        @pl.when(i >= 2)
        def _():
            y_wait(i - 2, slot)

        for idx in range(p_chunks):
            cols = pl.ds(idx * DOWN_CHUNK, DOWN_CHUNK)
            p_copy(slot, idx).wait_recv()
            both = (_f32(pown[OWN, :, cols]) + _f32(prcv[slot, :, cols])) + _f32(b_down[:, cols])
            ybuf[slot, :, cols] = (_f32(x1buf[:, cols]) + _f32(both.astype(jnp.bfloat16))).astype(jnp.bfloat16)
            y_start(i, slot, cols)
        y_local(i, slot).start()

        @pl.when(i < eager)
        def _():
            y_mate(i, slot).start()

            @pl.when(i >= 1)
            def _():
                y_forward(i - 1)

    def step(i, carry):
        def attention_kind(kind, inner):
            attention(kind, i)
            return inner

        lax.fori_loop(0, 2, attention_kind, 0)

        @pl.when(lagged & (i >= 1))
        def _():
            finish(i - 1)
        mlp(MATE, i)
        mlp(OWN, i)

        @pl.when(jnp.logical_not(lagged))
        def _():
            finish(i)
        return carry

    lax.fori_loop(0, units, step, 0)

    @pl.when(lagged)
    def _():
        finish(units - 1)

    for i in range(max(units - 2, 0), units):
        y_wait(i, i % 2)

    def late(i, carry):
        y_mate_late(i).start()
        return carry

    def forward(i, carry):
        y_forward(i)
        return carry

    lax.fori_loop(eager, units, late, 0)
    lax.fori_loop(jnp.maximum(eager - 1, 0), units, forward, 0)

    helped = min(RELAY_UNITS, units)

    @pl.when(helps)
    def _():
        def pass_on(i, carry):
            @pl.when(i < helped)
            def _():
                y_hop_in(i).wait_recv()
                y_hop_over(i).start()

            @pl.when(i >= 1)
            def _():
                y_hop_over(i - 1).wait_recv()
                y_hop_out(i - 1).start()
            return carry

        lax.fori_loop(0, helped + 1, pass_on, 0)
        rows = pl.ds(0, helped * seq)
        remote(relay_a.at[rows], relay_b.at[rows], ryh_sem.at[0], ryb_sem.at[0], to_mate).wait_send()
        remote(relay_b.at[rows], relay_a.at[rows], ryh_sem.at[1], yf_sem.at[1], {"pp": ally}).wait_send()

    for i in range(max(units - 2, 0), units):
        for kind in range(2):
            for grp in range(2):
                o_copy(kind, i % 2, grp).wait_send()

        @pl.when(has_prev)
        def _():
            wb_copy(i, i % 2).wait_send()
    for idx in range(p_chunks):
        p_copy(0, idx).wait_send()
    for copy in passes:
        copy.wait_send()

    @pl.when(jnp.logical_not(lender) & lends_all)
    def _():
        remote(relay_a, relay_b, hop_sem.at[0], rb_sem.at[0], to_mate).wait_send()
        remote(relay_b, wdn.at[1], hop_sem.at[1], wr_sem.at[7], {"pp": ally}).wait_send()

    @pl.when(jnp.logical_not(lender) & jnp.logical_not(lends_all))
    def _():
        some = pl.ds(0, lend_some * part)
        remote(relay_a.at[some], relay_b.at[some], hop_sem.at[0], rb_sem.at[0], to_mate).wait_send()
        remote(relay_b.at[some], wdn.at[1, some], hop_sem.at[1], wr_sem.at[7], {"pp": ally}).wait_send()

    def late_sent(i, carry):
        y_mate_late(i).wait_send()
        return carry

    lax.fori_loop(eager, units, late_sent, 0)

    def arrived(i, carry):
        @pl.when(by_mate(i))
        def _():
            y_mate_late(i).wait_recv()

        @pl.when(jnp.logical_not(by_mate(i)))
        def _():
            twin_arrival(i).wait_recv()
        return carry

    lax.fori_loop(0, units, arrived, 0)
    mate_rows = pl.ds(mate * units, units)
    remote(y_hbm.at[mate_rows], y_hbm.at[mate_rows], yf_sem.at[0], yf_sem.at[1], to_twin).wait()


def _copy_kernel(src, dst, buf, in_sem, out_sem):
    slots, rows = buf.shape[:2]
    blocks = src.shape[0] // rows

    def load(c):
        return pltpu.make_async_copy(src.at[pl.ds(c * rows, rows)], buf.at[c % slots], in_sem.at[c % slots])

    def store(c):
        return pltpu.make_async_copy(buf.at[c % slots], dst.at[pl.ds(c * rows, rows)], out_sem.at[c % slots])

    for c in range(min(slots, blocks)):
        load(c).start()
    for c in range(blocks):
        load(c).wait()
        store(c).start()
        if c >= 1 and c - 1 + slots < blocks:
            store(c - 1).wait()
            load(c - 1 + slots).start()
    for c in range(max(blocks - slots, 0), blocks):
        store(c).wait()


def solution(mesh):
    stages = mesh.shape["pp"]
    weight_specs = (
        P('pp', None), P('pp', None),
        P('pp', None, None, 'tp', None), P('pp', None, 'tp', None),
        P('pp', 'tp', None, None), P('pp', None),
        P('pp', None), P('pp', None),
        P('pp', None, 'tp'), P('pp', 'tp'),
        P('pp', 'tp', None), P('pp', None),
    )
    if mesh.shape["tp"] != 4 or stages % 4:
        raise ValueError("unsupported mesh")

    def local_run(x_micro, ln1_gain, ln1_bias, w_qkv, b_qkv, w_out, b_out, ln2_gain, ln2_bias, w_up, b_up, w_down, b_down):
        micro, rows, seq, d_model = x_micro.shape
        total = micro * rows
        units = total // mesh.shape["tp"]
        _, _, _, heads, head_dim = w_qkv.shape
        group_w = heads * head_dim
        ff = w_up.shape[-1]
        x_seqs = x_micro.reshape(total, seq, d_model)
        w_qkv = jnp.transpose(w_qkv[0], (0, 2, 3, 1)).reshape(3 * group_w, d_model)
        w_out = w_out.reshape(group_w, d_model)
        any_spec = pl.BlockSpec(memory_space=pl.ANY)
        vmem_spec = pl.BlockSpec(memory_space=pltpu.VMEM)
        bf16, dma = jnp.bfloat16, pltpu.SemaphoreType.DMA
        p_chunks = d_model // DOWN_CHUNK
        y_all = pl.pallas_call(
            functools.partial(_pipeline_kernel, stages, head_dim),
            out_shape=jax.ShapeDtypeStruct((total, seq, d_model), bf16),
            in_specs=[any_spec] * 5 + [vmem_spec, any_spec] + [vmem_spec] * 6,
            out_specs=any_spec,
            scratch_shapes=[
                pltpu.VMEM((d_model, 6 * group_w), bf16),
                pltpu.VMEM((4, group_w, d_model), bf16),
                pltpu.VMEM((2, d_model, ff), bf16),
                pltpu.VMEM((2, ff, d_model), bf16),
                pltpu.VMEM((1, 6 * group_w), jnp.float32),
                pltpu.VMEM((2, 1, ff), bf16),
                pltpu.VMEM((2, units, seq, d_model), bf16),
                pltpu.VMEM((seq, d_model), bf16),
                pltpu.VMEM((seq, 6 * group_w), bf16),
                pltpu.VMEM((2, 2, 2, seq, 2 * group_w), bf16),
                pltpu.VMEM((2, seq, d_model), jnp.float32),
                pltpu.VMEM((seq, d_model), bf16),
                pltpu.VMEM((2, seq, ff), bf16),
                pltpu.VMEM((2, seq, d_model), bf16),
                pltpu.VMEM((2, seq, d_model), bf16),
                pltpu.VMEM((2, seq, d_model), bf16),
                pltpu.VMEM((ff, d_model), bf16),
                pltpu.VMEM((ff, d_model), bf16),
                pltpu.VMEM((2, TURN_ROWS, d_model), bf16),
                dma((2, units)), dma((6,)), dma((10,)), dma((10,)),
                dma((2, 2, 2)), dma((2, 2, 2)), dma((p_chunks,)), dma((2, p_chunks)),
                dma((2,)), dma((2,)), dma((2,)), dma((2,)), dma((units,)), dma((2,)), dma((units,)), dma((units,)),
                dma((2,)), dma((RELAY_STEPS,)), dma((RELAY_STEPS,)), dma((2,)),
                dma((units,)), dma((units,)), dma((2,)),
            ],
            compiler_params=pltpu.CompilerParams(collective_id=0, has_side_effects=True, vmem_limit_bytes=60 * 1024 * 1024),
            name="stage_pipeline",
        )(x_seqs, w_qkv, w_out, w_up.reshape(d_model, ff), w_down.reshape(ff, d_model), b_qkv, b_up,
          ln1_gain, ln1_bias, b_out, ln2_gain, ln2_bias, b_down)
        block_rows = max(d for d in range(1, COPY_ROWS + 1) if total % d == 0)
        y_all = pl.pallas_call(
            _copy_kernel,
            out_shape=jax.ShapeDtypeStruct((total, seq, d_model), bf16),
            in_specs=[any_spec],
            out_specs=any_spec,
            scratch_shapes=[pltpu.VMEM((COPY_SLOTS, block_rows, seq, d_model), bf16), dma((COPY_SLOTS,)), dma((COPY_SLOTS,))],
            compiler_params=pltpu.CompilerParams(vmem_limit_bytes=56 * 1024 * 1024),
            name="result_copy",
        )(y_all)
        return y_all.reshape(1, micro, rows, seq, d_model)

    return jax.shard_map(local_run, mesh=mesh, in_specs=(P(None, 'dp', None, None),) + weight_specs, out_specs=P('pp', None, 'dp', None, None), check_vma=False)
```

```python
import functools

import jax
import jax.numpy as jnp
from jax import lax
from jax.experimental import pallas as pl
from jax.experimental.pallas import tpu as pltpu
from jax.sharding import PartitionSpec as P

LN_EPS = 1e-5
LOG2_E = 1.4426950408889634
MESH = pl.DeviceIdType.MESH
LN_ROWS = 16
UP_CHUNK = 512
DOWN_CHUNK = 512
OUT_CHUNK = 512
RELAY_STEPS = 16
LAGGED_STAGES = 2
LAG_PLACES = (1, 1)
COPY_PLACES = (0, 0)
RELAY_UNITS = (0, 0, 0, 10)
EAGER_UNITS = (0, 0, 2, 12)
TURN_ROWS = 128
COPY_ROWS = 1
COPY_SLOTS = 32


def _f32(val):
    return val.astype(jnp.float32)


def _norm_rows(rows, gain, bias):
    width = rows.shape[-1]
    mean = jnp.sum(rows, axis=-1, keepdims=True) * (1.0 / width)
    cen = rows - mean
    var = jnp.sum(cen * cen, axis=-1, keepdims=True) * (1.0 / width)
    return (cen * lax.rsqrt(var + LN_EPS) * gain + bias).astype(jnp.bfloat16)


def _dot(lhs, rhs):
    return jnp.dot(lhs, rhs, preferred_element_type=jnp.float32)


def _pipeline_kernel(stages, head_dim, x_hbm, wqkv_hbm, wout_hbm, wup_hbm, wdn_hbm, bqkv_hbm, bup_in,
                     ln1_gain_hbm, ln1_bias_hbm, b_out_hbm, ln2_gain_hbm, ln2_bias_hbm, b_down_hbm,
                     y_hbm,
                     wqkv, wout, wup, wdn, bqkv, bup, xbuf, hbuf, qkv, obuf, acc, x1buf, ubuf, pown, prcv, ybuf,
                     relay_a, relay_b, turn,
                     x_sem, wl_sem, ws_sem, wr_sem, os_sem, or_sem, ps_sem, pr_sem, yl_sem, yn_sem, yd_sem, ym_sem, ymr_sem, yf_sem, yt_sem, yl_late,
                     wb_sem, ra_sem, rb_sem, hop_sem, rya_sem, ryb_sem, ryh_sem,
                     bqkv_in, ln1_gain, ln1_bias, b_out, ln2_gain, ln2_bias, b_down, small_sem):
    _, units, seq, d_model = xbuf.shape
    group_w = wout_hbm.shape[0]
    group_heads = group_w // head_dim
    qk_w = 2 * group_w
    v_col, twin_col = qk_w, qk_w + 2 * group_w
    ff = wup_hbm.shape[1]
    rr = lax.axis_index("tp")
    pp = lax.axis_index("pp")
    odd = pp % 2
    near, far = rr + 1 - 2 * (rr % 2), 3 - rr
    mate = odd * near + (1 - odd) * far
    twin = odd * far + (1 - odd) * near
    has_next = pp + 1 < stages
    has_prev = pp > 0
    lagged = pp >= stages - LAGGED_STAGES
    is_last = pp == stages - 1
    copy_place = jnp.where(is_last, COPY_PLACES[1], COPY_PLACES[0])
    lag_place = jnp.where(is_last, LAG_PLACES[1], LAG_PLACES[0])
    cross = rr + 2 - 4 * (rr // 2)
    quarter = pp * 4 // stages

    def by_quarter(amounts, at):
        return sum(jnp.where(at == idx, min(amount, units), 0) for idx, amount in enumerate(amounts))

    eager = by_quarter(EAGER_UNITS, quarter)
    relayed = by_quarter(RELAY_UNITS, quarter)
    helped = by_quarter(RELAY_UNITS, 3 - quarter)
    lender = pp < stages // 2
    ally = stages - 1 - pp
    OWN, MATE = 0, 1

    def local(src, dst, sem):
        return pltpu.make_async_copy(src, dst, sem)

    def remote(src, dst, send, recv, dev):
        return pltpu.make_async_remote_copy(src_ref=src, dst_ref=dst, send_sem=send, recv_sem=recv, device_id=dev, device_id_type=MESH)

    barrier = pltpu.get_barrier_semaphore()

    def greet(dev):
        pl.semaphore_signal(barrier, inc=1, device_id=dev, device_id_type=MESH)

    greet({"tp": mate})
    greet({"tp": twin})
    greet({"pp": ally})

    @pl.when(has_next)
    def _():
        greet({"pp": pp + 1})
        greet({"tp": twin, "pp": pp + 1})

    @pl.when(has_prev)
    def _():
        greet({"pp": pp - 1})
        greet({"tp": mate, "pp": pp - 1})

    own_qk, twin_qk = pl.ds(0, qk_w), pl.ds(twin_col, qk_w)
    own_v, twin_v = pl.ds(v_col, group_w), pl.ds(v_col + group_w, group_w)
    turn_rows = turn.shape[1]
    turns = 3 * group_w // turn_rows

    def turn_load(c, slot):
        return local(wqkv_hbm.at[pl.ds(c * turn_rows, turn_rows)], turn.at[slot], wl_sem.at[slot])

    loads = [
        local(wout_hbm, wout.at[0], wl_sem.at[2]),
        local(wup_hbm, wup.at[0], wl_sem.at[3]),
        local(bup_in, bup.at[0], wl_sem.at[4]),
        local(wdn_hbm, wdn.at[0], wl_sem.at[5]),
    ]
    to_twin, to_mate = {"tp": twin}, {"tp": mate}
    passes = [
        remote(wqkv.at[:, own_qk], wqkv.at[:, twin_qk], ws_sem.at[0], wr_sem.at[0], to_twin),
        remote(bqkv.at[:, own_qk], bqkv.at[:, twin_qk], ws_sem.at[1], wr_sem.at[1], to_twin),
        remote(wout_hbm, wout.at[1], ws_sem.at[2], wr_sem.at[2], to_twin),
        remote(wout_hbm, wout.at[2], ws_sem.at[3], wr_sem.at[3], to_mate),
        remote(wout.at[1], wout.at[3], ws_sem.at[4], wr_sem.at[4], to_mate),
        remote(wup_hbm, wup.at[1], ws_sem.at[5], wr_sem.at[5], to_twin),
        remote(bup_in, bup.at[1], ws_sem.at[6], wr_sem.at[6], to_twin),
        remote(wdn_hbm, wdn.at[1], ws_sem.at[7], wr_sem.at[7], to_twin),
        remote(wqkv.at[:, own_v], wqkv.at[:, twin_v], ws_sem.at[8], wr_sem.at[8], to_twin),
        remote(bqkv.at[:, own_v], bqkv.at[:, twin_v], ws_sem.at[9], wr_sem.at[9], to_twin),
    ]

    def x_load(kind, i, row):
        return local(x_hbm.at[row * units + i], xbuf.at[kind, i], x_sem.at[kind, i])

    small = [
        local(src, dst, small_sem.at[idx])
        for idx, (src, dst) in enumerate([
            (bqkv_hbm, bqkv_in), (ln1_gain_hbm, ln1_gain), (ln1_bias_hbm, ln1_bias), (b_out_hbm, b_out),
            (ln2_gain_hbm, ln2_gain), (ln2_bias_hbm, ln2_bias), (b_down_hbm, b_down)])
    ]
    for copy in small:
        copy.start()
    turn_load(0, 0).start()
    turn_load(1, 1).start()

    @pl.when(pp == 0)
    def _():
        def start_x(i, carry):
            x_load(OWN, i, rr).start()
            x_load(MATE, i, mate).start()
            return carry
        lax.fori_loop(0, units, start_x, 0)

    for copy in loads:
        copy.start()

    pl.semaphore_wait(barrier, 3 + 2 * (jnp.where(has_next, 1, 0) + jnp.where(has_prev, 1, 0)))

    passes[2].start()

    steps = RELAY_STEPS
    part = ff // steps
    lend_some = max(steps // 4, 1)
    lends_all = (pp < stages // 4) | (pp >= stages - stages // 4)
    lent = jnp.where(lends_all, steps, lend_some)

    def relay_rows(c):
        return pl.ds(c * part, part)

    def hop_in(c):
        return remote(wdn_hbm.at[relay_rows(c)], relay_a.at[relay_rows(c)], ws_sem.at[7], ra_sem.at[c], {"pp": ally})

    def hop_over(c):
        return remote(relay_a.at[relay_rows(c)], relay_b.at[relay_rows(c)], hop_sem.at[0], rb_sem.at[c], to_mate)

    def hop_out(c):
        return remote(relay_b.at[relay_rows(c)], wdn.at[1, relay_rows(c)], hop_sem.at[1], wr_sem.at[7], {"pp": ally})

    def direct(c):
        return remote(wdn_hbm.at[relay_rows(c)], wdn.at[1, relay_rows(c)], ws_sem.at[7], wr_sem.at[7], to_twin)

    @pl.when(lender)
    def _():
        def lend(c, carry):
            hop_in(c).start()
            return carry
        lax.fori_loop(0, lent, lend, 0)
        passes[3].start()
        passes[2].wait_recv()
        passes[4].start()

    def turn_block(c, carry):
        slot = c % 2
        turn_load(c, slot).wait()
        wqkv[:, pl.ds(pl.multiple_of(c * turn_rows, 128), turn_rows)] = turn[slot].T

        @pl.when(c + 2 < turns)
        def _():
            turn_load(c + 2, slot).start()
        return carry

    lax.fori_loop(0, turns, turn_block, 0)
    for copy in small:
        copy.wait()
    spread_row = lax.broadcasted_iota(jnp.int32, (head_dim, group_w), 0)
    spread_col = lax.broadcasted_iota(jnp.int32, (head_dim, group_w), 1)
    spread = jnp.zeros((head_dim, group_w), jnp.float32)
    for hd in range(group_heads):
        spread = spread + jnp.where(spread_row + hd * head_dim == spread_col, 1.0, 0.0)
    spread = spread.astype(jnp.bfloat16)
    head_row = lax.broadcasted_iota(jnp.int32, (group_heads, group_w), 0)
    head_lane = lax.broadcasted_iota(jnp.int32, (group_heads, group_w), 1)
    in_head = (head_lane >= head_row * head_dim) & (head_lane < (head_row + 1) * head_dim)
    for third in range(3):
        wide = jnp.where(in_head, _dot(bqkv_in[0, third], spread), 0.0)
        bqkv[:, pl.ds(third * group_w, group_w)] = jnp.sum(wide, axis=0, keepdims=True)
    for idx in (0, 8, 1, 9, 5, 6):
        passes[idx].start()

    @pl.when(lender)
    def _():
        def keep(c, carry):
            direct(c).start()
            return carry
        lax.fori_loop(lent, steps, keep, 0)

    @pl.when(jnp.logical_not(lender))
    def _():
        passes[7].start()

        def relay(c, carry):
            @pl.when(c < lent)
            def _():
                hop_in(c).wait_recv()
                hop_over(c).start()

            @pl.when(c >= 1)
            def _():
                hop_over(c - 1).wait_recv()
                hop_out(c - 1).start()
            return carry
        lax.fori_loop(0, lent + 1, relay, 0)
        passes[3].start()
        passes[2].wait_recv()
        passes[4].start()

    def wait_weights(load_idx, pass_idx):
        for idx in load_idx:
            loads[idx].wait()
        for idx in pass_idx:
            passes[idx].wait_recv()

    row_id = lax.broadcasted_iota(jnp.int32, (seq, seq), 0)
    col_id = lax.broadcasted_iota(jnp.int32, (seq, seq), 1)

    def o_copy(kind, slot, grp):
        cols = pl.ds(grp * group_w, group_w)
        return remote(obuf.at[slot, kind, 0, :, cols], obuf.at[slot, 1 - kind, 1, :, cols],
                      os_sem.at[slot, kind, grp], or_sem.at[slot, 1 - kind, grp], to_mate)

    def p_copy(slot, idx):
        cols = pl.ds(idx * DOWN_CHUNK, DOWN_CHUNK)
        return remote(pown.at[MATE, :, cols], prcv.at[slot, :, cols], ps_sem.at[idx], pr_sem.at[slot, idx], to_mate)

    p_chunks = d_model // DOWN_CHUNK
    all_cols = pl.ds(0, d_model)

    def y_local(i, slot):
        return local(ybuf.at[slot], y_hbm.at[rr * units + i], yl_sem.at[slot])

    def y_next(i, slot, cols):
        return remote(ybuf.at[slot, :, cols], xbuf.at[OWN, i, :, cols], yn_sem.at[slot], x_sem.at[OWN, i], {"pp": pp + 1})

    def y_diag(i, slot, cols):
        return remote(ybuf.at[slot, :, cols], xbuf.at[MATE, i, :, cols], yd_sem.at[slot], x_sem.at[MATE, i], {"tp": twin, "pp": pp + 1})

    def y_twin(i, slot, cols):
        return remote(ybuf.at[slot, :, cols], y_hbm.at[rr * units + i, :, cols], yd_sem.at[slot], yt_sem.at[i], to_twin)

    def y_mate(i, slot):
        return remote(ybuf.at[slot], y_hbm.at[rr * units + i], ym_sem.at[slot], ymr_sem.at[i], to_mate)

    def y_mate_late(i):
        ref = y_hbm.at[rr * units + i]
        return remote(ref, ref, yl_late.at[i], ymr_sem.at[i], to_mate)

    def y_forward_mate(i):
        ref = y_hbm.at[mate * units + i]
        return remote(ref, ref, yf_sem.at[0], yf_sem.at[1], to_twin)

    def y_forward_twin(i):
        ref = y_hbm.at[twin * units + i]
        return remote(ref, ref, yf_sem.at[0], yf_sem.at[1], to_mate)

    def twin_arrival(i):
        ref = y_hbm.at[twin * units + i]
        return remote(ref, ref, yd_sem.at[0], yt_sem.at[i], to_twin)

    def y_hop_in(i):
        return remote(y_hbm.at[mate * units + i], relay_a.at[pl.ds(i * seq, seq)], yf_sem.at[0], rya_sem.at[i], {"pp": ally})

    def y_hop_over(i):
        rows = pl.ds(i * seq, seq)
        return remote(relay_a.at[rows], relay_b.at[rows], ryh_sem.at[0], ryb_sem.at[i], to_mate)

    def y_hop_out(i):
        return remote(relay_b.at[pl.ds(i * seq, seq)], y_hbm.at[cross * units + i], ryh_sem.at[1], yf_sem.at[1], {"pp": ally})

    def by_mate(i):
        return is_last & (i % 2 == 0) & (i >= relayed)

    def y_forward(i):
        @pl.when(by_mate(i))
        def _():
            twin_arrival(i).wait_recv()
            y_forward_twin(i).start()

        @pl.when(jnp.logical_not(by_mate(i)))
        def _():
            y_mate_late(i).wait_recv()

            @pl.when(i < relayed)
            def _():
                y_hop_in(i).start()

            @pl.when(i >= relayed)
            def _():
                y_forward_mate(i).start()

    def y_start(i, slot, cols):
        @pl.when(has_next)
        def _():
            y_next(i, slot, cols).start()
            y_diag(i, slot, cols).start()

        @pl.when(jnp.logical_not(has_next))
        def _():
            y_twin(i, slot, cols).start()

    def y_wait(i, slot):
        y_local(i, slot).wait()

        @pl.when(has_next)
        def _():
            y_next(i, slot, all_cols).wait_send()
            y_diag(i, slot, all_cols).wait_send()

        @pl.when(jnp.logical_not(has_next))
        def _():
            y_twin(i, slot, all_cols).wait_send()

        @pl.when(i < eager)
        def _():
            y_mate(i, slot).wait_send()

    def wb_copy(i, slot):
        return remote(xbuf.at[MATE, i], y_hbm.at[mate * units + i], wb_sem.at[slot], yt_sem.at[i], {"pp": pp - 1})

    def attention(kind, i):
        slot = i % 2
        x_load(kind, i, rr).wait()

        @pl.when((kind == MATE) & has_prev)
        def _():
            @pl.when(i >= 2)
            def _():
                wb_copy(i - 2, slot).wait_send()
            wb_copy(i, slot).start()

        @pl.when((kind == OWN) & (i == 0))
        def _():
            wait_weights((), (0, 1, 8, 9))

        @pl.when(i >= 2)
        def _():
            for grp in range(2):
                o_copy(kind, slot, grp).wait_send()

        gain, bias = _f32(ln1_gain[...]), _f32(ln1_bias[...])
        for r0 in range(0, seq, LN_ROWS):
            rows = pl.ds(r0, LN_ROWS)
            hbuf[rows, :] = _norm_rows(_f32(xbuf[kind, i, rows, :]), gain, bias)

        lane_head = lax.broadcasted_iota(jnp.int32, (seq, group_w), 1)
        masks = [(lane_head >= hd * head_dim) & (lane_head < (hd + 1) * head_dim) for hd in range(group_heads)]
        causal = row_id <= col_id

        def project(col):
            cols = pl.ds(col, qk_w)
            qkv[:, cols] = (_dot(hbuf[...], wqkv[:, cols]) + bqkv[:, cols]).astype(jnp.bfloat16)

        def by_head(act):
            zero = jnp.zeros_like(act)
            return jnp.concatenate([jnp.where(m, act, zero) for m in masks], axis=0)

        def scores_of(grp):
            q_heads = by_head(qkv[:, pl.ds(grp * twin_col, group_w)])
            key = qkv[:, pl.ds(grp * twin_col + group_w, group_w)]
            return lax.dot_general(key, q_heads, (((1,), (1,)), ((), ())), preferred_element_type=jnp.float32)

        def probs_of(scores):
            probs = []
            for hd in range(group_heads):
                sc = jnp.where(causal, scores[:, hd * seq:(hd + 1) * seq], -1e30)
                ex = jnp.exp2((sc - jnp.max(sc, axis=0, keepdims=True)) * (head_dim ** -0.5 * LOG2_E))
                probs.append((ex * (1.0 / jnp.sum(ex, axis=0, keepdims=True))).astype(jnp.bfloat16).T)
            return jnp.concatenate(probs, axis=1)

        def send_heads(grp, probs):
            val = qkv[:, pl.ds(v_col + grp * group_w, group_w)]
            obuf[slot, kind, 0, :, pl.ds(grp * group_w, group_w)] = _dot(probs, by_head(val)).astype(jnp.bfloat16)
            o_copy(kind, slot, grp).start()

        project(0)
        scores_0 = scores_of(0)
        project(v_col)
        send_heads(0, probs_of(scores_0))
        project(twin_col)
        send_heads(1, probs_of(scores_of(1)))

    def mlp(kind, i):
        slot = i % 2
        if kind == MATE:
            @pl.when(i == 0)
            def _():
                wait_weights((0,), (3, 4))

        def out_part(half, cols, kind=kind):
            return _dot(obuf[slot, kind, half], jnp.concatenate([wout[2 * half, :, cols], wout[2 * half + 1, :, cols]], axis=0))

        if kind == MATE:
            for both in (MATE, OWN):
                for c0 in range(0, d_model, OUT_CHUNK):
                    cols = pl.ds(c0, OUT_CHUNK)
                    acc[both, :, cols] = out_part(0, cols, both)
        for grp in range(2):
            o_copy(1 - kind, slot, grp).wait_recv()
        for c0 in range(0, d_model, OUT_CHUNK):
            cols = pl.ds(c0, OUT_CHUNK)
            att = ((acc[kind, :, cols] + out_part(1, cols)) + _f32(b_out[:, cols])).astype(jnp.bfloat16)
            x1buf[kind, :, cols] = (_f32(xbuf[kind, i, :, cols]) + _f32(att)).astype(jnp.bfloat16)

        gain, bias = _f32(ln2_gain[...]), _f32(ln2_bias[...])
        for r0 in range(0, seq, LN_ROWS):
            rows = pl.ds(r0, LN_ROWS)
            hbuf[rows, :] = _norm_rows(_f32(x1buf[kind, rows, :]), gain, bias)

        if kind == MATE:
            @pl.when(i == 0)
            def _():
                wait_weights((1, 2), (5, 6))

        for grp in range(2):
            for c0 in range(0, ff, UP_CHUNK):
                cols = pl.ds(c0, UP_CHUNK)
                pre = _dot(hbuf[...], wup[grp, :, cols]) + _f32(bup[grp, :, cols])
                ubuf[grp, :, cols] = jax.nn.gelu(pre, approximate=True).astype(jnp.bfloat16)

        if kind == MATE:
            @pl.when(i == 0)
            def _():
                wait_weights((3,), (7,))

            @pl.when(i >= 1)
            def _():
                for idx in range(p_chunks):
                    p_copy(slot, idx).wait_send()

        for idx in range(p_chunks):
            cols = pl.ds(idx * DOWN_CHUNK, DOWN_CHUNK)
            pown[kind, :, cols] = (_dot(ubuf[0], wdn[0, :, cols]) + _dot(ubuf[1], wdn[1, :, cols])).astype(jnp.bfloat16)
            if kind == MATE:
                p_copy(slot, idx).start()

    def finish(i):
        slot = i % 2

        @pl.when(i >= 2)
        def _():
            y_wait(i - 2, slot)

        for idx in range(p_chunks):
            cols = pl.ds(idx * DOWN_CHUNK, DOWN_CHUNK)
            p_copy(slot, idx).wait_recv()
            both = (_f32(pown[OWN, :, cols]) + _f32(prcv[slot, :, cols])) + _f32(b_down[:, cols])
            ybuf[slot, :, cols] = (_f32(x1buf[OWN, :, cols]) + _f32(both.astype(jnp.bfloat16))).astype(jnp.bfloat16)
            y_start(i, slot, cols)
        y_local(i, slot).start()

    def replicate(i):
        @pl.when(i < eager)
        def _():
            y_mate(i, i % 2).start()

            @pl.when(i >= 1)
            def _():
                y_forward(i - 1)

    def step(i, carry):
        def finish_before(place):
            @pl.when(lagged & (i >= 1) & (lag_place == place))
            def _():
                finish(i - 1)

        def attention_kind(kind, inner):
            attention(kind, i)

            @pl.when(kind == OWN)
            def _():
                finish_before(0)
            return inner

        lax.fori_loop(0, 2, attention_kind, 0)
        finish_before(1)

        @pl.when(lagged & (i >= 1) & (copy_place == 0))
        def _():
            replicate(i - 1)
        mlp(MATE, i)

        @pl.when(lagged & (i >= 1) & (copy_place == 1))
        def _():
            replicate(i - 1)
        mlp(OWN, i)

        @pl.when(lagged & (i >= 1) & (copy_place == 2))
        def _():
            replicate(i - 1)

        @pl.when(jnp.logical_not(lagged))
        def _():
            finish(i)
            replicate(i)
        return carry

    lax.fori_loop(0, units, step, 0)

    @pl.when(lagged)
    def _():
        finish(units - 1)
        replicate(units - 1)

    for i in range(max(units - 2, 0), units):
        y_wait(i, i % 2)

    def late(i, carry):
        y_mate_late(i).start()
        return carry

    def forward(i, carry):
        y_forward(i)
        return carry

    lax.fori_loop(eager, units, late, 0)
    lax.fori_loop(jnp.maximum(eager - 1, 0), units, forward, 0)

    @pl.when(helped > 0)
    def _():
        def pass_on(i, carry):
            @pl.when(i < helped)
            def _():
                y_hop_in(i).wait_recv()
                y_hop_over(i).start()

            @pl.when(i >= 1)
            def _():
                y_hop_over(i - 1).wait_recv()
                y_hop_out(i - 1).start()
            return carry

        lax.fori_loop(0, helped + 1, pass_on, 0)

    for idx, amount in enumerate(RELAY_UNITS):
        if amount:
            @pl.when(3 - quarter == idx)
            def _(amount=amount):
                rows = pl.ds(0, min(amount, units) * seq)
                remote(relay_a.at[rows], relay_b.at[rows], ryh_sem.at[0], ryb_sem.at[0], to_mate).wait_send()
                remote(relay_b.at[rows], relay_a.at[rows], ryh_sem.at[1], yf_sem.at[1], {"pp": ally}).wait_send()

    for i in range(max(units - 2, 0), units):
        for kind in range(2):
            for grp in range(2):
                o_copy(kind, i % 2, grp).wait_send()

        @pl.when(has_prev)
        def _():
            wb_copy(i, i % 2).wait_send()
    for idx in range(p_chunks):
        p_copy(0, idx).wait_send()
    for copy in passes:
        copy.wait_send()

    @pl.when(jnp.logical_not(lender) & lends_all)
    def _():
        remote(relay_a, relay_b, hop_sem.at[0], rb_sem.at[0], to_mate).wait_send()
        remote(relay_b, wdn.at[1], hop_sem.at[1], wr_sem.at[7], {"pp": ally}).wait_send()

    @pl.when(jnp.logical_not(lender) & jnp.logical_not(lends_all))
    def _():
        some = pl.ds(0, lend_some * part)
        remote(relay_a.at[some], relay_b.at[some], hop_sem.at[0], rb_sem.at[0], to_mate).wait_send()
        remote(relay_b.at[some], wdn.at[1, some], hop_sem.at[1], wr_sem.at[7], {"pp": ally}).wait_send()

    def late_sent(i, carry):
        y_mate_late(i).wait_send()
        return carry

    lax.fori_loop(eager, units, late_sent, 0)

    def arrived(i, carry):
        @pl.when(by_mate(i))
        def _():
            y_mate_late(i).wait_recv()

        @pl.when(jnp.logical_not(by_mate(i)))
        def _():
            twin_arrival(i).wait_recv()
        return carry

    lax.fori_loop(0, units, arrived, 0)
    mate_rows = pl.ds(mate * units, units)
    remote(y_hbm.at[mate_rows], y_hbm.at[mate_rows], yf_sem.at[0], yf_sem.at[1], to_twin).wait()


def _copy_kernel(src, dst, buf, in_sem, out_sem):
    slots, rows = buf.shape[:2]
    blocks = src.shape[0] // rows

    def load(c):
        return pltpu.make_async_copy(src.at[pl.ds(c * rows, rows)], buf.at[c % slots], in_sem.at[c % slots])

    def store(c):
        return pltpu.make_async_copy(buf.at[c % slots], dst.at[pl.ds(c * rows, rows)], out_sem.at[c % slots])

    for c in range(min(slots, blocks)):
        load(c).start()
    for c in range(blocks):
        load(c).wait()
        store(c).start()
        if c >= 1 and c - 1 + slots < blocks:
            store(c - 1).wait()
            load(c - 1 + slots).start()
    for c in range(max(blocks - slots, 0), blocks):
        store(c).wait()


def solution(mesh):
    stages = mesh.shape["pp"]
    weight_specs = (
        P('pp', None), P('pp', None),
        P('pp', None, None, 'tp', None), P('pp', None, 'tp', None),
        P('pp', 'tp', None, None), P('pp', None),
        P('pp', None), P('pp', None),
        P('pp', None, 'tp'), P('pp', 'tp'),
        P('pp', 'tp', None), P('pp', None),
    )
    if mesh.shape["tp"] != 4 or stages % 4:
        raise ValueError("unsupported mesh")

    def local_run(x_micro, ln1_gain, ln1_bias, w_qkv, b_qkv, w_out, b_out, ln2_gain, ln2_bias, w_up, b_up, w_down, b_down):
        micro, rows, seq, d_model = x_micro.shape
        total = micro * rows
        units = total // mesh.shape["tp"]
        _, _, _, heads, head_dim = w_qkv.shape
        group_w = heads * head_dim
        ff = w_up.shape[-1]
        x_seqs = x_micro.reshape(total, seq, d_model)
        w_qkv = jnp.transpose(w_qkv[0], (0, 2, 3, 1)).reshape(3 * group_w, d_model)
        w_out = w_out.reshape(group_w, d_model)
        any_spec = pl.BlockSpec(memory_space=pl.ANY)
        bf16, dma = jnp.bfloat16, pltpu.SemaphoreType.DMA
        p_chunks = d_model // DOWN_CHUNK
        y_all = pl.pallas_call(
            functools.partial(_pipeline_kernel, stages, head_dim),
            out_shape=jax.ShapeDtypeStruct((total, seq, d_model), bf16),
            in_specs=[any_spec] * 13,
            out_specs=any_spec,
            scratch_shapes=[
                pltpu.VMEM((d_model, 6 * group_w), bf16),
                pltpu.VMEM((4, group_w, d_model), bf16),
                pltpu.VMEM((2, d_model, ff), bf16),
                pltpu.VMEM((2, ff, d_model), bf16),
                pltpu.VMEM((1, 6 * group_w), jnp.float32),
                pltpu.VMEM((2, 1, ff), bf16),
                pltpu.VMEM((2, units, seq, d_model), bf16),
                pltpu.VMEM((seq, d_model), bf16),
                pltpu.VMEM((seq, 6 * group_w), bf16),
                pltpu.VMEM((2, 2, 2, seq, 2 * group_w), bf16),
                pltpu.VMEM((2, seq, d_model), jnp.float32),
                pltpu.VMEM((2, seq, d_model), bf16),
                pltpu.VMEM((2, seq, ff), bf16),
                pltpu.VMEM((2, seq, d_model), bf16),
                pltpu.VMEM((2, seq, d_model), bf16),
                pltpu.VMEM((2, seq, d_model), bf16),
                pltpu.VMEM((ff, d_model), bf16),
                pltpu.VMEM((ff, d_model), bf16),
                pltpu.VMEM((2, TURN_ROWS, d_model), bf16),
                dma((2, units)), dma((6,)), dma((10,)), dma((10,)),
                dma((2, 2, 2)), dma((2, 2, 2)), dma((p_chunks,)), dma((2, p_chunks)),
                dma((2,)), dma((2,)), dma((2,)), dma((2,)), dma((units,)), dma((2,)), dma((units,)), dma((units,)),
                dma((2,)), dma((RELAY_STEPS,)), dma((RELAY_STEPS,)), dma((2,)),
                dma((units,)), dma((units,)), dma((2,)),
                pltpu.VMEM(b_qkv.shape, bf16), *[pltpu.VMEM((1, d_model), bf16) for _ in range(6)], dma((7,)),
            ],
            compiler_params=pltpu.CompilerParams(collective_id=0, has_side_effects=True, vmem_limit_bytes=60 * 1024 * 1024),
            name="stage_pipeline",
        )(x_seqs, w_qkv, w_out, w_up.reshape(d_model, ff), w_down.reshape(ff, d_model), b_qkv, b_up,
          ln1_gain, ln1_bias, b_out, ln2_gain, ln2_bias, b_down)
        block_rows = max(d for d in range(1, COPY_ROWS + 1) if total % d == 0)
        y_all = pl.pallas_call(
            _copy_kernel,
            out_shape=jax.ShapeDtypeStruct((total, seq, d_model), bf16),
            in_specs=[any_spec],
            out_specs=any_spec,
            scratch_shapes=[pltpu.VMEM((COPY_SLOTS, block_rows, seq, d_model), bf16), dma((COPY_SLOTS,)), dma((COPY_SLOTS,))],
            compiler_params=pltpu.CompilerParams(vmem_limit_bytes=56 * 1024 * 1024),
            name="result_copy",
        )(y_all)
        return y_all.reshape(1, micro, rows, seq, d_model)

    return jax.shard_map(local_run, mesh=mesh, in_specs=(P(None, 'dp', None, None),) + weight_specs, out_specs=P('pp', None, 'dp', None, None), check_vma=False)
```

```python
import functools

import jax
import jax.numpy as jnp
from jax import lax
from jax.experimental import pallas as pl
from jax.experimental.pallas import tpu as pltpu
from jax.sharding import PartitionSpec as P

LN_EPS = 1e-5
LOG2_E = 1.4426950408889634
MESH = pl.DeviceIdType.MESH
LN_ROWS = 16
UP_CHUNK = 512
DOWN_CHUNK = 512
OUT_CHUNK = 512
RELAY_STEPS = 16
LAGGED_STAGES = 2
LAG_PLACES = (1, 1)
COPY_PLACES = (0, 0)
RELAY_UNITS = (0, 0, 0, 10)
EAGER_UNITS = (0, 0, 2, 12)
TURN_ROWS = 128
COPY_ROWS = 1
COPY_SLOTS = 32


def _f32(val):
    return val.astype(jnp.float32)


def _norm_rows(rows, gain, bias):
    width = rows.shape[-1]
    mean = jnp.sum(rows, axis=-1, keepdims=True) * (1.0 / width)
    cen = rows - mean
    var = jnp.sum(cen * cen, axis=-1, keepdims=True) * (1.0 / width)
    return (cen * lax.rsqrt(var + LN_EPS) * gain + bias).astype(jnp.bfloat16)


def _dot(lhs, rhs):
    return jnp.dot(lhs, rhs, preferred_element_type=jnp.float32)


def _pipeline_kernel(stages, head_dim, x_hbm, wqkv_hbm, wout_hbm, wup_hbm, wdn_hbm, bqkv_hbm, bup_in,
                     ln1_gain_hbm, ln1_bias_hbm, b_out_hbm, ln2_gain_hbm, ln2_bias_hbm, b_down_hbm,
                     y_hbm,
                     wqkv, wout, wup, wdn, bqkv, bup, xbuf, hbuf, qkv, obuf, acc, x1buf, ubuf, pown, prcv, ybuf,
                     relay_a, relay_b, turn,
                     x_sem, wl_sem, ws_sem, wr_sem, os_sem, or_sem, ps_sem, pr_sem, yl_sem, yn_sem, yd_sem, ym_sem, ymr_sem, yf_sem, yt_sem, yl_late,
                     wb_sem, ra_sem, rb_sem, hop_sem, rya_sem, ryb_sem, ryh_sem, xo_sem,
                     bqkv_in, ln1_gain, ln1_bias, b_out, ln2_gain, ln2_bias, b_down, small_sem):
    _, units, seq, d_model = xbuf.shape
    group_w = wout_hbm.shape[0]
    group_heads = group_w // head_dim
    qk_w = 2 * group_w
    v_col, twin_col = qk_w, qk_w + 2 * group_w
    ff = wup_hbm.shape[1]
    rr = lax.axis_index("tp")
    pp = lax.axis_index("pp")
    odd = pp % 2
    near, far = rr + 1 - 2 * (rr % 2), 3 - rr
    mate = odd * near + (1 - odd) * far
    twin = odd * far + (1 - odd) * near
    has_next = pp + 1 < stages
    has_prev = pp > 0
    lagged = pp >= stages - LAGGED_STAGES
    is_last = pp == stages - 1
    hands_over = (odd == 1) & has_next
    copy_place = jnp.where(is_last, COPY_PLACES[1], COPY_PLACES[0])
    lag_place = jnp.where(is_last, LAG_PLACES[1], LAG_PLACES[0])
    cross = rr + 2 - 4 * (rr // 2)
    quarter = pp * 4 // stages

    def by_quarter(amounts, at):
        return sum(jnp.where(at == idx, min(amount, units), 0) for idx, amount in enumerate(amounts))

    eager = by_quarter(EAGER_UNITS, quarter)
    relayed = by_quarter(RELAY_UNITS, quarter)
    helped = by_quarter(RELAY_UNITS, 3 - quarter)
    lender = pp < stages // 2
    ally = stages - 1 - pp
    OWN, MATE = 0, 1

    def local(src, dst, sem):
        return pltpu.make_async_copy(src, dst, sem)

    def remote(src, dst, send, recv, dev):
        return pltpu.make_async_remote_copy(src_ref=src, dst_ref=dst, send_sem=send, recv_sem=recv, device_id=dev, device_id_type=MESH)

    barrier = pltpu.get_barrier_semaphore()

    def greet(dev):
        pl.semaphore_signal(barrier, inc=1, device_id=dev, device_id_type=MESH)

    greet({"tp": mate})
    greet({"tp": twin})
    greet({"pp": ally})

    @pl.when(has_next)
    def _():
        greet({"pp": pp + 1})
        greet({"tp": twin, "pp": pp + 1})

    @pl.when(has_prev)
    def _():
        greet({"pp": pp - 1})
        greet({"tp": mate, "pp": pp - 1})

    own_qk, twin_qk = pl.ds(0, qk_w), pl.ds(twin_col, qk_w)
    own_v, twin_v = pl.ds(v_col, group_w), pl.ds(v_col + group_w, group_w)
    turn_rows = turn.shape[1]
    turns = 3 * group_w // turn_rows

    def turn_load(c, slot):
        return local(wqkv_hbm.at[pl.ds(c * turn_rows, turn_rows)], turn.at[slot], wl_sem.at[slot])

    loads = [
        local(wout_hbm, wout.at[0], wl_sem.at[2]),
        local(wup_hbm, wup.at[0], wl_sem.at[3]),
        local(bup_in, bup.at[0], wl_sem.at[4]),
        local(wdn_hbm, wdn.at[0], wl_sem.at[5]),
    ]
    to_twin, to_mate = {"tp": twin}, {"tp": mate}
    passes = [
        remote(wqkv.at[:, own_qk], wqkv.at[:, twin_qk], ws_sem.at[0], wr_sem.at[0], to_twin),
        remote(bqkv.at[:, own_qk], bqkv.at[:, twin_qk], ws_sem.at[1], wr_sem.at[1], to_twin),
        remote(wout_hbm, wout.at[1], ws_sem.at[2], wr_sem.at[2], to_twin),
        remote(wout_hbm, wout.at[2], ws_sem.at[3], wr_sem.at[3], to_mate),
        remote(wout.at[1], wout.at[3], ws_sem.at[4], wr_sem.at[4], to_mate),
        remote(wup_hbm, wup.at[1], ws_sem.at[5], wr_sem.at[5], to_twin),
        remote(bup_in, bup.at[1], ws_sem.at[6], wr_sem.at[6], to_twin),
        remote(wdn_hbm, wdn.at[1], ws_sem.at[7], wr_sem.at[7], to_twin),
        remote(wqkv.at[:, own_v], wqkv.at[:, twin_v], ws_sem.at[8], wr_sem.at[8], to_twin),
        remote(bqkv.at[:, own_v], bqkv.at[:, twin_v], ws_sem.at[9], wr_sem.at[9], to_twin),
    ]

    def x_load(kind, i, row):
        return local(x_hbm.at[row * units + i], xbuf.at[kind, i], x_sem.at[kind, i])

    small = [
        local(src, dst, small_sem.at[idx])
        for idx, (src, dst) in enumerate([
            (bqkv_hbm, bqkv_in), (ln1_gain_hbm, ln1_gain), (ln1_bias_hbm, ln1_bias), (b_out_hbm, b_out),
            (ln2_gain_hbm, ln2_gain), (ln2_bias_hbm, ln2_bias), (b_down_hbm, b_down)])
    ]
    for copy in small:
        copy.start()
    turn_load(0, 0).start()
    turn_load(1, 1).start()

    @pl.when(pp == 0)
    def _():
        def start_x(i, carry):
            x_load(OWN, i, rr).start()
            x_load(MATE, i, mate).start()
            return carry
        lax.fori_loop(0, units, start_x, 0)

    for copy in loads:
        copy.start()

    pl.semaphore_wait(barrier, 3 + 2 * (jnp.where(has_next, 1, 0) + jnp.where(has_prev, 1, 0)))

    passes[2].start()

    steps = RELAY_STEPS
    part = ff // steps
    lend_some = max(steps // 4, 1)
    lends_all = (pp < stages // 4) | (pp >= stages - stages // 4)
    lent = jnp.where(lends_all, steps, lend_some)

    def relay_rows(c):
        return pl.ds(c * part, part)

    def hop_in(c):
        return remote(wdn_hbm.at[relay_rows(c)], relay_a.at[relay_rows(c)], ws_sem.at[7], ra_sem.at[c], {"pp": ally})

    def hop_over(c):
        return remote(relay_a.at[relay_rows(c)], relay_b.at[relay_rows(c)], hop_sem.at[0], rb_sem.at[c], to_mate)

    def hop_out(c):
        return remote(relay_b.at[relay_rows(c)], wdn.at[1, relay_rows(c)], hop_sem.at[1], wr_sem.at[7], {"pp": ally})

    def direct(c):
        return remote(wdn_hbm.at[relay_rows(c)], wdn.at[1, relay_rows(c)], ws_sem.at[7], wr_sem.at[7], to_twin)

    @pl.when(lender)
    def _():
        def lend(c, carry):
            hop_in(c).start()
            return carry
        lax.fori_loop(0, lent, lend, 0)
        passes[3].start()
        passes[2].wait_recv()
        passes[4].start()

    def turn_block(c, carry):
        slot = c % 2
        turn_load(c, slot).wait()
        wqkv[:, pl.ds(pl.multiple_of(c * turn_rows, 128), turn_rows)] = turn[slot].T

        @pl.when(c + 2 < turns)
        def _():
            turn_load(c + 2, slot).start()
        return carry

    lax.fori_loop(0, turns, turn_block, 0)
    for copy in small:
        copy.wait()
    spread_row = lax.broadcasted_iota(jnp.int32, (head_dim, group_w), 0)
    spread_col = lax.broadcasted_iota(jnp.int32, (head_dim, group_w), 1)
    spread = jnp.zeros((head_dim, group_w), jnp.float32)
    for hd in range(group_heads):
        spread = spread + jnp.where(spread_row + hd * head_dim == spread_col, 1.0, 0.0)
    spread = spread.astype(jnp.bfloat16)
    head_row = lax.broadcasted_iota(jnp.int32, (group_heads, group_w), 0)
    head_lane = lax.broadcasted_iota(jnp.int32, (group_heads, group_w), 1)
    in_head = (head_lane >= head_row * head_dim) & (head_lane < (head_row + 1) * head_dim)
    for third in range(3):
        wide = jnp.where(in_head, _dot(bqkv_in[0, third], spread), 0.0)
        bqkv[:, pl.ds(third * group_w, group_w)] = jnp.sum(wide, axis=0, keepdims=True)
    for idx in (0, 8, 1, 9, 5, 6):
        passes[idx].start()

    @pl.when(lender)
    def _():
        def keep(c, carry):
            direct(c).start()
            return carry
        lax.fori_loop(lent, steps, keep, 0)

    @pl.when(jnp.logical_not(lender))
    def _():
        passes[7].start()

        def relay(c, carry):
            @pl.when(c < lent)
            def _():
                hop_in(c).wait_recv()
                hop_over(c).start()

            @pl.when(c >= 1)
            def _():
                hop_over(c - 1).wait_recv()
                hop_out(c - 1).start()
            return carry
        lax.fori_loop(0, lent + 1, relay, 0)
        passes[3].start()
        passes[2].wait_recv()
        passes[4].start()

    def wait_weights(load_idx, pass_idx):
        for idx in load_idx:
            loads[idx].wait()
        for idx in pass_idx:
            passes[idx].wait_recv()

    row_id = lax.broadcasted_iota(jnp.int32, (seq, seq), 0)
    col_id = lax.broadcasted_iota(jnp.int32, (seq, seq), 1)

    def o_copy(kind, slot, grp):
        cols = pl.ds(grp * group_w, group_w)
        return remote(obuf.at[slot, kind, 0, :, cols], obuf.at[slot, 1 - kind, 1, :, cols],
                      os_sem.at[slot, kind, grp], or_sem.at[slot, 1 - kind, grp], to_mate)

    def p_copy(slot, idx):
        cols = pl.ds(idx * DOWN_CHUNK, DOWN_CHUNK)
        return remote(pown.at[MATE, :, cols], prcv.at[slot, :, cols], ps_sem.at[idx], pr_sem.at[slot, idx], to_mate)

    p_chunks = d_model // DOWN_CHUNK
    all_cols = pl.ds(0, d_model)

    def y_local(i, slot):
        return local(ybuf.at[slot], y_hbm.at[rr * units + i], yl_sem.at[slot])

    def y_next(i, slot, cols):
        return remote(ybuf.at[slot, :, cols], xbuf.at[OWN, i, :, cols], yn_sem.at[slot], x_sem.at[OWN, i], {"pp": pp + 1})

    def y_diag(i, slot, cols):
        return remote(ybuf.at[slot, :, cols], xbuf.at[MATE, i, :, cols], yd_sem.at[slot], x_sem.at[MATE, i], {"tp": twin, "pp": pp + 1})

    def y_twin(i, slot, cols):
        return remote(ybuf.at[slot, :, cols], y_hbm.at[rr * units + i, :, cols], yd_sem.at[slot], yt_sem.at[i], to_twin)

    def y_mate(i, slot):
        return remote(ybuf.at[slot], y_hbm.at[rr * units + i], ym_sem.at[slot], ymr_sem.at[i], to_mate)

    def y_mate_late(i):
        ref = y_hbm.at[rr * units + i]
        return remote(ref, ref, yl_late.at[i], ymr_sem.at[i], to_mate)

    def y_forward_mate(i):
        ref = y_hbm.at[mate * units + i]
        return remote(ref, ref, yf_sem.at[0], yf_sem.at[1], to_twin)

    def y_forward_twin(i):
        ref = y_hbm.at[twin * units + i]
        return remote(ref, ref, yf_sem.at[0], yf_sem.at[1], to_mate)

    def twin_arrival(i):
        ref = y_hbm.at[twin * units + i]
        return remote(ref, ref, yd_sem.at[0], yt_sem.at[i], to_twin)

    def y_hop_in(i):
        return remote(y_hbm.at[mate * units + i], relay_a.at[pl.ds(i * seq, seq)], yf_sem.at[0], rya_sem.at[i], {"pp": ally})

    def y_hop_over(i):
        rows = pl.ds(i * seq, seq)
        return remote(relay_a.at[rows], relay_b.at[rows], ryh_sem.at[0], ryb_sem.at[i], to_mate)

    def y_hop_out(i):
        return remote(relay_b.at[pl.ds(i * seq, seq)], y_hbm.at[cross * units + i], ryh_sem.at[1], yf_sem.at[1], {"pp": ally})

    def by_mate(i):
        return is_last & (i % 2 == 0) & (i >= relayed)

    def y_forward(i):
        @pl.when(by_mate(i))
        def _():
            twin_arrival(i).wait_recv()
            y_forward_twin(i).start()

        @pl.when(jnp.logical_not(by_mate(i)))
        def _():
            y_mate_late(i).wait_recv()

            @pl.when(i < relayed)
            def _():
                y_hop_in(i).start()

            @pl.when(i >= relayed)
            def _():
                y_forward_mate(i).start()

    def y_start(i, slot, cols):
        @pl.when(has_next)
        def _():
            y_next(i, slot, cols).start()

        @pl.when(odd == 0)
        def _():
            y_diag(i, slot, cols).start()

        @pl.when(odd == 1)
        def _():
            y_twin(i, slot, cols).start()

    def y_wait(i, slot):
        y_local(i, slot).wait()

        @pl.when(has_next)
        def _():
            y_next(i, slot, all_cols).wait_send()

        @pl.when(odd == 0)
        def _():
            y_diag(i, slot, all_cols).wait_send()

        @pl.when(odd == 1)
        def _():
            y_twin(i, slot, all_cols).wait_send()

        @pl.when(i < eager)
        def _():
            y_mate(i, slot).wait_send()

    def x_over(i):
        return remote(y_hbm.at[twin * units + i], xbuf.at[MATE, i], xo_sem.at[i], x_sem.at[MATE, i], {"pp": pp + 1})

    def hand_over(i):
        @pl.when(hands_over)
        def _():
            twin_arrival(i).wait_recv()
            x_over(i).start()

    def wb_copy(i, slot):
        return remote(xbuf.at[MATE, i], y_hbm.at[mate * units + i], wb_sem.at[slot], yt_sem.at[i], {"pp": pp - 1})

    def attention(kind, i):
        slot = i % 2
        x_load(kind, i, rr).wait()

        @pl.when((kind == MATE) & (odd == 1))
        def _():
            @pl.when(i >= 2)
            def _():
                wb_copy(i - 2, slot).wait_send()
            wb_copy(i, slot).start()

        @pl.when((kind == OWN) & (i == 0))
        def _():
            wait_weights((), (0, 1, 8, 9))

        @pl.when(i >= 2)
        def _():
            for grp in range(2):
                o_copy(kind, slot, grp).wait_send()

        gain, bias = _f32(ln1_gain[...]), _f32(ln1_bias[...])
        for r0 in range(0, seq, LN_ROWS):
            rows = pl.ds(r0, LN_ROWS)
            hbuf[rows, :] = _norm_rows(_f32(xbuf[kind, i, rows, :]), gain, bias)

        lane_head = lax.broadcasted_iota(jnp.int32, (seq, group_w), 1)
        masks = [(lane_head >= hd * head_dim) & (lane_head < (hd + 1) * head_dim) for hd in range(group_heads)]
        causal = row_id <= col_id

        def project(col):
            cols = pl.ds(col, qk_w)
            qkv[:, cols] = (_dot(hbuf[...], wqkv[:, cols]) + bqkv[:, cols]).astype(jnp.bfloat16)

        def by_head(act):
            zero = jnp.zeros_like(act)
            return jnp.concatenate([jnp.where(m, act, zero) for m in masks], axis=0)

        def scores_of(grp):
            q_heads = by_head(qkv[:, pl.ds(grp * twin_col, group_w)])
            key = qkv[:, pl.ds(grp * twin_col + group_w, group_w)]
            return lax.dot_general(key, q_heads, (((1,), (1,)), ((), ())), preferred_element_type=jnp.float32)

        def probs_of(scores):
            probs = []
            for hd in range(group_heads):
                sc = jnp.where(causal, scores[:, hd * seq:(hd + 1) * seq], -1e30)
                ex = jnp.exp2((sc - jnp.max(sc, axis=0, keepdims=True)) * (head_dim ** -0.5 * LOG2_E))
                probs.append((ex * (1.0 / jnp.sum(ex, axis=0, keepdims=True))).astype(jnp.bfloat16).T)
            return jnp.concatenate(probs, axis=1)

        def send_heads(grp, probs):
            val = qkv[:, pl.ds(v_col + grp * group_w, group_w)]
            obuf[slot, kind, 0, :, pl.ds(grp * group_w, group_w)] = _dot(probs, by_head(val)).astype(jnp.bfloat16)
            o_copy(kind, slot, grp).start()

        project(0)
        scores_0 = scores_of(0)
        project(v_col)
        send_heads(0, probs_of(scores_0))
        project(twin_col)
        send_heads(1, probs_of(scores_of(1)))

    def mlp(kind, i):
        slot = i % 2
        if kind == MATE:
            @pl.when(i == 0)
            def _():
                wait_weights((0,), (3, 4))

        def out_part(half, cols, kind=kind):
            return _dot(obuf[slot, kind, half], jnp.concatenate([wout[2 * half, :, cols], wout[2 * half + 1, :, cols]], axis=0))

        if kind == MATE:
            for both in (MATE, OWN):
                for c0 in range(0, d_model, OUT_CHUNK):
                    cols = pl.ds(c0, OUT_CHUNK)
                    acc[both, :, cols] = out_part(0, cols, both)
        for grp in range(2):
            o_copy(1 - kind, slot, grp).wait_recv()
        for c0 in range(0, d_model, OUT_CHUNK):
            cols = pl.ds(c0, OUT_CHUNK)
            att = ((acc[kind, :, cols] + out_part(1, cols)) + _f32(b_out[:, cols])).astype(jnp.bfloat16)
            x1buf[kind, :, cols] = (_f32(xbuf[kind, i, :, cols]) + _f32(att)).astype(jnp.bfloat16)

        gain, bias = _f32(ln2_gain[...]), _f32(ln2_bias[...])
        for r0 in range(0, seq, LN_ROWS):
            rows = pl.ds(r0, LN_ROWS)
            hbuf[rows, :] = _norm_rows(_f32(x1buf[kind, rows, :]), gain, bias)

        if kind == MATE:
            @pl.when(i == 0)
            def _():
                wait_weights((1, 2), (5, 6))

        for grp in range(2):
            for c0 in range(0, ff, UP_CHUNK):
                cols = pl.ds(c0, UP_CHUNK)
                pre = _dot(hbuf[...], wup[grp, :, cols]) + _f32(bup[grp, :, cols])
                ubuf[grp, :, cols] = jax.nn.gelu(pre, approximate=True).astype(jnp.bfloat16)

        if kind == MATE:
            @pl.when(i == 0)
            def _():
                wait_weights((3,), (7,))

            @pl.when(i >= 1)
            def _():
                for idx in range(p_chunks):
                    p_copy(slot, idx).wait_send()

        for idx in range(p_chunks):
            cols = pl.ds(idx * DOWN_CHUNK, DOWN_CHUNK)
            pown[kind, :, cols] = (_dot(ubuf[0], wdn[0, :, cols]) + _dot(ubuf[1], wdn[1, :, cols])).astype(jnp.bfloat16)
            if kind == MATE:
                p_copy(slot, idx).start()

    def finish(i):
        slot = i % 2

        @pl.when(i >= 2)
        def _():
            y_wait(i - 2, slot)

        for idx in range(p_chunks):
            cols = pl.ds(idx * DOWN_CHUNK, DOWN_CHUNK)
            p_copy(slot, idx).wait_recv()
            both = (_f32(pown[OWN, :, cols]) + _f32(prcv[slot, :, cols])) + _f32(b_down[:, cols])
            ybuf[slot, :, cols] = (_f32(x1buf[OWN, :, cols]) + _f32(both.astype(jnp.bfloat16))).astype(jnp.bfloat16)
            y_start(i, slot, cols)
        y_local(i, slot).start()

    def replicate(i):
        @pl.when(i < eager)
        def _():
            y_mate(i, i % 2).start()

            @pl.when(i >= 1)
            def _():
                y_forward(i - 1)

    def step(i, carry):
        def finish_before(place):
            @pl.when(lagged & (i >= 1) & (lag_place == place))
            def _():
                finish(i - 1)

        def attention_kind(kind, inner):
            attention(kind, i)

            @pl.when(kind == OWN)
            def _():
                finish_before(0)
            return inner

        lax.fori_loop(0, 2, attention_kind, 0)
        finish_before(1)

        @pl.when(lagged & (i >= 1) & (copy_place == 0))
        def _():
            replicate(i - 1)
        mlp(MATE, i)

        @pl.when(i >= 1)
        def _():
            hand_over(i - 1)

        @pl.when(lagged & (i >= 1) & (copy_place == 1))
        def _():
            replicate(i - 1)
        mlp(OWN, i)

        @pl.when(lagged & (i >= 1) & (copy_place == 2))
        def _():
            replicate(i - 1)

        @pl.when(jnp.logical_not(lagged))
        def _():
            finish(i)
            replicate(i)
        return carry

    lax.fori_loop(0, units, step, 0)

    @pl.when(lagged)
    def _():
        finish(units - 1)
        replicate(units - 1)

    hand_over(units - 1)
    for i in range(max(units - 2, 0), units):
        y_wait(i, i % 2)

    def late(i, carry):
        y_mate_late(i).start()
        return carry

    def forward(i, carry):
        y_forward(i)
        return carry

    lax.fori_loop(eager, units, late, 0)
    lax.fori_loop(jnp.maximum(eager - 1, 0), units, forward, 0)

    @pl.when(helped > 0)
    def _():
        def pass_on(i, carry):
            @pl.when(i < helped)
            def _():
                y_hop_in(i).wait_recv()
                y_hop_over(i).start()

            @pl.when(i >= 1)
            def _():
                y_hop_over(i - 1).wait_recv()
                y_hop_out(i - 1).start()
            return carry

        lax.fori_loop(0, helped + 1, pass_on, 0)

    for idx, amount in enumerate(RELAY_UNITS):
        if amount:
            @pl.when(3 - quarter == idx)
            def _(amount=amount):
                rows = pl.ds(0, min(amount, units) * seq)
                remote(relay_a.at[rows], relay_b.at[rows], ryh_sem.at[0], ryb_sem.at[0], to_mate).wait_send()
                remote(relay_b.at[rows], relay_a.at[rows], ryh_sem.at[1], yf_sem.at[1], {"pp": ally}).wait_send()

    for i in range(max(units - 2, 0), units):
        for kind in range(2):
            for grp in range(2):
                o_copy(kind, i % 2, grp).wait_send()

        @pl.when(odd == 1)
        def _():
            wb_copy(i, i % 2).wait_send()
    for idx in range(p_chunks):
        p_copy(0, idx).wait_send()
    for copy in passes:
        copy.wait_send()

    @pl.when(jnp.logical_not(lender) & lends_all)
    def _():
        remote(relay_a, relay_b, hop_sem.at[0], rb_sem.at[0], to_mate).wait_send()
        remote(relay_b, wdn.at[1], hop_sem.at[1], wr_sem.at[7], {"pp": ally}).wait_send()

    @pl.when(jnp.logical_not(lender) & jnp.logical_not(lends_all))
    def _():
        some = pl.ds(0, lend_some * part)
        remote(relay_a.at[some], relay_b.at[some], hop_sem.at[0], rb_sem.at[0], to_mate).wait_send()
        remote(relay_b.at[some], wdn.at[1, some], hop_sem.at[1], wr_sem.at[7], {"pp": ally}).wait_send()

    def late_sent(i, carry):
        y_mate_late(i).wait_send()
        return carry

    lax.fori_loop(eager, units, late_sent, 0)

    def arrived(i, carry):
        @pl.when(by_mate(i))
        def _():
            y_mate_late(i).wait_recv()

        @pl.when(jnp.logical_not(by_mate(i) | hands_over))
        def _():
            twin_arrival(i).wait_recv()

        @pl.when(hands_over)
        def _():
            x_over(i).wait_send()
        return carry

    lax.fori_loop(0, units, arrived, 0)
    mate_rows = pl.ds(mate * units, units)
    remote(y_hbm.at[mate_rows], y_hbm.at[mate_rows], yf_sem.at[0], yf_sem.at[1], to_twin).wait()


def _copy_kernel(src, dst, buf, in_sem, out_sem):
    slots, rows = buf.shape[:2]
    blocks = src.shape[0] // rows

    def load(c):
        return pltpu.make_async_copy(src.at[pl.ds(c * rows, rows)], buf.at[c % slots], in_sem.at[c % slots])

    def store(c):
        return pltpu.make_async_copy(buf.at[c % slots], dst.at[pl.ds(c * rows, rows)], out_sem.at[c % slots])

    for c in range(min(slots, blocks)):
        load(c).start()
    for c in range(blocks):
        load(c).wait()
        store(c).start()
        if c >= 1 and c - 1 + slots < blocks:
            store(c - 1).wait()
            load(c - 1 + slots).start()
    for c in range(max(blocks - slots, 0), blocks):
        store(c).wait()


def solution(mesh):
    stages = mesh.shape["pp"]
    weight_specs = (
        P('pp', None), P('pp', None),
        P('pp', None, None, 'tp', None), P('pp', None, 'tp', None),
        P('pp', 'tp', None, None), P('pp', None),
        P('pp', None), P('pp', None),
        P('pp', None, 'tp'), P('pp', 'tp'),
        P('pp', 'tp', None), P('pp', None),
    )
    if mesh.shape["tp"] != 4 or stages % 4:
        raise ValueError("unsupported mesh")

    def local_run(x_micro, ln1_gain, ln1_bias, w_qkv, b_qkv, w_out, b_out, ln2_gain, ln2_bias, w_up, b_up, w_down, b_down):
        micro, rows, seq, d_model = x_micro.shape
        total = micro * rows
        units = total // mesh.shape["tp"]
        _, _, _, heads, head_dim = w_qkv.shape
        group_w = heads * head_dim
        ff = w_up.shape[-1]
        x_seqs = x_micro.reshape(total, seq, d_model)
        w_qkv = jnp.transpose(w_qkv[0], (0, 2, 3, 1)).reshape(3 * group_w, d_model)
        w_out = w_out.reshape(group_w, d_model)
        any_spec = pl.BlockSpec(memory_space=pl.ANY)
        bf16, dma = jnp.bfloat16, pltpu.SemaphoreType.DMA
        p_chunks = d_model // DOWN_CHUNK
        y_all = pl.pallas_call(
            functools.partial(_pipeline_kernel, stages, head_dim),
            out_shape=jax.ShapeDtypeStruct((total, seq, d_model), bf16),
            in_specs=[any_spec] * 13,
            out_specs=any_spec,
            scratch_shapes=[
                pltpu.VMEM((d_model, 6 * group_w), bf16),
                pltpu.VMEM((4, group_w, d_model), bf16),
                pltpu.VMEM((2, d_model, ff), bf16),
                pltpu.VMEM((2, ff, d_model), bf16),
                pltpu.VMEM((1, 6 * group_w), jnp.float32),
                pltpu.VMEM((2, 1, ff), bf16),
                pltpu.VMEM((2, units, seq, d_model), bf16),
                pltpu.VMEM((seq, d_model), bf16),
                pltpu.VMEM((seq, 6 * group_w), bf16),
                pltpu.VMEM((2, 2, 2, seq, 2 * group_w), bf16),
                pltpu.VMEM((2, seq, d_model), jnp.float32),
                pltpu.VMEM((2, seq, d_model), bf16),
                pltpu.VMEM((2, seq, ff), bf16),
                pltpu.VMEM((2, seq, d_model), bf16),
                pltpu.VMEM((2, seq, d_model), bf16),
                pltpu.VMEM((2, seq, d_model), bf16),
                pltpu.VMEM((ff, d_model), bf16),
                pltpu.VMEM((ff, d_model), bf16),
                pltpu.VMEM((2, TURN_ROWS, d_model), bf16),
                dma((2, units)), dma((6,)), dma((10,)), dma((10,)),
                dma((2, 2, 2)), dma((2, 2, 2)), dma((p_chunks,)), dma((2, p_chunks)),
                dma((2,)), dma((2,)), dma((2,)), dma((2,)), dma((units,)), dma((2,)), dma((units,)), dma((units,)),
                dma((2,)), dma((RELAY_STEPS,)), dma((RELAY_STEPS,)), dma((2,)),
                dma((units,)), dma((units,)), dma((2,)), dma((units,)),
                pltpu.VMEM(b_qkv.shape, bf16), *[pltpu.VMEM((1, d_model), bf16) for _ in range(6)], dma((7,)),
            ],
            compiler_params=pltpu.CompilerParams(collective_id=0, has_side_effects=True, vmem_limit_bytes=60 * 1024 * 1024),
            name="stage_pipeline",
        )(x_seqs, w_qkv, w_out, w_up.reshape(d_model, ff), w_down.reshape(ff, d_model), b_qkv, b_up,
          ln1_gain, ln1_bias, b_out, ln2_gain, ln2_bias, b_down)
        block_rows = max(d for d in range(1, COPY_ROWS + 1) if total % d == 0)
        y_all = pl.pallas_call(
            _copy_kernel,
            out_shape=jax.ShapeDtypeStruct((total, seq, d_model), bf16),
            in_specs=[any_spec],
            out_specs=any_spec,
            scratch_shapes=[pltpu.VMEM((COPY_SLOTS, block_rows, seq, d_model), bf16), dma((COPY_SLOTS,)), dma((COPY_SLOTS,))],
            compiler_params=pltpu.CompilerParams(vmem_limit_bytes=56 * 1024 * 1024),
            name="result_copy",
        )(y_all)
        return y_all.reshape(1, micro, rows, seq, d_model)

    return jax.shard_map(local_run, mesh=mesh, in_specs=(P(None, 'dp', None, None),) + weight_specs, out_specs=P('pp', None, 'dp', None, None), check_vma=False)
```

```python
import functools

import jax
import jax.numpy as jnp
from jax import lax
from jax.experimental import pallas as pl
from jax.experimental.pallas import tpu as pltpu
from jax.sharding import PartitionSpec as P

LN_EPS = 1e-5
LOG2_E = 1.4426950408889634
MESH = pl.DeviceIdType.MESH
LN_ROWS = 16
UP_CHUNK = 512
DOWN_CHUNK = 512
OUT_CHUNK = 512
RELAY_STEPS = 16
LAGGED_STAGES = 2
LAG_PLACES = (1, 1)
COPY_PLACES = (0, 0)
RELAY_UNITS = (0, 0, 4, 10)
EAGER_UNITS = (0, 0, 3, 12)
TURN_ROWS = 128
COPY_ROWS = 1
COPY_SLOTS = 32


def _f32(val):
    return val.astype(jnp.float32)


def _norm_rows(rows, gain, bias):
    width = rows.shape[-1]
    mean = jnp.sum(rows, axis=-1, keepdims=True) * (1.0 / width)
    cen = rows - mean
    var = jnp.sum(cen * cen, axis=-1, keepdims=True) * (1.0 / width)
    return (cen * lax.rsqrt(var + LN_EPS) * gain + bias).astype(jnp.bfloat16)


def _dot(lhs, rhs):
    return jnp.dot(lhs, rhs, preferred_element_type=jnp.float32)


def _pipeline_kernel(stages, head_dim, x_hbm, wqkv_hbm, wout_hbm, wup_hbm, wdn_hbm, bqkv_hbm, bup_in,
                     ln1_gain_hbm, ln1_bias_hbm, b_out_hbm, ln2_gain_hbm, ln2_bias_hbm, b_down_hbm,
                     y_hbm,
                     wqkv, wout, wup, wdn, bqkv, bup, xbuf, hbuf, qkv, obuf, acc, x1buf, ubuf, pown, prcv, ybuf,
                     relay_a, relay_b, turn,
                     x_sem, wl_sem, ws_sem, wr_sem, os_sem, or_sem, ps_sem, pr_sem, yl_sem, yn_sem, yd_sem, ym_sem, ymr_sem, yf_sem, yt_sem, yl_late,
                     wb_sem, ra_sem, rb_sem, hop_sem, rya_sem, ryb_sem, ryh_sem, xo_sem,
                     bqkv_in, ln1_gain, ln1_bias, b_out, ln2_gain, ln2_bias, b_down, small_sem):
    _, units, seq, d_model = xbuf.shape
    group_w = wout_hbm.shape[0]
    group_heads = group_w // head_dim
    qk_w = 2 * group_w
    v_col, twin_col = qk_w, qk_w + 2 * group_w
    ff = wup_hbm.shape[1]
    rr = lax.axis_index("tp")
    pp = lax.axis_index("pp")
    odd = pp % 2
    near, far = rr + 1 - 2 * (rr % 2), 3 - rr
    mate = odd * near + (1 - odd) * far
    twin = odd * far + (1 - odd) * near
    has_next = pp + 1 < stages
    has_prev = pp > 0
    lagged = pp >= stages - LAGGED_STAGES
    is_last = pp == stages - 1
    hands_over = (odd == 1) & has_next
    copy_place = jnp.where(is_last, COPY_PLACES[1], COPY_PLACES[0])
    lag_place = jnp.where(is_last, LAG_PLACES[1], LAG_PLACES[0])
    cross = rr + 2 - 4 * (rr // 2)
    quarter = pp * 4 // stages

    def by_quarter(amounts, at):
        return sum(jnp.where(at == idx, min(amount, units), 0) for idx, amount in enumerate(amounts))

    eager = by_quarter(EAGER_UNITS, quarter)
    relayed = by_quarter(RELAY_UNITS, quarter)
    helped = by_quarter(RELAY_UNITS, 3 - quarter)
    lender = pp < stages // 2
    ally = stages - 1 - pp
    OWN, MATE = 0, 1

    def local(src, dst, sem):
        return pltpu.make_async_copy(src, dst, sem)

    def remote(src, dst, send, recv, dev):
        return pltpu.make_async_remote_copy(src_ref=src, dst_ref=dst, send_sem=send, recv_sem=recv, device_id=dev, device_id_type=MESH)

    barrier = pltpu.get_barrier_semaphore()

    def greet(dev):
        pl.semaphore_signal(barrier, inc=1, device_id=dev, device_id_type=MESH)

    greet({"tp": mate})
    greet({"tp": twin})
    greet({"pp": ally})

    @pl.when(has_next)
    def _():
        greet({"pp": pp + 1})
        greet({"tp": twin, "pp": pp + 1})

    @pl.when(has_prev)
    def _():
        greet({"pp": pp - 1})
        greet({"tp": mate, "pp": pp - 1})

    own_qk, twin_qk = pl.ds(0, qk_w), pl.ds(twin_col, qk_w)
    own_v, twin_v = pl.ds(v_col, group_w), pl.ds(v_col + group_w, group_w)
    turn_rows = turn.shape[1]
    turns = 3 * group_w // turn_rows

    def turn_load(c, slot):
        return local(wqkv_hbm.at[pl.ds(c * turn_rows, turn_rows)], turn.at[slot], wl_sem.at[slot])

    loads = [
        local(wout_hbm, wout.at[0], wl_sem.at[2]),
        local(wup_hbm, wup.at[0], wl_sem.at[3]),
        local(bup_in, bup.at[0], wl_sem.at[4]),
        local(wdn_hbm, wdn.at[0], wl_sem.at[5]),
    ]
    to_twin, to_mate = {"tp": twin}, {"tp": mate}
    passes = [
        remote(wqkv.at[:, own_qk], wqkv.at[:, twin_qk], ws_sem.at[0], wr_sem.at[0], to_twin),
        remote(bqkv.at[:, own_qk], bqkv.at[:, twin_qk], ws_sem.at[1], wr_sem.at[1], to_twin),
        remote(wout_hbm, wout.at[1], ws_sem.at[2], wr_sem.at[2], to_twin),
        remote(wout_hbm, wout.at[2], ws_sem.at[3], wr_sem.at[3], to_mate),
        remote(wout.at[1], wout.at[3], ws_sem.at[4], wr_sem.at[4], to_mate),
        remote(wup_hbm, wup.at[1], ws_sem.at[5], wr_sem.at[5], to_twin),
        remote(bup_in, bup.at[1], ws_sem.at[6], wr_sem.at[6], to_twin),
        remote(wdn_hbm, wdn.at[1], ws_sem.at[7], wr_sem.at[7], to_twin),
        remote(wqkv.at[:, own_v], wqkv.at[:, twin_v], ws_sem.at[8], wr_sem.at[8], to_twin),
        remote(bqkv.at[:, own_v], bqkv.at[:, twin_v], ws_sem.at[9], wr_sem.at[9], to_twin),
    ]

    def x_load(kind, i, row):
        return local(x_hbm.at[row * units + i], xbuf.at[kind, i], x_sem.at[kind, i])

    small = [
        local(src, dst, small_sem.at[idx])
        for idx, (src, dst) in enumerate([
            (bqkv_hbm, bqkv_in), (ln1_gain_hbm, ln1_gain), (ln1_bias_hbm, ln1_bias), (b_out_hbm, b_out),
            (ln2_gain_hbm, ln2_gain), (ln2_bias_hbm, ln2_bias), (b_down_hbm, b_down)])
    ]
    for copy in small:
        copy.start()
    turn_load(0, 0).start()
    turn_load(1, 1).start()

    @pl.when(pp == 0)
    def _():
        def start_x(i, carry):
            x_load(OWN, i, rr).start()
            x_load(MATE, i, mate).start()
            return carry
        lax.fori_loop(0, units, start_x, 0)

    for copy in loads:
        copy.start()

    pl.semaphore_wait(barrier, 3 + 2 * (jnp.where(has_next, 1, 0) + jnp.where(has_prev, 1, 0)))

    passes[2].start()

    steps = RELAY_STEPS
    part = ff // steps
    lend_some = max(steps // 4, 1)
    lends_all = (pp < stages // 4) | (pp >= stages - stages // 4)
    lent = jnp.where(lends_all, steps, lend_some)

    def relay_rows(c):
        return pl.ds(c * part, part)

    def hop_in(c):
        return remote(wdn_hbm.at[relay_rows(c)], relay_a.at[relay_rows(c)], ws_sem.at[7], ra_sem.at[c], {"pp": ally})

    def hop_over(c):
        return remote(relay_a.at[relay_rows(c)], relay_b.at[relay_rows(c)], hop_sem.at[0], rb_sem.at[c], to_mate)

    def hop_out(c):
        return remote(relay_b.at[relay_rows(c)], wdn.at[1, relay_rows(c)], hop_sem.at[1], wr_sem.at[7], {"pp": ally})

    def direct(c):
        return remote(wdn_hbm.at[relay_rows(c)], wdn.at[1, relay_rows(c)], ws_sem.at[7], wr_sem.at[7], to_twin)

    @pl.when(lender)
    def _():
        def lend(c, carry):
            hop_in(c).start()
            return carry
        lax.fori_loop(0, lent, lend, 0)
        passes[3].start()
        passes[2].wait_recv()
        passes[4].start()

    def turn_block(c, carry):
        slot = c % 2
        turn_load(c, slot).wait()
        wqkv[:, pl.ds(pl.multiple_of(c * turn_rows, 128), turn_rows)] = turn[slot].T

        @pl.when(c + 2 < turns)
        def _():
            turn_load(c + 2, slot).start()
        return carry

    lax.fori_loop(0, turns, turn_block, 0)
    for copy in small:
        copy.wait()
    spread_row = lax.broadcasted_iota(jnp.int32, (head_dim, group_w), 0)
    spread_col = lax.broadcasted_iota(jnp.int32, (head_dim, group_w), 1)
    spread = jnp.zeros((head_dim, group_w), jnp.float32)
    for hd in range(group_heads):
        spread = spread + jnp.where(spread_row + hd * head_dim == spread_col, 1.0, 0.0)
    spread = spread.astype(jnp.bfloat16)
    head_row = lax.broadcasted_iota(jnp.int32, (group_heads, group_w), 0)
    head_lane = lax.broadcasted_iota(jnp.int32, (group_heads, group_w), 1)
    in_head = (head_lane >= head_row * head_dim) & (head_lane < (head_row + 1) * head_dim)
    for third in range(3):
        wide = jnp.where(in_head, _dot(bqkv_in[0, third], spread), 0.0)
        bqkv[:, pl.ds(third * group_w, group_w)] = jnp.sum(wide, axis=0, keepdims=True)
    for idx in (0, 8, 1, 9, 5, 6):
        passes[idx].start()

    @pl.when(lender)
    def _():
        def keep(c, carry):
            direct(c).start()
            return carry
        lax.fori_loop(lent, steps, keep, 0)

    @pl.when(jnp.logical_not(lender))
    def _():
        passes[7].start()

        def relay(c, carry):
            @pl.when(c < lent)
            def _():
                hop_in(c).wait_recv()
                hop_over(c).start()

            @pl.when(c >= 1)
            def _():
                hop_over(c - 1).wait_recv()
                hop_out(c - 1).start()
            return carry
        lax.fori_loop(0, lent + 1, relay, 0)
        passes[3].start()
        passes[2].wait_recv()
        passes[4].start()

    def wait_weights(load_idx, pass_idx):
        for idx in load_idx:
            loads[idx].wait()
        for idx in pass_idx:
            passes[idx].wait_recv()

    row_id = lax.broadcasted_iota(jnp.int32, (seq, seq), 0)
    col_id = lax.broadcasted_iota(jnp.int32, (seq, seq), 1)

    def o_copy(kind, slot, grp):
        cols = pl.ds(grp * group_w, group_w)
        return remote(obuf.at[slot, kind, 0, :, cols], obuf.at[slot, 1 - kind, 1, :, cols],
                      os_sem.at[slot, kind, grp], or_sem.at[slot, 1 - kind, grp], to_mate)

    def p_copy(slot, idx):
        cols = pl.ds(idx * DOWN_CHUNK, DOWN_CHUNK)
        return remote(pown.at[MATE, :, cols], prcv.at[slot, :, cols], ps_sem.at[idx], pr_sem.at[slot, idx], to_mate)

    p_chunks = d_model // DOWN_CHUNK
    all_cols = pl.ds(0, d_model)

    def y_local(i, slot):
        return local(ybuf.at[slot], y_hbm.at[rr * units + i], yl_sem.at[slot])

    def y_next(i, slot, cols):
        return remote(ybuf.at[slot, :, cols], xbuf.at[OWN, i, :, cols], yn_sem.at[slot], x_sem.at[OWN, i], {"pp": pp + 1})

    def y_diag(i, slot, cols):
        return remote(ybuf.at[slot, :, cols], xbuf.at[MATE, i, :, cols], yd_sem.at[slot], x_sem.at[MATE, i], {"tp": twin, "pp": pp + 1})

    def y_twin(i, slot, cols):
        return remote(ybuf.at[slot, :, cols], y_hbm.at[rr * units + i, :, cols], yd_sem.at[slot], yt_sem.at[i], to_twin)

    def y_mate(i, slot):
        return remote(ybuf.at[slot], y_hbm.at[rr * units + i], ym_sem.at[slot], ymr_sem.at[i], to_mate)

    def y_mate_late(i):
        ref = y_hbm.at[rr * units + i]
        return remote(ref, ref, yl_late.at[i], ymr_sem.at[i], to_mate)

    def y_forward_mate(i):
        ref = y_hbm.at[mate * units + i]
        return remote(ref, ref, yf_sem.at[0], yf_sem.at[1], to_twin)

    def y_forward_twin(i):
        ref = y_hbm.at[twin * units + i]
        return remote(ref, ref, yf_sem.at[0], yf_sem.at[1], to_mate)

    def twin_arrival(i):
        ref = y_hbm.at[twin * units + i]
        return remote(ref, ref, yd_sem.at[0], yt_sem.at[i], to_twin)

    def y_hop_in(i):
        return remote(y_hbm.at[mate * units + i], relay_a.at[pl.ds(i * seq, seq)], yf_sem.at[0], rya_sem.at[i], {"pp": ally})

    def y_hop_over(i):
        rows = pl.ds(i * seq, seq)
        return remote(relay_a.at[rows], relay_b.at[rows], ryh_sem.at[0], ryb_sem.at[i], to_mate)

    def y_hop_out(i):
        return remote(relay_b.at[pl.ds(i * seq, seq)], y_hbm.at[cross * units + i], ryh_sem.at[1], yf_sem.at[1], {"pp": ally})

    def by_mate(i):
        return is_last & (i % 2 == 0) & (i >= relayed)

    def y_forward(i):
        @pl.when(by_mate(i))
        def _():
            twin_arrival(i).wait_recv()
            y_forward_twin(i).start()

        @pl.when(jnp.logical_not(by_mate(i)))
        def _():
            y_mate_late(i).wait_recv()

            @pl.when(i < relayed)
            def _():
                y_hop_in(i).start()

            @pl.when(i >= relayed)
            def _():
                y_forward_mate(i).start()

    def y_start(i, slot, cols):
        @pl.when(has_next)
        def _():
            y_next(i, slot, cols).start()

        @pl.when(odd == 0)
        def _():
            y_diag(i, slot, cols).start()

        @pl.when(odd == 1)
        def _():
            y_twin(i, slot, cols).start()

    def y_wait(i, slot):
        y_local(i, slot).wait()

        @pl.when(has_next)
        def _():
            y_next(i, slot, all_cols).wait_send()

        @pl.when(odd == 0)
        def _():
            y_diag(i, slot, all_cols).wait_send()

        @pl.when(odd == 1)
        def _():
            y_twin(i, slot, all_cols).wait_send()

        @pl.when(i < eager)
        def _():
            y_mate(i, slot).wait_send()

    def x_over(i):
        return remote(y_hbm.at[twin * units + i], xbuf.at[MATE, i], xo_sem.at[i], x_sem.at[MATE, i], {"pp": pp + 1})

    def hand_over(i):
        @pl.when(hands_over)
        def _():
            twin_arrival(i).wait_recv()
            x_over(i).start()

    def wb_copy(i, slot):
        return remote(xbuf.at[MATE, i], y_hbm.at[mate * units + i], wb_sem.at[slot], yt_sem.at[i], {"pp": pp - 1})

    def attention(kind, i):
        slot = i % 2
        x_load(kind, i, rr).wait()

        @pl.when((kind == MATE) & (odd == 1))
        def _():
            @pl.when(i >= 2)
            def _():
                wb_copy(i - 2, slot).wait_send()
            wb_copy(i, slot).start()

        @pl.when((kind == OWN) & (i == 0))
        def _():
            wait_weights((), (0, 1, 8, 9))

        @pl.when(i >= 2)
        def _():
            for grp in range(2):
                o_copy(kind, slot, grp).wait_send()

        gain, bias = _f32(ln1_gain[...]), _f32(ln1_bias[...])
        for r0 in range(0, seq, LN_ROWS):
            rows = pl.ds(r0, LN_ROWS)
            hbuf[rows, :] = _norm_rows(_f32(xbuf[kind, i, rows, :]), gain, bias)

        lane_head = lax.broadcasted_iota(jnp.int32, (seq, group_w), 1)
        masks = [(lane_head >= hd * head_dim) & (lane_head < (hd + 1) * head_dim) for hd in range(group_heads)]
        causal = row_id <= col_id

        def project(col):
            cols = pl.ds(col, qk_w)
            qkv[:, cols] = (_dot(hbuf[...], wqkv[:, cols]) + bqkv[:, cols]).astype(jnp.bfloat16)

        def by_head(act):
            zero = jnp.zeros_like(act)
            return jnp.concatenate([jnp.where(m, act, zero) for m in masks], axis=0)

        def scores_of(grp):
            q_heads = by_head(qkv[:, pl.ds(grp * twin_col, group_w)])
            key = qkv[:, pl.ds(grp * twin_col + group_w, group_w)]
            return lax.dot_general(key, q_heads, (((1,), (1,)), ((), ())), preferred_element_type=jnp.float32)

        def probs_of(scores):
            probs = []
            for hd in range(group_heads):
                sc = jnp.where(causal, scores[:, hd * seq:(hd + 1) * seq], -1e30)
                ex = jnp.exp2((sc - jnp.max(sc, axis=0, keepdims=True)) * (head_dim ** -0.5 * LOG2_E))
                probs.append((ex * (1.0 / jnp.sum(ex, axis=0, keepdims=True))).astype(jnp.bfloat16).T)
            return jnp.concatenate(probs, axis=1)

        def send_heads(grp, probs):
            val = qkv[:, pl.ds(v_col + grp * group_w, group_w)]
            obuf[slot, kind, 0, :, pl.ds(grp * group_w, group_w)] = _dot(probs, by_head(val)).astype(jnp.bfloat16)
            o_copy(kind, slot, grp).start()

        project(0)
        scores_0 = scores_of(0)
        project(v_col)
        send_heads(0, probs_of(scores_0))
        project(twin_col)
        send_heads(1, probs_of(scores_of(1)))

    def mlp(kind, i):
        slot = i % 2
        if kind == MATE:
            @pl.when(i == 0)
            def _():
                wait_weights((0,), (3, 4))

        def out_part(half, cols, kind=kind):
            return _dot(obuf[slot, kind, half], jnp.concatenate([wout[2 * half, :, cols], wout[2 * half + 1, :, cols]], axis=0))

        if kind == MATE:
            for both in (MATE, OWN):
                for c0 in range(0, d_model, OUT_CHUNK):
                    cols = pl.ds(c0, OUT_CHUNK)
                    acc[both, :, cols] = out_part(0, cols, both)
        for grp in range(2):
            o_copy(1 - kind, slot, grp).wait_recv()
        for c0 in range(0, d_model, OUT_CHUNK):
            cols = pl.ds(c0, OUT_CHUNK)
            att = ((acc[kind, :, cols] + out_part(1, cols)) + _f32(b_out[:, cols])).astype(jnp.bfloat16)
            x1buf[kind, :, cols] = (_f32(xbuf[kind, i, :, cols]) + _f32(att)).astype(jnp.bfloat16)

        gain, bias = _f32(ln2_gain[...]), _f32(ln2_bias[...])
        for r0 in range(0, seq, LN_ROWS):
            rows = pl.ds(r0, LN_ROWS)
            hbuf[rows, :] = _norm_rows(_f32(x1buf[kind, rows, :]), gain, bias)

        if kind == MATE:
            @pl.when(i == 0)
            def _():
                wait_weights((1, 2), (5, 6))

        for grp in range(2):
            for c0 in range(0, ff, UP_CHUNK):
                cols = pl.ds(c0, UP_CHUNK)
                pre = _dot(hbuf[...], wup[grp, :, cols]) + _f32(bup[grp, :, cols])
                ubuf[grp, :, cols] = jax.nn.gelu(pre, approximate=True).astype(jnp.bfloat16)

        if kind == MATE:
            @pl.when(i == 0)
            def _():
                wait_weights((3,), (7,))

            @pl.when(i >= 1)
            def _():
                for idx in range(p_chunks):
                    p_copy(slot, idx).wait_send()

        for idx in range(p_chunks):
            cols = pl.ds(idx * DOWN_CHUNK, DOWN_CHUNK)
            pown[kind, :, cols] = (_dot(ubuf[0], wdn[0, :, cols]) + _dot(ubuf[1], wdn[1, :, cols])).astype(jnp.bfloat16)
            if kind == MATE:
                p_copy(slot, idx).start()

    def finish(i):
        slot = i % 2

        @pl.when(i >= 2)
        def _():
            y_wait(i - 2, slot)

        for idx in range(p_chunks):
            cols = pl.ds(idx * DOWN_CHUNK, DOWN_CHUNK)
            p_copy(slot, idx).wait_recv()
            both = (_f32(pown[OWN, :, cols]) + _f32(prcv[slot, :, cols])) + _f32(b_down[:, cols])
            ybuf[slot, :, cols] = (_f32(x1buf[OWN, :, cols]) + _f32(both.astype(jnp.bfloat16))).astype(jnp.bfloat16)
            y_start(i, slot, cols)
        y_local(i, slot).start()

    def replicate(i):
        @pl.when(i < eager)
        def _():
            y_mate(i, i % 2).start()

            @pl.when(i >= 1)
            def _():
                y_forward(i - 1)

    def step(i, carry):
        def finish_before(place):
            @pl.when(lagged & (i >= 1) & (lag_place == place))
            def _():
                finish(i - 1)

        def attention_kind(kind, inner):
            attention(kind, i)

            @pl.when(kind == OWN)
            def _():
                finish_before(0)
            return inner

        lax.fori_loop(0, 2, attention_kind, 0)
        @pl.when(i >= 1)
        def _():
            hand_over(i - 1)
        finish_before(1)

        @pl.when(lagged & (i >= 1) & (copy_place == 0))
        def _():
            replicate(i - 1)
        mlp(MATE, i)

        @pl.when(lagged & (i >= 1) & (copy_place == 1))
        def _():
            replicate(i - 1)
        mlp(OWN, i)

        @pl.when(lagged & (i >= 1) & (copy_place == 2))
        def _():
            replicate(i - 1)

        @pl.when(jnp.logical_not(lagged))
        def _():
            finish(i)
            replicate(i)
        return carry

    lax.fori_loop(0, units, step, 0)

    @pl.when(lagged)
    def _():
        finish(units - 1)
        replicate(units - 1)

    hand_over(units - 1)
    for i in range(max(units - 2, 0), units):
        y_wait(i, i % 2)

    def late(i, carry):
        y_mate_late(i).start()
        return carry

    def forward(i, carry):
        y_forward(i)
        return carry

    lax.fori_loop(eager, units, late, 0)
    lax.fori_loop(jnp.maximum(eager - 1, 0), units, forward, 0)

    @pl.when(helped > 0)
    def _():
        def pass_on(i, carry):
            @pl.when(i < helped)
            def _():
                y_hop_in(i).wait_recv()
                y_hop_over(i).start()

            @pl.when(i >= 1)
            def _():
                y_hop_over(i - 1).wait_recv()
                y_hop_out(i - 1).start()
            return carry

        lax.fori_loop(0, helped + 1, pass_on, 0)

    for idx, amount in enumerate(RELAY_UNITS):
        if amount:
            @pl.when(3 - quarter == idx)
            def _(amount=amount):
                rows = pl.ds(0, min(amount, units) * seq)
                remote(relay_a.at[rows], relay_b.at[rows], ryh_sem.at[0], ryb_sem.at[0], to_mate).wait_send()
                remote(relay_b.at[rows], relay_a.at[rows], ryh_sem.at[1], yf_sem.at[1], {"pp": ally}).wait_send()

    for i in range(max(units - 2, 0), units):
        for kind in range(2):
            for grp in range(2):
                o_copy(kind, i % 2, grp).wait_send()

        @pl.when(odd == 1)
        def _():
            wb_copy(i, i % 2).wait_send()
    for idx in range(p_chunks):
        p_copy(0, idx).wait_send()
    for copy in passes:
        copy.wait_send()

    @pl.when(jnp.logical_not(lender) & lends_all)
    def _():
        remote(relay_a, relay_b, hop_sem.at[0], rb_sem.at[0], to_mate).wait_send()
        remote(relay_b, wdn.at[1], hop_sem.at[1], wr_sem.at[7], {"pp": ally}).wait_send()

    @pl.when(jnp.logical_not(lender) & jnp.logical_not(lends_all))
    def _():
        some = pl.ds(0, lend_some * part)
        remote(relay_a.at[some], relay_b.at[some], hop_sem.at[0], rb_sem.at[0], to_mate).wait_send()
        remote(relay_b.at[some], wdn.at[1, some], hop_sem.at[1], wr_sem.at[7], {"pp": ally}).wait_send()

    def late_sent(i, carry):
        y_mate_late(i).wait_send()
        return carry

    lax.fori_loop(eager, units, late_sent, 0)

    def arrived(i, carry):
        @pl.when(by_mate(i))
        def _():
            y_mate_late(i).wait_recv()

        @pl.when(jnp.logical_not(by_mate(i) | hands_over))
        def _():
            twin_arrival(i).wait_recv()

        @pl.when(hands_over)
        def _():
            x_over(i).wait_send()
        return carry

    lax.fori_loop(0, units, arrived, 0)
    mate_rows = pl.ds(mate * units, units)
    remote(y_hbm.at[mate_rows], y_hbm.at[mate_rows], yf_sem.at[0], yf_sem.at[1], to_twin).wait()


def _copy_kernel(src, dst, buf, in_sem, out_sem):
    slots, rows = buf.shape[:2]
    blocks = src.shape[0] // rows

    def load(c):
        return pltpu.make_async_copy(src.at[pl.ds(c * rows, rows)], buf.at[c % slots], in_sem.at[c % slots])

    def store(c):
        return pltpu.make_async_copy(buf.at[c % slots], dst.at[pl.ds(c * rows, rows)], out_sem.at[c % slots])

    for c in range(min(slots, blocks)):
        load(c).start()
    for c in range(blocks):
        load(c).wait()
        store(c).start()
        if c >= 1 and c - 1 + slots < blocks:
            store(c - 1).wait()
            load(c - 1 + slots).start()
    for c in range(max(blocks - slots, 0), blocks):
        store(c).wait()


def solution(mesh):
    stages = mesh.shape["pp"]
    weight_specs = (
        P('pp', None), P('pp', None),
        P('pp', None, None, 'tp', None), P('pp', None, 'tp', None),
        P('pp', 'tp', None, None), P('pp', None),
        P('pp', None), P('pp', None),
        P('pp', None, 'tp'), P('pp', 'tp'),
        P('pp', 'tp', None), P('pp', None),
    )
    if mesh.shape["tp"] != 4 or stages % 4:
        raise ValueError("unsupported mesh")

    def local_run(x_micro, ln1_gain, ln1_bias, w_qkv, b_qkv, w_out, b_out, ln2_gain, ln2_bias, w_up, b_up, w_down, b_down):
        micro, rows, seq, d_model = x_micro.shape
        total = micro * rows
        units = total // mesh.shape["tp"]
        _, _, _, heads, head_dim = w_qkv.shape
        group_w = heads * head_dim
        ff = w_up.shape[-1]
        x_seqs = x_micro.reshape(total, seq, d_model)
        w_qkv = jnp.transpose(w_qkv[0], (0, 2, 3, 1)).reshape(3 * group_w, d_model)
        w_out = w_out.reshape(group_w, d_model)
        any_spec = pl.BlockSpec(memory_space=pl.ANY)
        bf16, dma = jnp.bfloat16, pltpu.SemaphoreType.DMA
        p_chunks = d_model // DOWN_CHUNK
        y_all = pl.pallas_call(
            functools.partial(_pipeline_kernel, stages, head_dim),
            out_shape=jax.ShapeDtypeStruct((total, seq, d_model), bf16),
            in_specs=[any_spec] * 13,
            out_specs=any_spec,
            scratch_shapes=[
                pltpu.VMEM((d_model, 6 * group_w), bf16),
                pltpu.VMEM((4, group_w, d_model), bf16),
                pltpu.VMEM((2, d_model, ff), bf16),
                pltpu.VMEM((2, ff, d_model), bf16),
                pltpu.VMEM((1, 6 * group_w), jnp.float32),
                pltpu.VMEM((2, 1, ff), bf16),
                pltpu.VMEM((2, units, seq, d_model), bf16),
                pltpu.VMEM((seq, d_model), bf16),
                pltpu.VMEM((seq, 6 * group_w), bf16),
                pltpu.VMEM((2, 2, 2, seq, 2 * group_w), bf16),
                pltpu.VMEM((2, seq, d_model), jnp.float32),
                pltpu.VMEM((2, seq, d_model), bf16),
                pltpu.VMEM((2, seq, ff), bf16),
                pltpu.VMEM((2, seq, d_model), bf16),
                pltpu.VMEM((2, seq, d_model), bf16),
                pltpu.VMEM((2, seq, d_model), bf16),
                pltpu.VMEM((ff, d_model), bf16),
                pltpu.VMEM((ff, d_model), bf16),
                pltpu.VMEM((2, TURN_ROWS, d_model), bf16),
                dma((2, units)), dma((6,)), dma((10,)), dma((10,)),
                dma((2, 2, 2)), dma((2, 2, 2)), dma((p_chunks,)), dma((2, p_chunks)),
                dma((2,)), dma((2,)), dma((2,)), dma((2,)), dma((units,)), dma((2,)), dma((units,)), dma((units,)),
                dma((2,)), dma((RELAY_STEPS,)), dma((RELAY_STEPS,)), dma((2,)),
                dma((units,)), dma((units,)), dma((2,)), dma((units,)),
                pltpu.VMEM(b_qkv.shape, bf16), *[pltpu.VMEM((1, d_model), bf16) for _ in range(6)], dma((7,)),
            ],
            compiler_params=pltpu.CompilerParams(collective_id=0, has_side_effects=True, vmem_limit_bytes=60 * 1024 * 1024),
            name="stage_pipeline",
        )(x_seqs, w_qkv, w_out, w_up.reshape(d_model, ff), w_down.reshape(ff, d_model), b_qkv, b_up,
          ln1_gain, ln1_bias, b_out, ln2_gain, ln2_bias, b_down)
        block_rows = max(d for d in range(1, COPY_ROWS + 1) if total % d == 0)
        y_all = pl.pallas_call(
            _copy_kernel,
            out_shape=jax.ShapeDtypeStruct((total, seq, d_model), bf16),
            in_specs=[any_spec],
            out_specs=any_spec,
            scratch_shapes=[pltpu.VMEM((COPY_SLOTS, block_rows, seq, d_model), bf16), dma((COPY_SLOTS,)), dma((COPY_SLOTS,))],
            compiler_params=pltpu.CompilerParams(vmem_limit_bytes=56 * 1024 * 1024),
            name="result_copy",
        )(y_all)
        return y_all.reshape(1, micro, rows, seq, d_model)

    return jax.shard_map(local_run, mesh=mesh, in_specs=(P(None, 'dp', None, None),) + weight_specs, out_specs=P('pp', None, 'dp', None, None), check_vma=False)
```

```python
import functools

import jax
import jax.numpy as jnp
from jax import lax
from jax.experimental import pallas as pl
from jax.experimental.pallas import tpu as pltpu
from jax.sharding import PartitionSpec as P

LN_EPS = 1e-5
LOG2_E = 1.4426950408889634
MESH = pl.DeviceIdType.MESH
LN_ROWS = 16
UP_CHUNK = 512
DOWN_CHUNK = 512
OUT_CHUNK = 512
RELAY_STEPS = 16
LAGGED_STAGES = 2
LAG_PLACES = (1, 1)
COPY_PLACES = (0, 0)
RELAY_UNITS = (0, 0, 5, 10)
EAGER_UNITS = (0, 0, 3, 12)
TURN_ROWS = 128
COPY_ROWS = 1
COPY_SLOTS = 32


def _f32(val):
    return val.astype(jnp.float32)


def _norm_rows(rows, gain, bias):
    width = rows.shape[-1]
    mean = jnp.sum(rows, axis=-1, keepdims=True) * (1.0 / width)
    cen = rows - mean
    var = jnp.sum(cen * cen, axis=-1, keepdims=True) * (1.0 / width)
    return (cen * lax.rsqrt(var + LN_EPS) * gain + bias).astype(jnp.bfloat16)


def _dot(lhs, rhs):
    return jnp.dot(lhs, rhs, preferred_element_type=jnp.float32)


def _pipeline_kernel(stages, head_dim, x_hbm, wqkv_hbm, wout_hbm, wup_hbm, wdn_hbm, bqkv_hbm, bup_in,
                     ln1_gain_hbm, ln1_bias_hbm, b_out_hbm, ln2_gain_hbm, ln2_bias_hbm, b_down_hbm,
                     y_hbm,
                     wqkv, wout, wup, wdn, bqkv, bup, xbuf, hbuf, qkv, obuf, acc, x1buf, ubuf, pown, prcv, ybuf,
                     relay_a, relay_b, turn,
                     x_sem, wl_sem, ws_sem, wr_sem, os_sem, or_sem, ps_sem, pr_sem, yl_sem, yn_sem, yd_sem, ym_sem, ymr_sem, yf_sem, yt_sem, yl_late,
                     wb_sem, ra_sem, rb_sem, hop_sem, rya_sem, ryb_sem, ryh_sem, xo_sem,
                     bqkv_in, ln1_gain, ln1_bias, b_out, ln2_gain, ln2_bias, b_down, small_sem):
    _, units, seq, d_model = xbuf.shape
    group_w = wout_hbm.shape[0]
    group_heads = group_w // head_dim
    qk_w = 2 * group_w
    v_col, twin_col = qk_w, qk_w + 2 * group_w
    ff = wup_hbm.shape[1]
    rr = lax.axis_index("tp")
    pp = lax.axis_index("pp")
    odd = pp % 2
    near, far = rr + 1 - 2 * (rr % 2), 3 - rr
    mate = odd * near + (1 - odd) * far
    twin = odd * far + (1 - odd) * near
    has_next = pp + 1 < stages
    has_prev = pp > 0
    lagged = pp >= stages - LAGGED_STAGES
    is_last = pp == stages - 1
    hands_over = (odd == 1) & has_next
    copy_place = jnp.where(is_last, COPY_PLACES[1], COPY_PLACES[0])
    lag_place = jnp.where(is_last, LAG_PLACES[1], LAG_PLACES[0])
    cross = rr + 2 - 4 * (rr // 2)
    quarter = pp * 4 // stages

    def by_quarter(amounts, at):
        return sum(jnp.where(at == idx, min(amount, units), 0) for idx, amount in enumerate(amounts))

    eager = by_quarter(EAGER_UNITS, quarter)
    relayed = by_quarter(RELAY_UNITS, quarter)
    helped = by_quarter(RELAY_UNITS, 3 - quarter)
    lender = pp < stages // 2
    ally = stages - 1 - pp
    OWN, MATE = 0, 1

    def local(src, dst, sem):
        return pltpu.make_async_copy(src, dst, sem)

    def remote(src, dst, send, recv, dev):
        return pltpu.make_async_remote_copy(src_ref=src, dst_ref=dst, send_sem=send, recv_sem=recv, device_id=dev, device_id_type=MESH)

    barrier = pltpu.get_barrier_semaphore()

    def greet(dev):
        pl.semaphore_signal(barrier, inc=1, device_id=dev, device_id_type=MESH)

    greet({"tp": mate})
    greet({"tp": twin})
    greet({"pp": ally})

    @pl.when(has_next)
    def _():
        greet({"pp": pp + 1})
        greet({"tp": twin, "pp": pp + 1})

    @pl.when(has_prev)
    def _():
        greet({"pp": pp - 1})
        greet({"tp": mate, "pp": pp - 1})

    own_qk, twin_qk = pl.ds(0, qk_w), pl.ds(twin_col, qk_w)
    own_v, twin_v = pl.ds(v_col, group_w), pl.ds(v_col + group_w, group_w)
    turn_rows = turn.shape[1]
    turns = 3 * group_w // turn_rows

    def turn_load(c, slot):
        return local(wqkv_hbm.at[pl.ds(c * turn_rows, turn_rows)], turn.at[slot], wl_sem.at[slot])

    loads = [
        local(wout_hbm, wout.at[0], wl_sem.at[2]),
        local(wup_hbm, wup.at[0], wl_sem.at[3]),
        local(bup_in, bup.at[0], wl_sem.at[4]),
        local(wdn_hbm, wdn.at[0], wl_sem.at[5]),
    ]
    to_twin, to_mate = {"tp": twin}, {"tp": mate}
    passes = [
        remote(wqkv.at[:, own_qk], wqkv.at[:, twin_qk], ws_sem.at[0], wr_sem.at[0], to_twin),
        remote(bqkv.at[:, own_qk], bqkv.at[:, twin_qk], ws_sem.at[1], wr_sem.at[1], to_twin),
        remote(wout_hbm, wout.at[1], ws_sem.at[2], wr_sem.at[2], to_twin),
        remote(wout_hbm, wout.at[2], ws_sem.at[3], wr_sem.at[3], to_mate),
        remote(wout.at[1], wout.at[3], ws_sem.at[4], wr_sem.at[4], to_mate),
        remote(wup_hbm, wup.at[1], ws_sem.at[5], wr_sem.at[5], to_twin),
        remote(bup_in, bup.at[1], ws_sem.at[6], wr_sem.at[6], to_twin),
        remote(wdn_hbm, wdn.at[1], ws_sem.at[7], wr_sem.at[7], to_twin),
        remote(wqkv.at[:, own_v], wqkv.at[:, twin_v], ws_sem.at[8], wr_sem.at[8], to_twin),
        remote(bqkv.at[:, own_v], bqkv.at[:, twin_v], ws_sem.at[9], wr_sem.at[9], to_twin),
    ]

    def x_load(kind, i, row):
        return local(x_hbm.at[row * units + i], xbuf.at[kind, i], x_sem.at[kind, i])

    small = [
        local(src, dst, small_sem.at[idx])
        for idx, (src, dst) in enumerate([
            (bqkv_hbm, bqkv_in), (ln1_gain_hbm, ln1_gain), (ln1_bias_hbm, ln1_bias), (b_out_hbm, b_out),
            (ln2_gain_hbm, ln2_gain), (ln2_bias_hbm, ln2_bias), (b_down_hbm, b_down)])
    ]
    for copy in small:
        copy.start()
    turn_load(0, 0).start()
    turn_load(1, 1).start()

    @pl.when(pp == 0)
    def _():
        def start_x(i, carry):
            x_load(OWN, i, rr).start()
            x_load(MATE, i, mate).start()
            return carry
        lax.fori_loop(0, units, start_x, 0)

    for copy in loads:
        copy.start()

    pl.semaphore_wait(barrier, 3 + 2 * (jnp.where(has_next, 1, 0) + jnp.where(has_prev, 1, 0)))

    passes[2].start()

    steps = RELAY_STEPS
    part = ff // steps
    lend_some = max(steps // 4, 1)
    lends_all = (pp < stages // 4) | (pp >= stages - stages // 4)
    lent = jnp.where(lends_all, steps, lend_some)

    def relay_rows(c):
        return pl.ds(c * part, part)

    def hop_in(c):
        return remote(wdn_hbm.at[relay_rows(c)], relay_a.at[relay_rows(c)], ws_sem.at[7], ra_sem.at[c], {"pp": ally})

    def hop_over(c):
        return remote(relay_a.at[relay_rows(c)], relay_b.at[relay_rows(c)], hop_sem.at[0], rb_sem.at[c], to_mate)

    def hop_out(c):
        return remote(relay_b.at[relay_rows(c)], wdn.at[1, relay_rows(c)], hop_sem.at[1], wr_sem.at[7], {"pp": ally})

    def direct(c):
        return remote(wdn_hbm.at[relay_rows(c)], wdn.at[1, relay_rows(c)], ws_sem.at[7], wr_sem.at[7], to_twin)

    @pl.when(lender)
    def _():
        def lend(c, carry):
            hop_in(c).start()
            return carry
        lax.fori_loop(0, lent, lend, 0)
        passes[3].start()
        passes[2].wait_recv()
        passes[4].start()

    def turn_block(c, carry):
        slot = c % 2
        turn_load(c, slot).wait()
        wqkv[:, pl.ds(pl.multiple_of(c * turn_rows, 128), turn_rows)] = turn[slot].T

        @pl.when(c + 2 < turns)
        def _():
            turn_load(c + 2, slot).start()
        return carry

    lax.fori_loop(0, turns, turn_block, 0)
    for copy in small:
        copy.wait()
    spread_row = lax.broadcasted_iota(jnp.int32, (head_dim, group_w), 0)
    spread_col = lax.broadcasted_iota(jnp.int32, (head_dim, group_w), 1)
    spread = jnp.zeros((head_dim, group_w), jnp.float32)
    for hd in range(group_heads):
        spread = spread + jnp.where(spread_row + hd * head_dim == spread_col, 1.0, 0.0)
    spread = spread.astype(jnp.bfloat16)
    head_row = lax.broadcasted_iota(jnp.int32, (group_heads, group_w), 0)
    head_lane = lax.broadcasted_iota(jnp.int32, (group_heads, group_w), 1)
    in_head = (head_lane >= head_row * head_dim) & (head_lane < (head_row + 1) * head_dim)
    for third in range(3):
        wide = jnp.where(in_head, _dot(bqkv_in[0, third], spread), 0.0)
        bqkv[:, pl.ds(third * group_w, group_w)] = jnp.sum(wide, axis=0, keepdims=True)
    for idx in (0, 8, 1, 9, 5, 6):
        passes[idx].start()

    @pl.when(lender)
    def _():
        def keep(c, carry):
            direct(c).start()
            return carry
        lax.fori_loop(lent, steps, keep, 0)

    @pl.when(jnp.logical_not(lender))
    def _():
        passes[7].start()

        def relay(c, carry):
            @pl.when(c < lent)
            def _():
                hop_in(c).wait_recv()
                hop_over(c).start()

            @pl.when(c >= 1)
            def _():
                hop_over(c - 1).wait_recv()
                hop_out(c - 1).start()
            return carry
        lax.fori_loop(0, lent + 1, relay, 0)
        passes[3].start()
        passes[2].wait_recv()
        passes[4].start()

    def wait_weights(load_idx, pass_idx):
        for idx in load_idx:
            loads[idx].wait()
        for idx in pass_idx:
            passes[idx].wait_recv()

    row_id = lax.broadcasted_iota(jnp.int32, (seq, seq), 0)
    col_id = lax.broadcasted_iota(jnp.int32, (seq, seq), 1)

    def o_copy(kind, slot, grp):
        cols = pl.ds(grp * group_w, group_w)
        return remote(obuf.at[slot, kind, 0, :, cols], obuf.at[slot, 1 - kind, 1, :, cols],
                      os_sem.at[slot, kind, grp], or_sem.at[slot, 1 - kind, grp], to_mate)

    def p_copy(slot, idx):
        cols = pl.ds(idx * DOWN_CHUNK, DOWN_CHUNK)
        return remote(pown.at[MATE, :, cols], prcv.at[slot, :, cols], ps_sem.at[idx], pr_sem.at[slot, idx], to_mate)

    p_chunks = d_model // DOWN_CHUNK
    all_cols = pl.ds(0, d_model)

    def y_local(i, slot):
        return local(ybuf.at[slot], y_hbm.at[rr * units + i], yl_sem.at[slot])

    def y_next(i, slot, cols):
        return remote(ybuf.at[slot, :, cols], xbuf.at[OWN, i, :, cols], yn_sem.at[slot], x_sem.at[OWN, i], {"pp": pp + 1})

    def y_diag(i, slot, cols):
        return remote(ybuf.at[slot, :, cols], xbuf.at[MATE, i, :, cols], yd_sem.at[slot], x_sem.at[MATE, i], {"tp": twin, "pp": pp + 1})

    def y_twin(i, slot, cols):
        return remote(ybuf.at[slot, :, cols], y_hbm.at[rr * units + i, :, cols], yd_sem.at[slot], yt_sem.at[i], to_twin)

    def y_mate(i, slot):
        return remote(ybuf.at[slot], y_hbm.at[rr * units + i], ym_sem.at[slot], ymr_sem.at[i], to_mate)

    def y_mate_late(i):
        ref = y_hbm.at[rr * units + i]
        return remote(ref, ref, yl_late.at[i], ymr_sem.at[i], to_mate)

    def y_forward_mate(i):
        ref = y_hbm.at[mate * units + i]
        return remote(ref, ref, yf_sem.at[0], yf_sem.at[1], to_twin)

    def y_forward_twin(i):
        ref = y_hbm.at[twin * units + i]
        return remote(ref, ref, yf_sem.at[0], yf_sem.at[1], to_mate)

    def twin_arrival(i):
        ref = y_hbm.at[twin * units + i]
        return remote(ref, ref, yd_sem.at[0], yt_sem.at[i], to_twin)

    def y_hop_in(i):
        return remote(y_hbm.at[mate * units + i], relay_a.at[pl.ds(i * seq, seq)], yf_sem.at[0], rya_sem.at[i], {"pp": ally})

    def y_hop_over(i):
        rows = pl.ds(i * seq, seq)
        return remote(relay_a.at[rows], relay_b.at[rows], ryh_sem.at[0], ryb_sem.at[i], to_mate)

    def y_hop_out(i):
        return remote(relay_b.at[pl.ds(i * seq, seq)], y_hbm.at[cross * units + i], ryh_sem.at[1], yf_sem.at[1], {"pp": ally})

    def by_mate(i):
        return is_last & (i % 2 == 0) & (i >= relayed)

    def y_forward(i):
        @pl.when(by_mate(i))
        def _():
            twin_arrival(i).wait_recv()
            y_forward_twin(i).start()

        @pl.when(jnp.logical_not(by_mate(i)))
        def _():
            y_mate_late(i).wait_recv()

            @pl.when(i < relayed)
            def _():
                y_hop_in(i).start()

            @pl.when(i >= relayed)
            def _():
                y_forward_mate(i).start()

    def y_start(i, slot, cols):
        @pl.when(has_next)
        def _():
            y_next(i, slot, cols).start()

        @pl.when(odd == 0)
        def _():
            y_diag(i, slot, cols).start()

        @pl.when(odd == 1)
        def _():
            y_twin(i, slot, cols).start()

    def y_wait(i, slot):
        y_local(i, slot).wait()

        @pl.when(has_next)
        def _():
            y_next(i, slot, all_cols).wait_send()

        @pl.when(odd == 0)
        def _():
            y_diag(i, slot, all_cols).wait_send()

        @pl.when(odd == 1)
        def _():
            y_twin(i, slot, all_cols).wait_send()

        @pl.when(i < eager)
        def _():
            y_mate(i, slot).wait_send()

    def x_over(i):
        return remote(y_hbm.at[twin * units + i], xbuf.at[MATE, i], xo_sem.at[i], x_sem.at[MATE, i], {"pp": pp + 1})

    def hand_over(i):
        @pl.when(hands_over)
        def _():
            twin_arrival(i).wait_recv()
            x_over(i).start()

    def wb_copy(i, slot):
        return remote(xbuf.at[MATE, i], y_hbm.at[mate * units + i], wb_sem.at[slot], yt_sem.at[i], {"pp": pp - 1})

    def attention(kind, i):
        slot = i % 2
        x_load(kind, i, rr).wait()

        @pl.when((kind == MATE) & (odd == 1))
        def _():
            @pl.when(i >= 2)
            def _():
                wb_copy(i - 2, slot).wait_send()
            wb_copy(i, slot).start()

        @pl.when((kind == OWN) & (i == 0))
        def _():
            wait_weights((), (0, 1, 8, 9))

        @pl.when(i >= 2)
        def _():
            for grp in range(2):
                o_copy(kind, slot, grp).wait_send()

        gain, bias = _f32(ln1_gain[...]), _f32(ln1_bias[...])
        for r0 in range(0, seq, LN_ROWS):
            rows = pl.ds(r0, LN_ROWS)
            hbuf[rows, :] = _norm_rows(_f32(xbuf[kind, i, rows, :]), gain, bias)

        lane_head = lax.broadcasted_iota(jnp.int32, (seq, group_w), 1)
        masks = [(lane_head >= hd * head_dim) & (lane_head < (hd + 1) * head_dim) for hd in range(group_heads)]
        causal = row_id <= col_id

        def project(col):
            cols = pl.ds(col, qk_w)
            qkv[:, cols] = (_dot(hbuf[...], wqkv[:, cols]) + bqkv[:, cols]).astype(jnp.bfloat16)

        def by_head(act):
            zero = jnp.zeros_like(act)
            return jnp.concatenate([jnp.where(m, act, zero) for m in masks], axis=0)

        def scores_of(grp):
            q_heads = by_head(qkv[:, pl.ds(grp * twin_col, group_w)])
            key = qkv[:, pl.ds(grp * twin_col + group_w, group_w)]
            return lax.dot_general(key, q_heads, (((1,), (1,)), ((), ())), preferred_element_type=jnp.float32)

        def probs_of(scores):
            probs = []
            for hd in range(group_heads):
                sc = jnp.where(causal, scores[:, hd * seq:(hd + 1) * seq], -1e30)
                ex = jnp.exp2((sc - jnp.max(sc, axis=0, keepdims=True)) * (head_dim ** -0.5 * LOG2_E))
                probs.append((ex * (1.0 / jnp.sum(ex, axis=0, keepdims=True))).astype(jnp.bfloat16).T)
            return jnp.concatenate(probs, axis=1)

        def send_heads(grp, probs):
            val = qkv[:, pl.ds(v_col + grp * group_w, group_w)]
            obuf[slot, kind, 0, :, pl.ds(grp * group_w, group_w)] = _dot(probs, by_head(val)).astype(jnp.bfloat16)
            o_copy(kind, slot, grp).start()

        project(0)
        scores_0 = scores_of(0)
        project(v_col)
        send_heads(0, probs_of(scores_0))
        project(twin_col)
        send_heads(1, probs_of(scores_of(1)))

    def mlp(kind, i):
        slot = i % 2
        if kind == MATE:
            @pl.when(i == 0)
            def _():
                wait_weights((0,), (3, 4))

        def out_part(half, cols, kind=kind):
            return _dot(obuf[slot, kind, half], jnp.concatenate([wout[2 * half, :, cols], wout[2 * half + 1, :, cols]], axis=0))

        if kind == MATE:
            for both in (MATE, OWN):
                for c0 in range(0, d_model, OUT_CHUNK):
                    cols = pl.ds(c0, OUT_CHUNK)
                    acc[both, :, cols] = out_part(0, cols, both)
        for grp in range(2):
            o_copy(1 - kind, slot, grp).wait_recv()
        for c0 in range(0, d_model, OUT_CHUNK):
            cols = pl.ds(c0, OUT_CHUNK)
            att = ((acc[kind, :, cols] + out_part(1, cols)) + _f32(b_out[:, cols])).astype(jnp.bfloat16)
            x1buf[kind, :, cols] = (_f32(xbuf[kind, i, :, cols]) + _f32(att)).astype(jnp.bfloat16)

        gain, bias = _f32(ln2_gain[...]), _f32(ln2_bias[...])
        for r0 in range(0, seq, LN_ROWS):
            rows = pl.ds(r0, LN_ROWS)
            hbuf[rows, :] = _norm_rows(_f32(x1buf[kind, rows, :]), gain, bias)

        if kind == MATE:
            @pl.when(i == 0)
            def _():
                wait_weights((1, 2), (5, 6))

        for grp in range(2):
            for c0 in range(0, ff, UP_CHUNK):
                cols = pl.ds(c0, UP_CHUNK)
                pre = _dot(hbuf[...], wup[grp, :, cols]) + _f32(bup[grp, :, cols])
                ubuf[grp, :, cols] = jax.nn.gelu(pre, approximate=True).astype(jnp.bfloat16)

        if kind == MATE:
            @pl.when(i == 0)
            def _():
                wait_weights((3,), (7,))

            @pl.when(i >= 1)
            def _():
                for idx in range(p_chunks):
                    p_copy(slot, idx).wait_send()

        for idx in range(p_chunks):
            cols = pl.ds(idx * DOWN_CHUNK, DOWN_CHUNK)
            pown[kind, :, cols] = (_dot(ubuf[0], wdn[0, :, cols]) + _dot(ubuf[1], wdn[1, :, cols])).astype(jnp.bfloat16)
            if kind == MATE:
                p_copy(slot, idx).start()

    def finish(i):
        slot = i % 2

        @pl.when(i >= 2)
        def _():
            y_wait(i - 2, slot)

        for idx in range(p_chunks):
            cols = pl.ds(idx * DOWN_CHUNK, DOWN_CHUNK)
            p_copy(slot, idx).wait_recv()
            both = (_f32(pown[OWN, :, cols]) + _f32(prcv[slot, :, cols])) + _f32(b_down[:, cols])
            ybuf[slot, :, cols] = (_f32(x1buf[OWN, :, cols]) + _f32(both.astype(jnp.bfloat16))).astype(jnp.bfloat16)
            y_start(i, slot, cols)
        y_local(i, slot).start()

    def replicate(i):
        @pl.when(i < eager)
        def _():
            y_mate(i, i % 2).start()

            @pl.when(i >= 1)
            def _():
                y_forward(i - 1)

    def step(i, carry):
        def finish_before(place):
            @pl.when(lagged & (i >= 1) & (lag_place == place))
            def _():
                finish(i - 1)

        def attention_kind(kind, inner):
            attention(kind, i)

            @pl.when(kind == OWN)
            def _():
                finish_before(0)
            return inner

        lax.fori_loop(0, 2, attention_kind, 0)
        @pl.when(i >= 1)
        def _():
            hand_over(i - 1)
        finish_before(1)

        @pl.when(lagged & (i >= 1) & (copy_place == 0))
        def _():
            replicate(i - 1)
        mlp(MATE, i)

        @pl.when(lagged & (i >= 1) & (copy_place == 1))
        def _():
            replicate(i - 1)
        mlp(OWN, i)

        @pl.when(lagged & (i >= 1) & (copy_place == 2))
        def _():
            replicate(i - 1)

        @pl.when(jnp.logical_not(lagged))
        def _():
            finish(i)
            replicate(i)
        return carry

    lax.fori_loop(0, units, step, 0)

    @pl.when(lagged)
    def _():
        finish(units - 1)
        replicate(units - 1)

    hand_over(units - 1)
    for i in range(max(units - 2, 0), units):
        y_wait(i, i % 2)

    def late(i, carry):
        y_mate_late(i).start()
        return carry

    def forward(i, carry):
        y_forward(i)
        return carry

    lax.fori_loop(eager, units, late, 0)
    lax.fori_loop(jnp.maximum(eager - 1, 0), units, forward, 0)

    @pl.when(helped > 0)
    def _():
        def pass_on(i, carry):
            @pl.when(i < helped)
            def _():
                y_hop_in(i).wait_recv()
                y_hop_over(i).start()

            @pl.when(i >= 1)
            def _():
                y_hop_over(i - 1).wait_recv()
                y_hop_out(i - 1).start()
            return carry

        lax.fori_loop(0, helped + 1, pass_on, 0)

    for idx, amount in enumerate(RELAY_UNITS):
        if amount:
            @pl.when(3 - quarter == idx)
            def _(amount=amount):
                rows = pl.ds(0, min(amount, units) * seq)
                remote(relay_a.at[rows], relay_b.at[rows], ryh_sem.at[0], ryb_sem.at[0], to_mate).wait_send()
                remote(relay_b.at[rows], relay_a.at[rows], ryh_sem.at[1], yf_sem.at[1], {"pp": ally}).wait_send()

    for i in range(max(units - 2, 0), units):
        for kind in range(2):
            for grp in range(2):
                o_copy(kind, i % 2, grp).wait_send()

        @pl.when(odd == 1)
        def _():
            wb_copy(i, i % 2).wait_send()
    for idx in range(p_chunks):
        p_copy(0, idx).wait_send()
    for copy in passes:
        copy.wait_send()

    @pl.when(jnp.logical_not(lender) & lends_all)
    def _():
        remote(relay_a, relay_b, hop_sem.at[0], rb_sem.at[0], to_mate).wait_send()
        remote(relay_b, wdn.at[1], hop_sem.at[1], wr_sem.at[7], {"pp": ally}).wait_send()

    @pl.when(jnp.logical_not(lender) & jnp.logical_not(lends_all))
    def _():
        some = pl.ds(0, lend_some * part)
        remote(relay_a.at[some], relay_b.at[some], hop_sem.at[0], rb_sem.at[0], to_mate).wait_send()
        remote(relay_b.at[some], wdn.at[1, some], hop_sem.at[1], wr_sem.at[7], {"pp": ally}).wait_send()

    def late_sent(i, carry):
        y_mate_late(i).wait_send()
        return carry

    lax.fori_loop(eager, units, late_sent, 0)

    def arrived(i, carry):
        @pl.when(by_mate(i))
        def _():
            y_mate_late(i).wait_recv()

        @pl.when(jnp.logical_not(by_mate(i) | hands_over))
        def _():
            twin_arrival(i).wait_recv()

        @pl.when(hands_over)
        def _():
            x_over(i).wait_send()
        return carry

    lax.fori_loop(0, units, arrived, 0)
    mate_rows = pl.ds(mate * units, units)
    remote(y_hbm.at[mate_rows], y_hbm.at[mate_rows], yf_sem.at[0], yf_sem.at[1], to_twin).wait()


def _copy_kernel(src, dst, buf, in_sem, out_sem):
    slots, rows = buf.shape[:2]
    blocks = src.shape[0] // rows

    def load(c):
        return pltpu.make_async_copy(src.at[pl.ds(c * rows, rows)], buf.at[c % slots], in_sem.at[c % slots])

    def store(c):
        return pltpu.make_async_copy(buf.at[c % slots], dst.at[pl.ds(c * rows, rows)], out_sem.at[c % slots])

    for c in range(min(slots, blocks)):
        load(c).start()
    for c in range(blocks):
        load(c).wait()
        store(c).start()
        if c >= 1 and c - 1 + slots < blocks:
            store(c - 1).wait()
            load(c - 1 + slots).start()
    for c in range(max(blocks - slots, 0), blocks):
        store(c).wait()


def solution(mesh):
    stages = mesh.shape["pp"]
    weight_specs = (
        P('pp', None), P('pp', None),
        P('pp', None, None, 'tp', None), P('pp', None, 'tp', None),
        P('pp', 'tp', None, None), P('pp', None),
        P('pp', None), P('pp', None),
        P('pp', None, 'tp'), P('pp', 'tp'),
        P('pp', 'tp', None), P('pp', None),
    )
    if mesh.shape["tp"] != 4 or stages % 4:
        raise ValueError("unsupported mesh")

    def local_run(x_micro, ln1_gain, ln1_bias, w_qkv, b_qkv, w_out, b_out, ln2_gain, ln2_bias, w_up, b_up, w_down, b_down):
        micro, rows, seq, d_model = x_micro.shape
        total = micro * rows
        units = total // mesh.shape["tp"]
        _, _, _, heads, head_dim = w_qkv.shape
        group_w = heads * head_dim
        ff = w_up.shape[-1]
        x_seqs = x_micro.reshape(total, seq, d_model)
        w_qkv = jnp.transpose(w_qkv[0], (0, 2, 3, 1)).reshape(3 * group_w, d_model)
        w_out = w_out.reshape(group_w, d_model)
        any_spec = pl.BlockSpec(memory_space=pl.ANY)
        bf16, dma = jnp.bfloat16, pltpu.SemaphoreType.DMA
        p_chunks = d_model // DOWN_CHUNK
        y_all = pl.pallas_call(
            functools.partial(_pipeline_kernel, stages, head_dim),
            out_shape=jax.ShapeDtypeStruct((total, seq, d_model), bf16),
            in_specs=[any_spec] * 13,
            out_specs=any_spec,
            scratch_shapes=[
                pltpu.VMEM((d_model, 6 * group_w), bf16),
                pltpu.VMEM((4, group_w, d_model), bf16),
                pltpu.VMEM((2, d_model, ff), bf16),
                pltpu.VMEM((2, ff, d_model), bf16),
                pltpu.VMEM((1, 6 * group_w), jnp.float32),
                pltpu.VMEM((2, 1, ff), bf16),
                pltpu.VMEM((2, units, seq, d_model), bf16),
                pltpu.VMEM((seq, d_model), bf16),
                pltpu.VMEM((seq, 6 * group_w), bf16),
                pltpu.VMEM((2, 2, 2, seq, 2 * group_w), bf16),
                pltpu.VMEM((2, seq, d_model), jnp.float32),
                pltpu.VMEM((2, seq, d_model), bf16),
                pltpu.VMEM((2, seq, ff), bf16),
                pltpu.VMEM((2, seq, d_model), bf16),
                pltpu.VMEM((2, seq, d_model), bf16),
                pltpu.VMEM((2, seq, d_model), bf16),
                pltpu.VMEM((ff, d_model), bf16),
                pltpu.VMEM((ff, d_model), bf16),
                pltpu.VMEM((2, TURN_ROWS, d_model), bf16),
                dma((2, units)), dma((6,)), dma((10,)), dma((10,)),
                dma((2, 2, 2)), dma((2, 2, 2)), dma((p_chunks,)), dma((2, p_chunks)),
                dma((2,)), dma((2,)), dma((2,)), dma((2,)), dma((units,)), dma((2,)), dma((units,)), dma((units,)),
                dma((2,)), dma((RELAY_STEPS,)), dma((RELAY_STEPS,)), dma((2,)),
                dma((units,)), dma((units,)), dma((2,)), dma((units,)),
                pltpu.VMEM(b_qkv.shape, bf16), *[pltpu.VMEM((1, d_model), bf16) for _ in range(6)], dma((7,)),
            ],
            compiler_params=pltpu.CompilerParams(collective_id=0, has_side_effects=True, vmem_limit_bytes=60 * 1024 * 1024),
            name="stage_pipeline",
        )(x_seqs, w_qkv, w_out, w_up.reshape(d_model, ff), w_down.reshape(ff, d_model), b_qkv, b_up,
          ln1_gain, ln1_bias, b_out, ln2_gain, ln2_bias, b_down)
        block_rows = max(d for d in range(1, COPY_ROWS + 1) if total % d == 0)
        y_all = pl.pallas_call(
            _copy_kernel,
            out_shape=jax.ShapeDtypeStruct((total, seq, d_model), bf16),
            in_specs=[any_spec],
            out_specs=any_spec,
            scratch_shapes=[pltpu.VMEM((COPY_SLOTS, block_rows, seq, d_model), bf16), dma((COPY_SLOTS,)), dma((COPY_SLOTS,))],
            compiler_params=pltpu.CompilerParams(vmem_limit_bytes=56 * 1024 * 1024),
            name="result_copy",
        )(y_all)
        return y_all.reshape(1, micro, rows, seq, d_model)

    return jax.shard_map(local_run, mesh=mesh, in_specs=(P(None, 'dp', None, None),) + weight_specs, out_specs=P('pp', None, 'dp', None, None), check_vma=False)
```
